32 devices in a mesh: gx: 4 (over x, core), gy: 2 (over y), gz: 4 (over z).
Axes of the slice: x: 2, y: 2, z: 4, core: 2. Of those that a mesh axis runs over, the one named last changes fastest.
Arguments:
- magnetization: float32 [3, 64, 64, 512], P(None, 'gx', 'gy', 'gz'), may hold values from -1 to 1, as said below
- kernel: float32 [6, 64, 512, 64], P(None, ('gx', 'gz'), 'gy'), may hold values from -3 to 3, as said below
- applied: float32 [3], replicated, may hold values from -4 to 4
Outputs:
- predicted: float32 [3, 64, 64, 512], P(None, 'gx', 'gy', 'gz')
- torque: float32 [3, 64, 64, 512], P(None, 'gx', 'gy', 'gz')
The draws below stay inside these ranges and needn't reach their ends.
Inputs may be any that keep to these rules, and one draw needn't show every extreme that they name: `magnetization`: each cell's three components form a vector of unit length. The tensor is even in wavenumber: kernel[c, ky, kz, kx] equals kernel[c, (64 - ky) mod 64, (512 - kz) mod 512, (64 - kx) mod 64].
All inputs are finite; a program needn't handle non-finite values.
Results may differ from the reference program's by a relative error of at most 0.00011.
Values sent between devices are 32-bit elements; how exact they have to be, the bound alone decides.
No kernel may reach another device: no remote copies, remote signals or barrier semaphores. Data moves between devices by JAX's collectives and lax.ppermute only.
A program may use at most 128 MiB of HBM per device.

```python
import math
import jax
import jax.numpy as jnp
from jax import lax

NX = 64
NY = 64
NZ = 512


def draw_magnetization(key, part):
    key_one, key_two = jax.random.split(jax.random.fold_in(key, 11))
    extent = (NX, NY, NZ)
    height = jax.random.uniform(key_one, extent, jnp.float32, -1.0, 1.0)
    azimuth = jax.random.uniform(key_two, extent, jnp.float32, -math.pi, math.pi)
    radius = jnp.sqrt(jnp.maximum(1.0 - height * height, 0.0))
    return jnp.stack([radius * jnp.cos(azimuth), radius * jnp.sin(azimuth), height])


def draw_kernel(key, part):
    inner = jax.random.fold_in(key, 23)
    extent = (6, NY, NZ, NX)
    raw = jnp.clip(0.5 * jax.random.normal(inner, extent, jnp.float32), -3.0, 3.0)
    mirrored = jnp.roll(jnp.flip(raw, (1, 2, 3)), 1, (1, 2, 3))
    return 0.5 * (raw + mirrored)


def gaussian(own_key, dims, width, limit, held_as=jnp.bfloat16):
    entries = width * jax.random.normal(own_key, dims, jnp.float32)
    return jnp.clip(entries, min=-limit, max=limit).astype(held_as)


def setup_inputs(seed: int = 0) -> dict:
    streams_of = jax.random.split(jax.random.key(seed), 4)
    return {
        "magnetization": draw_magnetization(jax.random.fold_in(streams_of[3], 71), 0),
        "kernel": draw_kernel(jax.random.fold_in(streams_of[3], 71), 0),
        "applied": gaussian(streams_of[2], (3,), 1.0, 4.0, jnp.float32),
    }


exchange_coeff = 1.0
damping = 0.3
time_step = 0.2

def cross_product(first_vec, second_vec):
    return jnp.stack([first_vec[1] * second_vec[2] - first_vec[2] * second_vec[1], first_vec[2] * second_vec[0] - first_vec[0] * second_vec[2], first_vec[0] * second_vec[1] - first_vec[1] * second_vec[0]])

def reference(magnetization, kernel, applied):
    laplace = -6.0 * magnetization
    for dimension in (1, 2, 3):
        laplace = laplace + jnp.roll(magnetization, 1, dimension) + jnp.roll(magnetization, -1, dimension)
    spectrum = jnp.fft.fftn(magnetization, axes=(1, 2, 3))
    tensor = jnp.transpose(kernel, (0, 3, 1, 2))
    product_spectrum = jnp.stack([tensor[0] * spectrum[0] + tensor[3] * spectrum[1] + tensor[4] * spectrum[2], tensor[3] * spectrum[0] + tensor[1] * spectrum[1] + tensor[5] * spectrum[2], tensor[4] * spectrum[0] + tensor[5] * spectrum[1] + tensor[2] * spectrum[2]])
    demagnetizing = -jnp.real(jnp.fft.ifftn(product_spectrum, axes=(1, 2, 3)))
    total_field = demagnetizing + exchange_coeff * laplace + applied[:, None, None, None]
    precess = cross_product(magnetization, total_field)
    double_twist = cross_product(magnetization, precess)
    torque = -(precess + damping * double_twist) / (1.0 + damping * damping)
    stepped = magnetization + time_step * torque
    length = jnp.sqrt(lax.optimization_barrier(jnp.sum(stepped * stepped, axis=0)))
    return (stepped / length, torque)
```

```python
import math

import jax
import jax.numpy as jnp
import numpy as np
from jax import lax
from jax.experimental import pallas as pl
from jax.experimental.pallas import tpu as pltpu
from jax.sharding import PartitionSpec as P

exchange_coeff = 1.0
damping = 0.3
time_step = 0.2
highest = lax.Precision.HIGHEST
LANES = 128
SUBS = 8
SLOTS = 8


def phase_table(row_index, col_index, length):
    product = row_index[:, None] * col_index[None, :] % length
    angles = product.astype(jnp.float32) * (2.0 * math.pi / length)
    return (jnp.cos(angles), jnp.sin(angles))


def forward_mix(real_part, imag_part, cosine_table, sine_table, pattern):
    real_out = jnp.einsum(pattern, real_part, cosine_table, precision=highest) + jnp.einsum(
        pattern, imag_part, sine_table, precision=highest
    )
    imag_out = jnp.einsum(pattern, imag_part, cosine_table, precision=highest) - jnp.einsum(
        pattern, real_part, sine_table, precision=highest
    )
    return (real_out, imag_out)


def inverse_mix(real_part, imag_part, cosine_table, sine_table, pattern):
    real_out = jnp.einsum(pattern, real_part, cosine_table, precision=highest) - jnp.einsum(
        pattern, imag_part, sine_table, precision=highest
    )
    imag_out = jnp.einsum(pattern, imag_part, cosine_table, precision=highest) + jnp.einsum(
        pattern, real_part, sine_table, precision=highest
    )
    return (real_out, imag_out)


def apply_tensor(kernel, spectrum):
    return jnp.stack(
        [
            kernel[0] * spectrum[0] + kernel[3] * spectrum[1] + kernel[4] * spectrum[2],
            kernel[3] * spectrum[0] + kernel[1] * spectrum[1] + kernel[5] * spectrum[2],
            kernel[4] * spectrum[0] + kernel[5] * spectrum[1] + kernel[2] * spectrum[2],
        ]
    )


def cross_product(first_vec, second_vec):
    return jnp.stack(
        [
            first_vec[1] * second_vec[2] - first_vec[2] * second_vec[1],
            first_vec[2] * second_vec[0] - first_vec[0] * second_vec[2],
            first_vec[0] * second_vec[1] - first_vec[1] * second_vec[0],
        ]
    )


def general_shards(magnetization, kernel, applied):
    count_gx = lax.axis_size("gx")
    count_gy = lax.axis_size("gy")
    count_gz = lax.axis_size("gz")
    local_x = magnetization.shape[1]
    local_y = magnetization.shape[2]
    local_z = magnetization.shape[3]
    full_x = local_x * count_gx
    full_y = local_y * count_gy
    full_z = local_z * count_gz
    part_x = local_x // count_gz
    part_y = full_y // (count_gx * count_gz)
    part_z = full_z // count_gy
    outside = applied[:, None, None, None]
    z_index = jnp.arange(full_z, dtype=jnp.int32)
    weights = jnp.ones((full_z,), jnp.float32)
    planes = z_index.shape[0] // count_gy
    wave_count = z_index.shape[0]
    zlines = lax.all_to_all(magnetization, "gz", split_axis=1, concat_axis=3, tiled=True)
    cos_zf, sin_zf = phase_table(z_index, z_index, full_z)
    cos_zb, sin_zb = phase_table(z_index, z_index, full_z)
    cos_zb = cos_zb * weights[:, None]
    sin_zb = sin_zb * weights[:, None]
    lines_shape = (3, part_x, local_y, full_z)
    wave_shape = (3, part_x, local_y, wave_count)
    z_rows = zlines.reshape(-1, full_z)
    spec_real = jnp.dot(z_rows, cos_zf, precision=highest).reshape(wave_shape)
    spec_imag = -jnp.dot(z_rows, sin_zf, precision=highest).reshape(wave_shape)
    spec_real, spec_imag = (
        lax.all_to_all(spec_real, "gy", split_axis=3, concat_axis=2, tiled=True),
        lax.all_to_all(spec_imag, "gy", split_axis=3, concat_axis=2, tiled=True),
    )
    y_index = jnp.arange(full_y, dtype=jnp.int32)
    cos_y, sin_y = phase_table(y_index, y_index, full_y)
    spec_real, spec_imag = forward_mix(spec_real, spec_imag, cos_y, sin_y, "cxyz,yk->ckxz")
    x_index = jnp.arange(full_x, dtype=jnp.int32)
    cos_xn, sin_xn = phase_table(x_index, x_index, full_x)
    spec_real, spec_imag = (
        lax.all_to_all(spec_real, ("gx", "gz"), split_axis=1, concat_axis=2, tiled=True),
        lax.all_to_all(spec_imag, ("gx", "gz"), split_axis=1, concat_axis=2, tiled=True),
    )
    cos_x, sin_x = (cos_xn, sin_xn)
    spec_real, spec_imag = forward_mix(spec_real, spec_imag, cos_x, sin_x, "cyxz,xk->cyzk")
    inverse_count = 1.0 / (full_x * full_y * full_z)
    out_real = -inverse_count * apply_tensor(kernel, spec_real)
    out_imag = -inverse_count * apply_tensor(kernel, spec_imag)
    wave_y = (lax.axis_index("gx") * count_gz + lax.axis_index("gz")) * part_y + jnp.arange(
        part_y, dtype=jnp.int32
    )
    wave_z = lax.axis_index("gy") * part_z + jnp.arange(planes, dtype=jnp.int32)
    eigenvalue = (
        lattice_eigen(wave_y, full_y)[:, None, None]
        + lattice_eigen(wave_z, full_z)[None, :, None]
        + lattice_eigen(x_index, full_x)[None, None, :]
    )
    factor = inverse_count * exchange_coeff * eigenvalue
    out_real = out_real + factor * spec_real
    out_imag = out_imag + factor * spec_imag
    back_real, back_imag = inverse_mix(out_real, out_imag, cos_xn, sin_xn, "cyzk,kx->cyxz")
    back_real, back_imag = (
        lax.all_to_all(back_real, ("gx", "gz"), split_axis=2, concat_axis=1, tiled=True),
        lax.all_to_all(back_imag, ("gx", "gz"), split_axis=2, concat_axis=1, tiled=True),
    )
    cos_yb, sin_yb = (cos_y, sin_y)
    back_real, back_imag = inverse_mix(back_real, back_imag, cos_yb, sin_yb, "cyxz,yn->cxnz")
    back_real, back_imag = (
        lax.all_to_all(back_real, "gy", split_axis=2, concat_axis=3, tiled=True),
        lax.all_to_all(back_imag, "gy", split_axis=2, concat_axis=3, tiled=True),
    )
    real_rows = back_real.reshape(-1, wave_count)
    imag_rows = back_imag.reshape(-1, wave_count)
    field_lines = (
        jnp.dot(real_rows, cos_zb, precision=highest)
        - jnp.dot(imag_rows, sin_zb, precision=highest)
    ).reshape(lines_shape)
    field_block = lax.all_to_all(field_lines, "gz", split_axis=3, concat_axis=1, tiled=True)
    total_field = field_block + outside
    precess = cross_product(magnetization, total_field)
    double_twist = cross_product(magnetization, precess)
    torque = -(precess + damping * double_twist) / (1.0 + damping * damping)
    stepped = magnetization + time_step * torque
    length = jnp.sqrt(jnp.sum(stepped * stepped, axis=0))
    return (stepped / length, torque)


def cmul_const(value, angle):
    re, im = value
    quarter = angle / (math.pi / 2)
    if abs(quarter - round(quarter)) < 1e-9:
        turn = round(quarter) % 4
        if turn == 0:
            return (re, im)
        if turn == 1:
            return (-im, re)
        if turn == 2:
            return (-re, -im)
        return (im, -re)
    c, s = math.cos(angle), math.sin(angle)
    if abs(abs(c) - abs(s)) < 1e-9:
        h = abs(c)
        sc, ss = math.copysign(1, c), math.copysign(1, s)
        first = re if sc > 0 else -re
        out_re = (first - im) if ss > 0 else (first + im)
        second = im if sc > 0 else -im
        out_im = (second + re) if ss > 0 else (second - re)
        return (h * out_re, h * out_im)
    return (c * re - s * im, c * im + s * re)


def cadd(a, b):
    return (a[0] + b[0], a[1] + b[1])


def csub(a, b):
    return (a[0] - b[0], a[1] - b[1])


def conj(a):
    return (a[0], -a[1])


def complex_fft(values, sign):
    n = len(values)
    if n == 1:
        return values
    even = complex_fft(values[0::2], sign)
    odd = complex_fft(values[1::2], sign)
    odd = [cmul_const(v, sign * 2 * math.pi * k / n) for k, v in enumerate(odd)]
    return [cadd(e, o) for e, o in zip(even, odd)] + [csub(e, o) for e, o in zip(even, odd)]


def real_fft(values):
    n = len(values)
    if n == 2:
        return [values[0] + values[1], values[0] - values[1]]
    even = real_fft(values[0::2])
    odd = real_fft(values[1::2])
    quarter = n // 4
    out = [None] * (n // 2 + 1)
    out[0] = even[0] + odd[0]
    out[n // 2] = even[0] - odd[0]
    for k in range(1, quarter):
        turned = cmul_const(odd[k], -2 * math.pi * k / n)
        out[k] = cadd(even[k], turned)
        out[n // 2 - k] = conj(csub(even[k], turned))
    out[quarter] = (even[quarter], -odd[quarter])
    return out


def real_ifft(values):
    n = 2 * (len(values) - 1)
    if n == 2:
        return [values[0] + values[1], values[0] - values[1]]
    quarter = n // 4
    even = [None] * (quarter + 1)
    odd = [None] * (quarter + 1)
    even[0] = values[0] + values[n // 2]
    odd[0] = values[0] - values[n // 2]
    for k in range(1, quarter):
        mirror = conj(values[n // 2 - k])
        even[k] = cadd(values[k], mirror)
        odd[k] = cmul_const(csub(values[k], mirror), 2 * math.pi * k / n)
    mid = values[quarter]
    even[quarter] = 2.0 * mid[0]
    odd[quarter] = -2.0 * mid[1]
    even = real_ifft(even)
    odd = real_ifft(odd)
    out = [None] * n
    out[0::2] = even
    out[1::2] = odd
    return out


def mm(a, b, dims):
    return lax.dot_general(
        a, b, (dims, ((), ())), precision=highest, preferred_element_type=jnp.float32
    )


class Plan:
    def __init__(self, cx, cy, cz, shape):
        comps, lx, ly, lz = shape
        self.comps, self.lx, self.ly, self.lz = comps, lx, ly, lz
        self.cx, self.cy, self.cz = cx, cy, cz
        self.nx, self.ny, self.nz = lx * cx, ly * cy, lz * cz
        self.planes = cx * cy
        self.groups = cx * cz
        self.devices = cx * cy * cz

    def fits(self):
        if self.devices % 1 or self.lz % self.planes:
            return False
        self.zc = self.lz // self.planes
        self.xl = LANES // self.ly if LANES % self.ly == 0 else 0
        return (
            self.comps == 3
            and self.xl == 4
            and self.cy == 2
            and self.nx == 16 * self.xl
            and self.lx % self.xl == 0
            and self.ly == 2 * self.groups
            and self.zc * SLOTS == LANES
            and self.lz == LANES
            and self.nz % self.zc == 0
        )


def slot_kx(plan, kx2, slot):
    if slot:
        return slot + 16 * kx2
    return (0, 16, 8, 24)[kx2]


def xy_tables(plan):
    lane = np.arange(LANES)
    xl, yl = lane // plan.ly, lane % plan.ly
    half = plan.ny // 2
    fwd = np.zeros((2, 256, 512))
    back = np.zeros((2, 256, 512))
    for r in range(2):
        for k2h in range(2):
            for g in range(plan.groups):
                for ri in range(2):
                    for k2l in range(2):
                        for ql in range(2):
                            block = ri if r == 0 else 1 - ri
                            f = (k2h * plan.groups + g) * 8 + block * 4 + k2l * 2 + ql
                            kx2 = 2 * k2h + k2l
                            ky = 2 * (2 * g + ql) + r
                            ph = 2 * math.pi * (xl * kx2 / 4 + yl * ky / plan.ny)
                            c, s = np.cos(ph), np.sin(ph)
                            if ri == 0:
                                fwd[r, f, 0:128], fwd[r, f, 128:256] = c, s
                                back[r, f, 0:128], back[r, f, 128:256] = c, s
                            else:
                                fwd[r, f, 0:128], fwd[r, f, 128:256] = -s, c
                                back[r, f, 0:128], back[r, f, 128:256] = -s, c
                            kx = slot_kx(plan, kx2, 0)
                            if kx2 == 0:
                                edge = ky in (0, half)
                                if edge:
                                    kx = 0 if ri == 0 else 32
                                else:
                                    kx = 0 if ky < half else 32
                            ph = 2 * math.pi * (xl * kx / plan.nx + yl * ky / plan.ny)
                            c, s = np.cos(ph), np.sin(ph)
                            at = 256 if kx % 16 == 0 else 384
                            if kx2 == 0 and edge:
                                fwd[r, f, at : at + 128] = c
                                back[r, f, at : at + 128] = c
                            else:
                                fwd[r, f, at : at + 128] = c if ri == 0 else -s
                                back[r, f, at : at + 128] = 2 * (c if ri == 0 else -s)
    return fwd.astype(np.float32), back.astype(np.float32)


def x_twiddles(plan):
    xl = np.arange(LANES) // plan.ly
    ph = 2 * math.pi * np.arange(SLOTS)[:, None] * xl[None, :] / plan.nx
    return np.stack([np.cos(ph), np.sin(ph)]).astype(np.float32)


def z_tables(plan):
    zc, nz = plan.zc, plan.nz
    lane = np.arange(LANES) % zc
    ph = 2 * math.pi * np.arange(plan.devices)[:, None] * lane[None, :] / nz
    twiddle = np.stack([np.cos(ph), np.sin(ph)]).astype(np.float32)
    small = 2 * math.pi * np.arange(zc)[:, None] * np.arange(zc)[None, :] / zc
    c = np.kron(np.eye(SLOTS), np.cos(small))
    s = np.kron(np.eye(SLOTS), np.sin(small))
    fwd = np.block([[c, -s], [s, c]]).astype(np.float32)
    back = np.block([[c, s], [-s, c]]).astype(np.float32)
    return twiddle, fwd, back


def pack_kernel(m_ref, out_ref):
    for t in range(m_ref.shape[0]):
        out_ref[:, LANES * t : LANES * (t + 1)] = m_ref[t].T


def xy_forward_kernel(plan, lines_ref, table_ref, tw_ref, out_ref, g_ref):
    zc = plan.zc
    per = plan.lx // plan.xl
    sub = lax.broadcasted_iota(jnp.int32, (SUBS, LANES), 0)
    low = sub < 4
    zero = jnp.zeros((zc, 256), jnp.float32)
    for r in range(2):
        g_ref[r, 0:zc, 0:256] = zero
        for k in range(1, SLOTS):
            g_ref[r, zc * k : zc * (k + 1), 256:512] = zero
    for c in range(plan.comps):
        parts = [[], []]
        for gx in range(plan.cx):
            for xh in range(per):
                at = c * (plan.lx * plan.ly) + xh * LANES
                first = lines_ref[gx * 2, :, at : at + LANES]
                second = lines_ref[gx * 2 + 1, :, at : at + LANES]
                parts[0].append(first + second)
                parts[1].append(first - second)
        outs = []
        for r in range(2):
            spec = real_fft(parts[r])
            g_ref[r, 0:zc, 256:384] = spec[0]
            g_ref[r, 0:zc, 384:512] = spec[8]
            for k in range(1, SLOTS):
                re, im = spec[k]
                tc = tw_ref[0, k : k + 1, :]
                ts = tw_ref[1, k : k + 1, :]
                g_ref[r, zc * k : zc * (k + 1), 0:128] = re * tc + im * ts
                g_ref[r, zc * k : zc * (k + 1), 128:256] = im * tc - re * ts
            outs.append(mm(table_ref[r], g_ref[r], ((1,), (1,))))
        for k2h in range(2):
            for g in range(plan.groups):
                f = (k2h * plan.groups + g) * SUBS
                one = outs[0][f : f + SUBS]
                two = outs[1][f : f + SUBS]
                gx, gz = g // plan.cz, g % plan.cz
                dest = gz * plan.planes + gx * plan.cy + k2h
                out_ref[dest, 2 * c] = jnp.where(low, one, two)
                out_ref[dest, 2 * c + 1] = pltpu.roll(jnp.where(low, two, one), 4, 0)


def xy_inverse_kernel(plan, spec_ref, table_ref, tw_ref, out_ref, h_ref):
    zc = plan.zc
    per = plan.lx // plan.xl
    sub = lax.broadcasted_iota(jnp.int32, (SUBS, LANES), 0)
    low = sub < 4
    for c in range(plan.comps):
        for k2h in range(2):
            for g in range(plan.groups):
                f = (k2h * plan.groups + g) * SUBS
                gx, gz = g // plan.cz, g % plan.cz
                src = gz * plan.planes + gx * plan.cy + k2h
                re = spec_ref[src, 2 * c]
                im = pltpu.roll(spec_ref[src, 2 * c + 1], 4, 0)
                h_ref[0, f : f + SUBS, :] = jnp.where(low, re, im)
                h_ref[1, f : f + SUBS, :] = jnp.where(low, im, re)
        pieces = [mm(h_ref[r].T, table_ref[r], ((1,), (0,))) for r in range(2)]
        fields = []
        for r in range(2):
            u = pieces[r]
            values = [u[0:zc, 256:384]]
            for k in range(1, SLOTS):
                re = u[zc * k : zc * (k + 1), 0:128]
                im = u[zc * k : zc * (k + 1), 128:256]
                tc = tw_ref[0, k : k + 1, :]
                ts = tw_ref[1, k : k + 1, :]
                values.append((re * tc - im * ts, im * tc + re * ts))
            values.append(u[0:zc, 384:512])
            fields.append(real_ifft(values))
        for gx in range(plan.cx):
            for xh in range(per):
                at = c * (plan.lx * plan.ly) + xh * LANES
                one = fields[0][gx * per + xh]
                two = fields[1][gx * per + xh]
                out_ref[gx * 2, :, at : at + LANES] = one + two
                out_ref[gx * 2 + 1, :, at : at + LANES] = one - two


def z_kernel(plan, in_ref, k_ref, kx_ref, mask_ref, tw_ref, fwd_ref, back_ref, out_ref, s_ref):
    n = plan.devices
    mask = mask_ref[...]
    keep = 1.0 - mask

    def to_spectrum(values, at):
        values = complex_fft(values, -1)
        for k in range(n):
            re, im = values[k]
            tc = tw_ref[0, k : k + 1, :]
            ts = tw_ref[1, k : k + 1, :]
            s_ref[at, SUBS * k : SUBS * (k + 1), 0:128] = re * tc + im * ts
            s_ref[at, SUBS * k : SUBS * (k + 1), 128:256] = im * tc - re * ts
        s_ref[at] = mm(s_ref[at], fwd_ref[...], ((1,), (0,)))

    def from_spectrum(at):
        s_ref[at] = mm(s_ref[at], back_ref[...], ((1,), (0,)))
        values = []
        for k in range(n):
            re = s_ref[at, SUBS * k : SUBS * (k + 1), 0:128]
            im = s_ref[at, SUBS * k : SUBS * (k + 1), 128:256]
            tc = tw_ref[0, k : k + 1, :]
            ts = tw_ref[1, k : k + 1, :]
            values.append((re * tc - im * ts, im * tc + re * ts))
        return complex_fft(values, 1)

    for c in range(plan.comps):
        to_spectrum([(in_ref[s, 2 * c], in_ref[s, 2 * c + 1] * keep) for s in range(n)], c)
    extra = []
    zeros = jnp.zeros((SUBS, LANES), jnp.float32)
    for s in range(n):
        e = in_ref[s, 1] * mask
        e = e + pltpu.roll(in_ref[s, 3] * mask, 1, 0)
        e = e + pltpu.roll(in_ref[s, 5] * mask, 2, 0)
        extra.append((e + pltpu.roll(e, 3, 0), zeros))
    to_spectrum(extra, 3)
    for k in range(n):
        rows = slice(SUBS * k, SUBS * (k + 1))
        t = [k_ref[i, k] for i in range(6)]
        d = [kx_ref[i, k] for i in range(3)]
        for half in range(2):
            lanes = slice(128 * half, 128 * (half + 1))
            a, b, g = (s_ref[c, rows, lanes] for c in range(3))
            s_ref[0, rows, lanes] = t[0] * a + t[3] * b + t[4] * g
            s_ref[1, rows, lanes] = t[3] * a + t[1] * b + t[5] * g
            s_ref[2, rows, lanes] = t[4] * a + t[5] * b + t[2] * g
            e = s_ref[3, rows, lanes]
            s_ref[3, rows, lanes] = (
                d[0] * e + d[1] * pltpu.roll(e, 7, 0) + d[2] * pltpu.roll(e, 6, 0)
            )
    extra = from_spectrum(3)
    for c in range(plan.comps):
        values = from_spectrum(c)
        for s in range(n):
            e = extra[s][0]
            if c:
                e = pltpu.roll(e, SUBS - c, 0)
            out_ref[s, 2 * c] = values[s][0]
            out_ref[s, 2 * c + 1] = values[s][1] * keep + e * mask


def finish_kernel(plan, field_ref, m_ref, applied_ref, pred_ref, torque_ref):
    tiles = plan.lx * plan.ly // LANES
    for t in range(tiles):
        h, m = [], []
        for c in range(3):
            at = (c * tiles + t) * LANES
            h.append(field_ref[:, at : at + LANES].T + applied_ref[c])
            m.append(m_ref[c * tiles + t])
        a = [m[1] * h[2] - m[2] * h[1], m[2] * h[0] - m[0] * h[2], m[0] * h[1] - m[1] * h[0]]
        b = [m[1] * a[2] - m[2] * a[1], m[2] * a[0] - m[0] * a[2], m[0] * a[1] - m[1] * a[0]]
        scale = -1.0 / (1.0 + damping * damping)
        torque = [(a[c] + damping * b[c]) * scale for c in range(3)]
        step = [m[c] + time_step * torque[c] for c in range(3)]
        total = step[0] * step[0] + step[1] * step[1] + step[2] * step[2]
        inverse = 1.0 / jnp.sqrt(total)
        for c in range(3):
            torque_ref[c * tiles + t] = torque[c]
            pred_ref[c * tiles + t] = step[c] * inverse


def lattice_eigen(wave_index, length):
    return 2.0 * jnp.cos(wave_index.astype(jnp.float32) * (2.0 * math.pi / length)) - 2.0


def field_tensor(plan, kernel):
    gx, gy, gz = (lax.axis_index(a) for a in ("gx", "gy", "gz"))
    group = gx * plan.cz + gz
    kzs = kernel.shape[2]
    kt = jnp.swapaxes(kernel, 2, 3)
    ky = 4 * group + jnp.arange(4)
    packed = jnp.where((ky <= plan.ny // 2)[None, :, None, None], kt[:, :, 0:1], kt[:, :, 32:33])
    cols = [
        jnp.concatenate([packed, kt[:, :, 1:8]], 2),
        jnp.concatenate([kt[:, :, 16:24]], 2),
        jnp.concatenate([kt[:, :, 8:9], kt[:, :, 33:40]], 2),
        jnp.concatenate([kt[:, :, 24:25], kt[:, :, 49:56]], 2),
    ]
    send = jnp.stack([jnp.stack(cols[0:2], 2), jnp.stack(cols[2:4], 2)])
    edge = jnp.stack([kt[:, 0, 32]] * 2)
    rows = send.reshape(2, 6 * 4 * 2 * 8, kzs)
    rows = jnp.concatenate([rows, edge], 1)
    got = lax.all_to_all(rows, "gy", split_axis=0, concat_axis=0, tiled=True)
    main = got[:, : 6 * 4 * 2 * 8].reshape(2, 6, 2, 2, 2, 8, kzs // 32, 32)
    main = jnp.transpose(main, (1, 7, 3, 4, 2, 5, 0, 6)).reshape(6, 32, 8, 128)
    edge = got[:, 6 * 4 * 2 * 8 :].reshape(2, 6, kzs // 32, 32)
    edge = jnp.transpose(edge, (1, 3, 0, 2)).reshape(6, 32, plan.zc)
    kz = jnp.arange(plan.nz).reshape(plan.zc, 32).T
    table = np.array([[slot_kx(plan, k2, s) for s in range(SLOTS)] for k2 in range(4)])
    kx = jnp.asarray(table.reshape(2, 2, SLOTS), jnp.int32)[gy]
    kyq = (4 * group + 2 * jnp.arange(2)[None, :] + jnp.arange(2)[:, None])
    kx_full = jnp.broadcast_to(kx[None, :, None, :], (2, 2, 2, SLOTS))
    swap = (gy == 0) & (kyq > plan.ny // 2)
    is_packed = (jnp.arange(2)[None, :, None, None] == 0) & (jnp.arange(SLOTS) == 0)
    kx_full = jnp.where(is_packed & swap[:, None, :, None], 32, kx_full)
    ex = lattice_eigen(kx_full, plan.nx)
    ey = lattice_eigen(kyq, plan.ny)
    ez = lattice_eigen(kz, plan.nz)
    plane = (ex + ey[:, None, :, None]).reshape(8, SLOTS)
    eig = plane[None, :, :, None] + ez[:, None, None, :]
    eig = eig.reshape(32, 8, 128)
    scale = 1.0 / (plan.nx * plan.ny * plan.nz)
    diag = jnp.asarray([1, 1, 1, 0, 0, 0], jnp.float32)[:, None, None, None]
    tensor = scale * (exchange_coeff * diag * eig[None] - main)
    edge_eig = lattice_eigen(jnp.asarray(32), plan.nx) + lattice_eigen(4 * group, plan.ny) + ez
    edge = scale * (exchange_coeff * diag[:, :, :, 0] * edge_eig[None] - edge)
    order = np.array([[0, 1, 2], [3, 5, 4], [4, 3, 5]])
    edge = edge[order]
    edge = jnp.transpose(edge, (0, 2, 1, 3))
    edge = jnp.pad(edge, ((0, 0), (0, 0), (0, 5), (0, LANES - plan.zc)))
    special = (gy == 0) & ((group == 0) | (group == plan.groups // 2))
    spot = (jnp.arange(8)[:, None] == 0) & (jnp.arange(LANES)[None, :] < plan.zc)
    mask = jnp.where(special & spot, 1.0, 0.0).astype(jnp.float32)
    return tensor, edge, mask


def call(body, outs, scratch=(), name=None, smem=()):
    def run(*args):
        specs = [
            pl.BlockSpec(memory_space=pltpu.SMEM if i in smem else pltpu.VMEM)
            for i in range(len(args))
        ]
        return pl.pallas_call(
            body,
            out_shape=outs,
            in_specs=specs,
            out_specs=jax.tree.map(lambda _: pl.BlockSpec(memory_space=pltpu.VMEM), outs),
            scratch_shapes=list(scratch),
            name=name,
            compiler_params=pltpu.CompilerParams(vmem_limit_bytes=56 * 2**20),
        )(*args)

    return run


def fast_shards(plan, magnetization, kernel, applied):
    f32 = jnp.float32
    sds = jax.ShapeDtypeStruct
    n, zc = plan.devices, plan.zc
    width = 3 * plan.lx * plan.ly
    tiles = width // LANES
    fwd, back = xy_tables(plan)
    tw = x_twiddles(plan)
    ztw, zf, zb = z_tables(plan)
    m_tiles = magnetization.reshape(tiles, LANES, LANES)
    tensor, edge, mask = field_tensor(plan, kernel)
    packed = call(pack_kernel, sds((plan.lz, width), f32), name="pack")(m_tiles)
    lines = lax.all_to_all(
        packed.reshape(plan.planes, zc, width), ("gx", "gy"), split_axis=0, concat_axis=0, tiled=True
    )
    spec = call(
        lambda *a: xy_forward_kernel(plan, *a),
        sds((n, 6, SUBS, LANES), f32),
        [pltpu.VMEM((2, 128, 512), f32)],
        name="xy_forward",
    )(lines, fwd, tw)
    spec = lax.all_to_all(spec, ("gz", "gx", "gy"), split_axis=0, concat_axis=0, tiled=True)
    spec = call(
        lambda *a: z_kernel(plan, *a),
        sds((n, 6, SUBS, LANES), f32),
        [pltpu.VMEM((4, n * SUBS, 256), f32)],
        name="z_step",
    )(spec, tensor, edge, mask, ztw, zf, zb)
    spec = lax.all_to_all(spec, ("gz", "gx", "gy"), split_axis=0, concat_axis=0, tiled=True)
    field = call(
        lambda *a: xy_inverse_kernel(plan, *a),
        sds((plan.planes, zc, width), f32),
        [pltpu.VMEM((2, 256, 128), f32)],
        name="xy_inverse",
    )(spec, back, tw)
    field = lax.all_to_all(field, ("gx", "gy"), split_axis=0, concat_axis=0, tiled=True)
    pred, torque = call(
        lambda *a: finish_kernel(plan, *a),
        (sds(m_tiles.shape, f32), sds(m_tiles.shape, f32)),
        name="finish",
        smem=(2,),
    )(field.reshape(plan.lz, width), m_tiles, applied)
    return pred.reshape(magnetization.shape), torque.reshape(magnetization.shape)


def solution(mesh):
    sizes = mesh.shape

    def shards(magnetization, kernel, applied):
        plan = Plan(sizes["gx"], sizes["gy"], sizes["gz"], magnetization.shape)
        if plan.fits():
            return fast_shards(plan, magnetization, kernel, applied)
        return general_shards(magnetization, kernel, applied)

    return jax.shard_map(
        shards,
        mesh=mesh,
        in_specs=(P(None, "gx", "gy", "gz"), P(None, ("gx", "gz"), "gy", None), P()),
        out_specs=(P(None, "gx", "gy", "gz"), P(None, "gx", "gy", "gz")),
        check_vma=False,
    )
```

```python
import math

import jax
import jax.numpy as jnp
import numpy as np
from jax import lax
from jax.experimental import pallas as pl
from jax.experimental.pallas import tpu as pltpu
from jax.sharding import PartitionSpec as P

exchange_coeff = 1.0
damping = 0.3
time_step = 0.2
highest = lax.Precision.HIGHEST
LANES = 128
SUBS = 8
SLOTS = 8


def phase_table(row_index, col_index, length):
    product = row_index[:, None] * col_index[None, :] % length
    angles = product.astype(jnp.float32) * (2.0 * math.pi / length)
    return (jnp.cos(angles), jnp.sin(angles))


def forward_mix(real_part, imag_part, cosine_table, sine_table, pattern):
    real_out = jnp.einsum(pattern, real_part, cosine_table, precision=highest) + jnp.einsum(
        pattern, imag_part, sine_table, precision=highest
    )
    imag_out = jnp.einsum(pattern, imag_part, cosine_table, precision=highest) - jnp.einsum(
        pattern, real_part, sine_table, precision=highest
    )
    return (real_out, imag_out)


def inverse_mix(real_part, imag_part, cosine_table, sine_table, pattern):
    real_out = jnp.einsum(pattern, real_part, cosine_table, precision=highest) - jnp.einsum(
        pattern, imag_part, sine_table, precision=highest
    )
    imag_out = jnp.einsum(pattern, imag_part, cosine_table, precision=highest) + jnp.einsum(
        pattern, real_part, sine_table, precision=highest
    )
    return (real_out, imag_out)


def apply_tensor(kernel, spectrum):
    return jnp.stack(
        [
            kernel[0] * spectrum[0] + kernel[3] * spectrum[1] + kernel[4] * spectrum[2],
            kernel[3] * spectrum[0] + kernel[1] * spectrum[1] + kernel[5] * spectrum[2],
            kernel[4] * spectrum[0] + kernel[5] * spectrum[1] + kernel[2] * spectrum[2],
        ]
    )


def cross_product(first_vec, second_vec):
    return jnp.stack(
        [
            first_vec[1] * second_vec[2] - first_vec[2] * second_vec[1],
            first_vec[2] * second_vec[0] - first_vec[0] * second_vec[2],
            first_vec[0] * second_vec[1] - first_vec[1] * second_vec[0],
        ]
    )


def general_shards(magnetization, kernel, applied):
    count_gx = lax.axis_size("gx")
    count_gy = lax.axis_size("gy")
    count_gz = lax.axis_size("gz")
    local_x = magnetization.shape[1]
    local_y = magnetization.shape[2]
    local_z = magnetization.shape[3]
    full_x = local_x * count_gx
    full_y = local_y * count_gy
    full_z = local_z * count_gz
    part_x = local_x // count_gz
    part_y = full_y // (count_gx * count_gz)
    part_z = full_z // count_gy
    outside = applied[:, None, None, None]
    z_index = jnp.arange(full_z, dtype=jnp.int32)
    weights = jnp.ones((full_z,), jnp.float32)
    planes = z_index.shape[0] // count_gy
    wave_count = z_index.shape[0]
    zlines = lax.all_to_all(magnetization, "gz", split_axis=1, concat_axis=3, tiled=True)
    cos_zf, sin_zf = phase_table(z_index, z_index, full_z)
    cos_zb, sin_zb = phase_table(z_index, z_index, full_z)
    cos_zb = cos_zb * weights[:, None]
    sin_zb = sin_zb * weights[:, None]
    lines_shape = (3, part_x, local_y, full_z)
    wave_shape = (3, part_x, local_y, wave_count)
    z_rows = zlines.reshape(-1, full_z)
    spec_real = jnp.dot(z_rows, cos_zf, precision=highest).reshape(wave_shape)
    spec_imag = -jnp.dot(z_rows, sin_zf, precision=highest).reshape(wave_shape)
    spec_real, spec_imag = (
        lax.all_to_all(spec_real, "gy", split_axis=3, concat_axis=2, tiled=True),
        lax.all_to_all(spec_imag, "gy", split_axis=3, concat_axis=2, tiled=True),
    )
    y_index = jnp.arange(full_y, dtype=jnp.int32)
    cos_y, sin_y = phase_table(y_index, y_index, full_y)
    spec_real, spec_imag = forward_mix(spec_real, spec_imag, cos_y, sin_y, "cxyz,yk->ckxz")
    x_index = jnp.arange(full_x, dtype=jnp.int32)
    cos_xn, sin_xn = phase_table(x_index, x_index, full_x)
    spec_real, spec_imag = (
        lax.all_to_all(spec_real, ("gx", "gz"), split_axis=1, concat_axis=2, tiled=True),
        lax.all_to_all(spec_imag, ("gx", "gz"), split_axis=1, concat_axis=2, tiled=True),
    )
    cos_x, sin_x = (cos_xn, sin_xn)
    spec_real, spec_imag = forward_mix(spec_real, spec_imag, cos_x, sin_x, "cyxz,xk->cyzk")
    inverse_count = 1.0 / (full_x * full_y * full_z)
    out_real = -inverse_count * apply_tensor(kernel, spec_real)
    out_imag = -inverse_count * apply_tensor(kernel, spec_imag)
    wave_y = (lax.axis_index("gx") * count_gz + lax.axis_index("gz")) * part_y + jnp.arange(
        part_y, dtype=jnp.int32
    )
    wave_z = lax.axis_index("gy") * part_z + jnp.arange(planes, dtype=jnp.int32)
    eigenvalue = (
        lattice_eigen(wave_y, full_y)[:, None, None]
        + lattice_eigen(wave_z, full_z)[None, :, None]
        + lattice_eigen(x_index, full_x)[None, None, :]
    )
    factor = inverse_count * exchange_coeff * eigenvalue
    out_real = out_real + factor * spec_real
    out_imag = out_imag + factor * spec_imag
    back_real, back_imag = inverse_mix(out_real, out_imag, cos_xn, sin_xn, "cyzk,kx->cyxz")
    back_real, back_imag = (
        lax.all_to_all(back_real, ("gx", "gz"), split_axis=2, concat_axis=1, tiled=True),
        lax.all_to_all(back_imag, ("gx", "gz"), split_axis=2, concat_axis=1, tiled=True),
    )
    cos_yb, sin_yb = (cos_y, sin_y)
    back_real, back_imag = inverse_mix(back_real, back_imag, cos_yb, sin_yb, "cyxz,yn->cxnz")
    back_real, back_imag = (
        lax.all_to_all(back_real, "gy", split_axis=2, concat_axis=3, tiled=True),
        lax.all_to_all(back_imag, "gy", split_axis=2, concat_axis=3, tiled=True),
    )
    real_rows = back_real.reshape(-1, wave_count)
    imag_rows = back_imag.reshape(-1, wave_count)
    field_lines = (
        jnp.dot(real_rows, cos_zb, precision=highest)
        - jnp.dot(imag_rows, sin_zb, precision=highest)
    ).reshape(lines_shape)
    field_block = lax.all_to_all(field_lines, "gz", split_axis=3, concat_axis=1, tiled=True)
    total_field = field_block + outside
    precess = cross_product(magnetization, total_field)
    double_twist = cross_product(magnetization, precess)
    torque = -(precess + damping * double_twist) / (1.0 + damping * damping)
    stepped = magnetization + time_step * torque
    length = jnp.sqrt(jnp.sum(stepped * stepped, axis=0))
    return (stepped / length, torque)


def cmul_const(value, angle):
    re, im = value
    quarter = angle / (math.pi / 2)
    if abs(quarter - round(quarter)) < 1e-9:
        turn = round(quarter) % 4
        if turn == 0:
            return (re, im)
        if turn == 1:
            return (-im, re)
        if turn == 2:
            return (-re, -im)
        return (im, -re)
    c, s = math.cos(angle), math.sin(angle)
    if abs(abs(c) - abs(s)) < 1e-9:
        h = abs(c)
        sc, ss = math.copysign(1, c), math.copysign(1, s)
        first = re if sc > 0 else -re
        out_re = (first - im) if ss > 0 else (first + im)
        second = im if sc > 0 else -im
        out_im = (second + re) if ss > 0 else (second - re)
        return (h * out_re, h * out_im)
    return (c * re - s * im, c * im + s * re)


def cadd(a, b):
    return (a[0] + b[0], a[1] + b[1])


def csub(a, b):
    return (a[0] - b[0], a[1] - b[1])


def conj(a):
    return (a[0], -a[1])


def complex_fft(values, sign):
    n = len(values)
    if n == 1:
        return values
    even = complex_fft(values[0::2], sign)
    odd = complex_fft(values[1::2], sign)
    odd = [cmul_const(v, sign * 2 * math.pi * k / n) for k, v in enumerate(odd)]
    return [cadd(e, o) for e, o in zip(even, odd)] + [csub(e, o) for e, o in zip(even, odd)]


def real_fft(values):
    n = len(values)
    if n == 2:
        return [values[0] + values[1], values[0] - values[1]]
    even = real_fft(values[0::2])
    odd = real_fft(values[1::2])
    quarter = n // 4
    out = [None] * (n // 2 + 1)
    out[0] = even[0] + odd[0]
    out[n // 2] = even[0] - odd[0]
    for k in range(1, quarter):
        turned = cmul_const(odd[k], -2 * math.pi * k / n)
        out[k] = cadd(even[k], turned)
        out[n // 2 - k] = conj(csub(even[k], turned))
    out[quarter] = (even[quarter], -odd[quarter])
    return out


def real_ifft(values):
    n = 2 * (len(values) - 1)
    if n == 2:
        return [values[0] + values[1], values[0] - values[1]]
    quarter = n // 4
    even = [None] * (quarter + 1)
    odd = [None] * (quarter + 1)
    even[0] = values[0] + values[n // 2]
    odd[0] = values[0] - values[n // 2]
    for k in range(1, quarter):
        mirror = conj(values[n // 2 - k])
        even[k] = cadd(values[k], mirror)
        odd[k] = cmul_const(csub(values[k], mirror), 2 * math.pi * k / n)
    mid = values[quarter]
    even[quarter] = 2.0 * mid[0]
    odd[quarter] = -2.0 * mid[1]
    even = real_ifft(even)
    odd = real_ifft(odd)
    out = [None] * n
    out[0::2] = even
    out[1::2] = odd
    return out


def split(value):
    high = value.astype(jnp.bfloat16)
    return high, (value - high.astype(jnp.float32)).astype(jnp.bfloat16)


def split_table(table, axis):
    high = table.astype(jnp.bfloat16)
    low = (table - high.astype(np.float32)).astype(jnp.bfloat16)
    return np.concatenate([high, low, high], axis)


def mm(a, b, dims):
    return lax.dot_general(a, b, (dims, ((), ())), preferred_element_type=jnp.float32)


class Plan:
    def __init__(self, cx, cy, cz, shape):
        comps, lx, ly, lz = shape
        self.comps, self.lx, self.ly, self.lz = comps, lx, ly, lz
        self.cx, self.cy, self.cz = cx, cy, cz
        self.nx, self.ny, self.nz = lx * cx, ly * cy, lz * cz
        self.planes = cx * cy
        self.groups = cx * cz
        self.devices = cx * cy * cz

    def fits(self):
        if self.devices % 1 or self.lz % self.planes:
            return False
        self.zc = self.lz // self.planes
        self.xl = LANES // self.ly if LANES % self.ly == 0 else 0
        return (
            self.comps == 3
            and self.xl == 4
            and self.cy == 2
            and self.nx == 16 * self.xl
            and self.lx % self.xl == 0
            and self.ly == 2 * self.groups
            and self.zc * SLOTS == LANES
            and self.lz == LANES
            and self.nz % self.zc == 0
        )


def slot_kx(plan, kx2, slot):
    if slot:
        return slot + 16 * kx2
    return (0, 16, 8, 24)[kx2]


def xy_tables(plan):
    lane = np.arange(LANES)
    xl, yl = lane // plan.ly, lane % plan.ly
    half = plan.ny // 2
    fwd = np.zeros((2, 256, 512))
    back = np.zeros((2, 256, 512))
    for r in range(2):
        for k2h in range(2):
            for g in range(plan.groups):
                for ri in range(2):
                    for k2l in range(2):
                        for ql in range(2):
                            block = ri if r == 0 else 1 - ri
                            f = (k2h * plan.groups + g) * 8 + block * 4 + k2l * 2 + ql
                            kx2 = 2 * k2h + k2l
                            ky = 2 * (2 * g + ql) + r
                            ph = 2 * math.pi * (xl * kx2 / 4 + yl * ky / plan.ny)
                            c, s = np.cos(ph), np.sin(ph)
                            if ri == 0:
                                fwd[r, f, 0:128], fwd[r, f, 128:256] = c, s
                                back[r, f, 0:128], back[r, f, 128:256] = c, s
                            else:
                                fwd[r, f, 0:128], fwd[r, f, 128:256] = -s, c
                                back[r, f, 0:128], back[r, f, 128:256] = -s, c
                            kx = slot_kx(plan, kx2, 0)
                            if kx2 == 0:
                                edge = ky in (0, half)
                                if edge:
                                    kx = 0 if ri == 0 else 32
                                else:
                                    kx = 0 if ky < half else 32
                            ph = 2 * math.pi * (xl * kx / plan.nx + yl * ky / plan.ny)
                            c, s = np.cos(ph), np.sin(ph)
                            at = 256 if kx % 16 == 0 else 384
                            if kx2 == 0 and edge:
                                fwd[r, f, at : at + 128] = c
                                back[r, f, at : at + 128] = c
                            else:
                                fwd[r, f, at : at + 128] = c if ri == 0 else -s
                                back[r, f, at : at + 128] = 2 * (c if ri == 0 else -s)
    return fwd.astype(np.float32), back.astype(np.float32)


def x_twiddles(plan):
    xl = np.arange(LANES) // plan.ly
    ph = 2 * math.pi * np.arange(SLOTS)[:, None] * xl[None, :] / plan.nx
    return np.stack([np.cos(ph), np.sin(ph)]).astype(np.float32)


def z_tables(plan):
    zc, nz = plan.zc, plan.nz
    lane = np.arange(LANES) % zc
    ph = 2 * math.pi * np.arange(plan.devices)[:, None] * lane[None, :] / nz
    twiddle = np.stack([np.cos(ph), np.sin(ph)]).astype(np.float32)
    small = 2 * math.pi * np.arange(zc)[:, None] * np.arange(zc)[None, :] / zc
    c = np.kron(np.eye(SLOTS), np.cos(small))
    s = np.kron(np.eye(SLOTS), np.sin(small))
    fwd = np.block([[c, -s], [s, c]]).astype(np.float32)
    back = np.block([[c, s], [-s, c]]).astype(np.float32)
    return twiddle, fwd, back


def pack_kernel(m_ref, out_ref):
    for t in range(m_ref.shape[0]):
        out_ref[:, LANES * t : LANES * (t + 1)] = m_ref[t].T


def xy_forward_kernel(plan, lines_ref, table_ref, edge_ref, tw_ref, out_ref, g_ref, e_ref):
    zc = plan.zc
    per = plan.lx // plan.xl
    low = lax.broadcasted_iota(jnp.int32, (SUBS, LANES), 0) < 4
    first_slot = lax.broadcasted_iota(jnp.int32, (SUBS, LANES), 1) < zc
    blank = jnp.zeros((zc, LANES), jnp.bfloat16)
    for r in range(2):
        for k in range(plan.comps, SLOTS):
            for q in range(4):
                e_ref[r, zc * k : zc * (k + 1), LANES * q : LANES * (q + 1)] = blank

    def keep(ref, at, rows, parts):
        for q, part in enumerate(parts):
            hi, lo = split(part)
            ref[(*at, rows, slice(LANES * q, LANES * (q + 1)))] = hi
            ref[(*at, rows, slice(LANES * (q + 2), LANES * (q + 3)))] = lo

    for c in range(plan.comps):
        parts = [[], []]
        for gx in range(plan.cx):
            for xh in range(per):
                at = c * (plan.lx * plan.ly) + xh * LANES
                first = lines_ref[gx * 2, :, at : at + LANES]
                second = lines_ref[gx * 2 + 1, :, at : at + LANES]
                parts[0].append(first + second)
                parts[1].append(first - second)
        for r in range(2):
            spec = real_fft(parts[r])
            keep(e_ref, (r,), slice(zc * c, zc * (c + 1)), (spec[0], spec[8]))
            for k in range(1, SLOTS):
                re, im = spec[k]
                tc = tw_ref[0, k : k + 1, :]
                ts = tw_ref[1, k : k + 1, :]
                rows = slice(zc * k, zc * (k + 1))
                keep(g_ref, (r, c), rows, (re * tc + im * ts, im * tc - re * ts))
            g_ref[r, c, 0:zc, :] = jnp.zeros((zc, 512), jnp.bfloat16)

    def widen(value):
        return jnp.concatenate([value[:, 0:256], value[:, 0:256], value[:, 256:512]], 1)

    edges = [mm(edge_ref[r], widen(e_ref[r]), ((1,), (1,))) for r in range(2)]
    for c in range(plan.comps):
        outs = [mm(table_ref[r], widen(g_ref[r, c]), ((1,), (1,))) for r in range(2)]
        for k2h in range(2):
            for g in range(plan.groups):
                f = (k2h * plan.groups + g) * SUBS
                both = []
                for r in range(2):
                    edge = edges[r][f : f + SUBS]
                    if c:
                        edge = pltpu.roll(edge, LANES - zc * c, 1)
                    both.append(jnp.where(first_slot, edge, outs[r][f : f + SUBS]))
                one, two = both
                gx, gz = g // plan.cz, g % plan.cz
                dest = gz * plan.planes + gx * plan.cy + k2h
                out_ref[dest, 2 * c] = jnp.where(low, one, two)
                out_ref[dest, 2 * c + 1] = pltpu.roll(jnp.where(low, two, one), 4, 0)


def xy_inverse_kernel(plan, spec_ref, table_ref, edge_ref, tw_ref, out_ref, h_ref, t_ref, u_ref):
    zc = plan.zc
    per = plan.lx // plan.xl
    low = lax.broadcasted_iota(jnp.int32, (SUBS, LANES), 0) < 4
    for c in range(plan.comps):
        for k2h in range(2):
            for g in range(plan.groups):
                f = (k2h * plan.groups + g) * SUBS
                gx, gz = g // plan.cz, g % plan.cz
                src = gz * plan.planes + gx * plan.cy + k2h
                re = spec_ref[src, 2 * c]
                im = pltpu.roll(spec_ref[src, 2 * c + 1], 4, 0)
                h_ref[c, 0, f : f + SUBS, :] = jnp.where(low, re, im)
                h_ref[c, 1, f : f + SUBS, :] = jnp.where(low, im, re)
        for r in range(2):
            hi, lo = split(h_ref[c, r].T)
            t_ref[r, LANES * c : LANES * (c + 1), 0:256] = hi
            t_ref[r, LANES * c : LANES * (c + 1), 256:512] = lo

    def widen(value):
        return jnp.concatenate([value[:, 0:256], value[:, 0:256], value[:, 256:512]], 1)

    edges = []
    for r in range(2):
        u_ref[r] = mm(widen(t_ref[r]), table_ref[r], ((1,), (0,)))
        rows = jnp.concatenate(
            [t_ref[r, LANES * c : LANES * c + zc, :] for c in range(plan.comps)], 0
        )
        edges.append(mm(widen(rows), edge_ref[r], ((1,), (0,))))
    for c in range(plan.comps):
        fields = []
        for r in range(2):
            edge = edges[r][zc * c : zc * (c + 1)]
            values = [edge[:, 0:128]]
            for k in range(1, SLOTS):
                rows = slice(LANES * c + zc * k, LANES * c + zc * (k + 1))
                re = u_ref[r, rows, 0:128]
                im = u_ref[r, rows, 128:256]
                tc = tw_ref[0, k : k + 1, :]
                ts = tw_ref[1, k : k + 1, :]
                values.append((re * tc - im * ts, im * tc + re * ts))
            values.append(edge[:, 128:256])
            fields.append(real_ifft(values))
        for gx in range(plan.cx):
            for xh in range(per):
                at = c * (plan.lx * plan.ly) + xh * LANES
                one = fields[0][gx * per + xh]
                two = fields[1][gx * per + xh]
                out_ref[gx * 2, :, at : at + LANES] = one + two
                out_ref[gx * 2 + 1, :, at : at + LANES] = one - two


def z_kernel(plan, in_ref, k_ref, kx_ref, mask_ref, tw_ref, fwd_ref, back_ref, out_ref, s_ref, b_ref):
    n = plan.devices
    half = n // 2 + 1
    mask = mask_ref[...]
    keep = 1.0 - mask

    def transform(at, count, table):
        hi, lo = split(s_ref[at, 0 : SUBS * count, :])
        wide = jnp.concatenate([hi, hi, lo], 1)
        s_ref[at, 0 : SUBS * count, :] = mm(wide, table[...], ((1,), (0,)))

    def to_spectrum(values, at):
        for k, (re, im) in enumerate(values):
            tc = tw_ref[0, k : k + 1, :]
            ts = tw_ref[1, k : k + 1, :]
            s_ref[at, SUBS * k : SUBS * (k + 1), 0:128] = re * tc + im * ts
            s_ref[at, SUBS * k : SUBS * (k + 1), 128:256] = im * tc - re * ts
        transform(at, len(values), fwd_ref)

    def from_spectrum(at, count):
        transform(at, count, back_ref)
        values = []
        for k in range(count):
            re = s_ref[at, SUBS * k : SUBS * (k + 1), 0:128]
            im = s_ref[at, SUBS * k : SUBS * (k + 1), 128:256]
            tc = tw_ref[0, k : k + 1, :]
            ts = tw_ref[1, k : k + 1, :]
            values.append((re * tc - im * ts, im * tc + re * ts))
        return values

    extra = []
    for s in range(n):
        e = in_ref[s, 1] * mask
        e = e + pltpu.roll(in_ref[s, 3] * mask, 1, 0)
        e = e + pltpu.roll(in_ref[s, 5] * mask, 2, 0)
        extra.append(e + pltpu.roll(e, 3, 0))
    extra = real_fft(extra)
    zero = jnp.zeros((SUBS, LANES), jnp.float32)
    extra[0] = (extra[0], zero)
    extra[-1] = (extra[-1], zero)
    to_spectrum(extra, 3)
    for c in range(plan.comps):
        values = [(in_ref[s, 2 * c], in_ref[s, 2 * c + 1] * keep) for s in range(n)]
        to_spectrum(complex_fft(values, -1), c)
    for k in range(n):
        rows = slice(SUBS * k, SUBS * (k + 1))
        t = [k_ref[i, k] for i in range(6)]
        for part in range(2):
            lanes = slice(LANES * part, LANES * (part + 1))
            a, b, g = (s_ref[c, rows, lanes] for c in range(3))
            s_ref[0, rows, lanes] = t[0] * a + t[3] * b + t[4] * g
            s_ref[1, rows, lanes] = t[3] * a + t[1] * b + t[5] * g
            s_ref[2, rows, lanes] = t[4] * a + t[5] * b + t[2] * g
            if k < half:
                d = [kx_ref[i, k] for i in range(3)]
                e = s_ref[3, rows, lanes]
                s_ref[3, rows, lanes] = (
                    d[0] * e + d[1] * pltpu.roll(e, 7, 0) + d[2] * pltpu.roll(e, 6, 0)
                )
    extra = from_spectrum(3, half)
    extra[0] = extra[0][0]
    extra[-1] = extra[-1][0]
    extra = real_ifft(extra)
    for s in range(n):
        b_ref[s] = extra[s]
    for c in range(plan.comps):
        values = complex_fft(from_spectrum(c, n), 1)
        for s in range(n):
            e = b_ref[s]
            if c:
                e = pltpu.roll(e, SUBS - c, 0)
            out_ref[s, 2 * c] = values[s][0]
            out_ref[s, 2 * c + 1] = values[s][1] * keep + e * mask


def finish_kernel(plan, field_ref, m_ref, applied_ref, pred_ref, torque_ref):
    tiles = plan.lx * plan.ly // LANES
    for t in range(tiles):
        h, m = [], []
        for c in range(3):
            at = (c * tiles + t) * LANES
            h.append(field_ref[:, at : at + LANES].T + applied_ref[c])
            m.append(m_ref[c * tiles + t])
        a = [m[1] * h[2] - m[2] * h[1], m[2] * h[0] - m[0] * h[2], m[0] * h[1] - m[1] * h[0]]
        b = [m[1] * a[2] - m[2] * a[1], m[2] * a[0] - m[0] * a[2], m[0] * a[1] - m[1] * a[0]]
        scale = -1.0 / (1.0 + damping * damping)
        torque = [(a[c] + damping * b[c]) * scale for c in range(3)]
        step = [m[c] + time_step * torque[c] for c in range(3)]
        total = step[0] * step[0] + step[1] * step[1] + step[2] * step[2]
        inverse = lax.rsqrt(total)
        for c in range(3):
            torque_ref[c * tiles + t] = torque[c]
            pred_ref[c * tiles + t] = step[c] * inverse


def lattice_eigen(wave_index, length):
    return 2.0 * jnp.cos(wave_index.astype(jnp.float32) * (2.0 * math.pi / length)) - 2.0


def tensor_rows(plan, kernel):
    gx, gz = (lax.axis_index(a) for a in ("gx", "gz"))
    group = gx * plan.cz + gz
    kzs = kernel.shape[2]
    kt = jnp.swapaxes(kernel, 2, 3)
    ky = 4 * group + jnp.arange(4)
    packed = jnp.where((ky <= plan.ny // 2)[None, :, None, None], kt[:, :, 0:1], kt[:, :, 32:33])
    cols = [
        jnp.concatenate([packed, kt[:, :, 1:8]], 2),
        jnp.concatenate([kt[:, :, 16:24]], 2),
        jnp.concatenate([kt[:, :, 8:9], kt[:, :, 33:40]], 2),
        jnp.concatenate([kt[:, :, 24:25], kt[:, :, 49:56]], 2),
    ]
    send = jnp.stack([jnp.stack(cols[0:2], 2), jnp.stack(cols[2:4], 2)])
    edge = jnp.stack([kt[:, 0, 32]] * 2)
    rows = send.reshape(2, 6 * 4 * 2 * 8, kzs)
    return jnp.concatenate([rows, edge], 1)


def field_tensor(plan, rows):
    gx, gy, gz = (lax.axis_index(a) for a in ("gx", "gy", "gz"))
    group = gx * plan.cz + gz
    kzs = rows.shape[2]
    own = lax.dynamic_index_in_dim(rows, gy, 0)
    other = lax.dynamic_index_in_dim(rows, 1 - gy, 0)
    other = lax.ppermute(other, "gy", [(0, 1), (1, 0)])
    got = jnp.where(gy == 0, jnp.concatenate([own, other]), jnp.concatenate([other, own]))
    main = got[:, : 6 * 4 * 2 * 8].reshape(2, 6, 2, 2, 2, 8, kzs // 32, 32)
    main = jnp.transpose(main, (1, 7, 3, 4, 2, 5, 0, 6)).reshape(6, 32, 8, 128)
    edge = got[:, 6 * 4 * 2 * 8 :].reshape(2, 6, kzs // 32, 32)
    edge = jnp.transpose(edge, (1, 3, 0, 2)).reshape(6, 32, plan.zc)
    kz = jnp.arange(plan.nz).reshape(plan.zc, 32).T
    table = np.array([[slot_kx(plan, k2, s) for s in range(SLOTS)] for k2 in range(4)])
    kx = jnp.asarray(table.reshape(2, 2, SLOTS), jnp.int32)[gy]
    kyq = (4 * group + 2 * jnp.arange(2)[None, :] + jnp.arange(2)[:, None])
    kx_full = jnp.broadcast_to(kx[None, :, None, :], (2, 2, 2, SLOTS))
    swap = (gy == 0) & (kyq > plan.ny // 2)
    is_packed = (jnp.arange(2)[None, :, None, None] == 0) & (jnp.arange(SLOTS) == 0)
    kx_full = jnp.where(is_packed & swap[:, None, :, None], 32, kx_full)
    ex = lattice_eigen(kx_full, plan.nx)
    ey = lattice_eigen(kyq, plan.ny)
    ez = lattice_eigen(kz, plan.nz)
    plane = (ex + ey[:, None, :, None]).reshape(8, SLOTS)
    eig = plane[None, :, :, None] + ez[:, None, None, :]
    eig = eig.reshape(32, 8, 128)
    scale = 1.0 / (plan.nx * plan.ny * plan.nz)
    diag = jnp.asarray([1, 1, 1, 0, 0, 0], jnp.float32)[:, None, None, None]
    tensor = scale * (exchange_coeff * diag * eig[None] - main)
    edge_eig = lattice_eigen(jnp.asarray(32), plan.nx) + lattice_eigen(4 * group, plan.ny) + ez
    edge = scale * (exchange_coeff * diag[:, :, :, 0] * edge_eig[None] - edge)
    order = np.array([[0, 1, 2], [3, 5, 4], [4, 3, 5]])
    edge = edge[order]
    edge = jnp.transpose(edge, (0, 2, 1, 3))
    edge = jnp.pad(edge, ((0, 0), (0, 0), (0, 5), (0, LANES - plan.zc)))
    special = (gy == 0) & ((group == 0) | (group == plan.groups // 2))
    spot = (jnp.arange(8)[:, None] == 0) & (jnp.arange(LANES)[None, :] < plan.zc)
    mask = jnp.where(special & spot, 1.0, 0.0).astype(jnp.float32)
    return tensor, edge, mask


def call(body, outs, scratch=(), name=None, smem=()):
    def run(*args):
        specs = [
            pl.BlockSpec(memory_space=pltpu.SMEM if i in smem else pltpu.VMEM)
            for i in range(len(args))
        ]
        return pl.pallas_call(
            body,
            out_shape=outs,
            in_specs=specs,
            out_specs=jax.tree.map(lambda _: pl.BlockSpec(memory_space=pltpu.VMEM), outs),
            scratch_shapes=list(scratch),
            name=name,
            compiler_params=pltpu.CompilerParams(vmem_limit_bytes=56 * 2**20),
        )(*args)

    return run


def fast_shards(plan, magnetization, kernel, applied):
    f32 = jnp.float32
    sds = jax.ShapeDtypeStruct
    n, zc = plan.devices, plan.zc
    width = 3 * plan.lx * plan.ly
    tiles = width // LANES
    fwd, back = xy_tables(plan)
    fwd = [split_table(t, 2) for t in (fwd[:, :, 0:256], fwd[:, :, 256:512])]
    back = [split_table(t, 1) for t in (back[:, :, 0:256], back[:, :, 256:512])]
    tw = x_twiddles(plan)
    ztw, zf, zb = z_tables(plan)
    zf, zb = split_table(zf, 0), split_table(zb, 0)
    m_tiles = magnetization.reshape(tiles, LANES, LANES)
    packed = call(pack_kernel, sds((plan.lz, width), f32), name="pack")(m_tiles)
    packed, kernel = lax.optimization_barrier((packed, kernel))
    tensor, edge, mask = field_tensor(plan, tensor_rows(plan, kernel))
    lines = lax.all_to_all(
        packed.reshape(plan.planes, zc, width), ("gx", "gy"), split_axis=0, concat_axis=0, tiled=True
    )
    spec = call(
        lambda *a: xy_forward_kernel(plan, *a),
        sds((n, 6, SUBS, LANES), f32),
        [pltpu.VMEM((2, 3, LANES, 512), jnp.bfloat16), pltpu.VMEM((2, LANES, 512), jnp.bfloat16)],
        name="xy_forward",
    )(lines, *fwd, tw)
    spec = lax.all_to_all(spec, ("gz", "gx", "gy"), split_axis=0, concat_axis=0, tiled=True)
    spec = call(
        lambda *a: z_kernel(plan, *a),
        sds((n, 6, SUBS, LANES), f32),
        [pltpu.VMEM((4, n * SUBS, 256), f32), pltpu.VMEM((n, SUBS, LANES), f32)],
        name="z_step",
    )(spec, tensor, edge, mask, ztw, zf, zb)
    spec = lax.all_to_all(spec, ("gz", "gx", "gy"), split_axis=0, concat_axis=0, tiled=True)
    field = call(
        lambda *a: xy_inverse_kernel(plan, *a),
        sds((plan.planes, zc, width), f32),
        [
            pltpu.VMEM((3, 2, 256, LANES), f32),
            pltpu.VMEM((2, 3 * LANES, 512), jnp.bfloat16),
            pltpu.VMEM((2, 3 * LANES, 256), f32),
        ],
        name="xy_inverse",
    )(spec, *back, tw)
    field = lax.all_to_all(field, ("gx", "gy"), split_axis=0, concat_axis=0, tiled=True)
    pred, torque = call(
        lambda *a: finish_kernel(plan, *a),
        (sds(m_tiles.shape, f32), sds(m_tiles.shape, f32)),
        name="finish",
        smem=(2,),
    )(field.reshape(plan.lz, width), m_tiles, applied)
    return pred.reshape(magnetization.shape), torque.reshape(magnetization.shape)


def solution(mesh):
    sizes = mesh.shape

    def shards(magnetization, kernel, applied):
        plan = Plan(sizes["gx"], sizes["gy"], sizes["gz"], magnetization.shape)
        if plan.fits():
            return fast_shards(plan, magnetization, kernel, applied)
        return general_shards(magnetization, kernel, applied)

    return jax.shard_map(
        shards,
        mesh=mesh,
        in_specs=(P(None, "gx", "gy", "gz"), P(None, ("gx", "gz"), "gy", None), P()),
        out_specs=(P(None, "gx", "gy", "gz"), P(None, "gx", "gy", "gz")),
        check_vma=False,
    )
```

```python
import math

import jax
import jax.numpy as jnp
import numpy as np
from jax import lax
from jax.experimental import pallas as pl
from jax.experimental.pallas import tpu as pltpu
from jax.sharding import PartitionSpec as P


exchange_coeff = 1.0
damping = 0.3
time_step = 0.2
highest = lax.Precision.HIGHEST
LANES = 128
SUBS = 8
SLOTS = 8


def phase_table(row_index, col_index, length):
    product = row_index[:, None] * col_index[None, :] % length
    angles = product.astype(jnp.float32) * (2.0 * math.pi / length)
    return (jnp.cos(angles), jnp.sin(angles))


def forward_mix(real_part, imag_part, cosine_table, sine_table, pattern):
    real_out = jnp.einsum(pattern, real_part, cosine_table, precision=highest) + jnp.einsum(
        pattern, imag_part, sine_table, precision=highest
    )
    imag_out = jnp.einsum(pattern, imag_part, cosine_table, precision=highest) - jnp.einsum(
        pattern, real_part, sine_table, precision=highest
    )
    return (real_out, imag_out)


def inverse_mix(real_part, imag_part, cosine_table, sine_table, pattern):
    real_out = jnp.einsum(pattern, real_part, cosine_table, precision=highest) - jnp.einsum(
        pattern, imag_part, sine_table, precision=highest
    )
    imag_out = jnp.einsum(pattern, imag_part, cosine_table, precision=highest) + jnp.einsum(
        pattern, real_part, sine_table, precision=highest
    )
    return (real_out, imag_out)


def apply_tensor(kernel, spectrum):
    return jnp.stack(
        [
            kernel[0] * spectrum[0] + kernel[3] * spectrum[1] + kernel[4] * spectrum[2],
            kernel[3] * spectrum[0] + kernel[1] * spectrum[1] + kernel[5] * spectrum[2],
            kernel[4] * spectrum[0] + kernel[5] * spectrum[1] + kernel[2] * spectrum[2],
        ]
    )


def cross_product(first_vec, second_vec):
    return jnp.stack(
        [
            first_vec[1] * second_vec[2] - first_vec[2] * second_vec[1],
            first_vec[2] * second_vec[0] - first_vec[0] * second_vec[2],
            first_vec[0] * second_vec[1] - first_vec[1] * second_vec[0],
        ]
    )


def general_shards(magnetization, kernel, applied):
    count_gx = lax.axis_size("gx")
    count_gy = lax.axis_size("gy")
    count_gz = lax.axis_size("gz")
    local_x = magnetization.shape[1]
    local_y = magnetization.shape[2]
    local_z = magnetization.shape[3]
    full_x = local_x * count_gx
    full_y = local_y * count_gy
    full_z = local_z * count_gz
    part_x = local_x // count_gz
    part_y = full_y // (count_gx * count_gz)
    part_z = full_z // count_gy
    outside = applied[:, None, None, None]
    z_index = jnp.arange(full_z, dtype=jnp.int32)
    weights = jnp.ones((full_z,), jnp.float32)
    planes = z_index.shape[0] // count_gy
    wave_count = z_index.shape[0]
    zlines = lax.all_to_all(magnetization, "gz", split_axis=1, concat_axis=3, tiled=True)
    cos_zf, sin_zf = phase_table(z_index, z_index, full_z)
    cos_zb, sin_zb = phase_table(z_index, z_index, full_z)
    cos_zb = cos_zb * weights[:, None]
    sin_zb = sin_zb * weights[:, None]
    lines_shape = (3, part_x, local_y, full_z)
    wave_shape = (3, part_x, local_y, wave_count)
    z_rows = zlines.reshape(-1, full_z)
    spec_real = jnp.dot(z_rows, cos_zf, precision=highest).reshape(wave_shape)
    spec_imag = -jnp.dot(z_rows, sin_zf, precision=highest).reshape(wave_shape)
    spec_real, spec_imag = (
        lax.all_to_all(spec_real, "gy", split_axis=3, concat_axis=2, tiled=True),
        lax.all_to_all(spec_imag, "gy", split_axis=3, concat_axis=2, tiled=True),
    )
    y_index = jnp.arange(full_y, dtype=jnp.int32)
    cos_y, sin_y = phase_table(y_index, y_index, full_y)
    spec_real, spec_imag = forward_mix(spec_real, spec_imag, cos_y, sin_y, "cxyz,yk->ckxz")
    x_index = jnp.arange(full_x, dtype=jnp.int32)
    cos_xn, sin_xn = phase_table(x_index, x_index, full_x)
    spec_real, spec_imag = (
        lax.all_to_all(spec_real, ("gx", "gz"), split_axis=1, concat_axis=2, tiled=True),
        lax.all_to_all(spec_imag, ("gx", "gz"), split_axis=1, concat_axis=2, tiled=True),
    )
    cos_x, sin_x = (cos_xn, sin_xn)
    spec_real, spec_imag = forward_mix(spec_real, spec_imag, cos_x, sin_x, "cyxz,xk->cyzk")
    inverse_count = 1.0 / (full_x * full_y * full_z)
    out_real = -inverse_count * apply_tensor(kernel, spec_real)
    out_imag = -inverse_count * apply_tensor(kernel, spec_imag)
    wave_y = (lax.axis_index("gx") * count_gz + lax.axis_index("gz")) * part_y + jnp.arange(
        part_y, dtype=jnp.int32
    )
    wave_z = lax.axis_index("gy") * part_z + jnp.arange(planes, dtype=jnp.int32)
    eigenvalue = (
        lattice_eigen(wave_y, full_y)[:, None, None]
        + lattice_eigen(wave_z, full_z)[None, :, None]
        + lattice_eigen(x_index, full_x)[None, None, :]
    )
    factor = inverse_count * exchange_coeff * eigenvalue
    out_real = out_real + factor * spec_real
    out_imag = out_imag + factor * spec_imag
    back_real, back_imag = inverse_mix(out_real, out_imag, cos_xn, sin_xn, "cyzk,kx->cyxz")
    back_real, back_imag = (
        lax.all_to_all(back_real, ("gx", "gz"), split_axis=2, concat_axis=1, tiled=True),
        lax.all_to_all(back_imag, ("gx", "gz"), split_axis=2, concat_axis=1, tiled=True),
    )
    cos_yb, sin_yb = (cos_y, sin_y)
    back_real, back_imag = inverse_mix(back_real, back_imag, cos_yb, sin_yb, "cyxz,yn->cxnz")
    back_real, back_imag = (
        lax.all_to_all(back_real, "gy", split_axis=2, concat_axis=3, tiled=True),
        lax.all_to_all(back_imag, "gy", split_axis=2, concat_axis=3, tiled=True),
    )
    real_rows = back_real.reshape(-1, wave_count)
    imag_rows = back_imag.reshape(-1, wave_count)
    field_lines = (
        jnp.dot(real_rows, cos_zb, precision=highest)
        - jnp.dot(imag_rows, sin_zb, precision=highest)
    ).reshape(lines_shape)
    field_block = lax.all_to_all(field_lines, "gz", split_axis=3, concat_axis=1, tiled=True)
    total_field = field_block + outside
    precess = cross_product(magnetization, total_field)
    double_twist = cross_product(magnetization, precess)
    torque = -(precess + damping * double_twist) / (1.0 + damping * damping)
    stepped = magnetization + time_step * torque
    length = jnp.sqrt(jnp.sum(stepped * stepped, axis=0))
    return (stepped / length, torque)


def cmul_const(value, angle):
    re, im = value
    quarter = angle / (math.pi / 2)
    if abs(quarter - round(quarter)) < 1e-9:
        turn = round(quarter) % 4
        if turn == 0:
            return (re, im)
        if turn == 1:
            return (-im, re)
        if turn == 2:
            return (-re, -im)
        return (im, -re)
    c, s = math.cos(angle), math.sin(angle)
    if abs(abs(c) - abs(s)) < 1e-9:
        h = abs(c)
        sc, ss = math.copysign(1, c), math.copysign(1, s)
        first = re if sc > 0 else -re
        out_re = (first - im) if ss > 0 else (first + im)
        second = im if sc > 0 else -im
        out_im = (second + re) if ss > 0 else (second - re)
        return (h * out_re, h * out_im)
    return (c * re - s * im, c * im + s * re)


def cadd(a, b):
    return (a[0] + b[0], a[1] + b[1])


def csub(a, b):
    return (a[0] - b[0], a[1] - b[1])


def conj(a):
    return (a[0], -a[1])


def complex_fft(values, sign):
    n = len(values)
    if n == 1:
        return values
    even = complex_fft(values[0::2], sign)
    odd = complex_fft(values[1::2], sign)
    odd = [cmul_const(v, sign * 2 * math.pi * k / n) for k, v in enumerate(odd)]
    return [cadd(e, o) for e, o in zip(even, odd)] + [csub(e, o) for e, o in zip(even, odd)]


def real_fft(values):
    n = len(values)
    if n == 2:
        return [values[0] + values[1], values[0] - values[1]]
    even = real_fft(values[0::2])
    odd = real_fft(values[1::2])
    quarter = n // 4
    out = [None] * (n // 2 + 1)
    out[0] = even[0] + odd[0]
    out[n // 2] = even[0] - odd[0]
    for k in range(1, quarter):
        turned = cmul_const(odd[k], -2 * math.pi * k / n)
        out[k] = cadd(even[k], turned)
        out[n // 2 - k] = conj(csub(even[k], turned))
    out[quarter] = (even[quarter], -odd[quarter])
    return out


def real_ifft(values):
    n = 2 * (len(values) - 1)
    if n == 2:
        return [values[0] + values[1], values[0] - values[1]]
    quarter = n // 4
    even = [None] * (quarter + 1)
    odd = [None] * (quarter + 1)
    even[0] = values[0] + values[n // 2]
    odd[0] = values[0] - values[n // 2]
    for k in range(1, quarter):
        mirror = conj(values[n // 2 - k])
        even[k] = cadd(values[k], mirror)
        odd[k] = cmul_const(csub(values[k], mirror), 2 * math.pi * k / n)
    mid = values[quarter]
    even[quarter] = 2.0 * mid[0]
    odd[quarter] = -2.0 * mid[1]
    even = real_ifft(even)
    odd = real_ifft(odd)
    out = [None] * n
    out[0::2] = even
    out[1::2] = odd
    return out


def split(value):
    high = value.astype(jnp.bfloat16)
    return high, (value - high.astype(jnp.float32)).astype(jnp.bfloat16)


def split_table(table, axis):
    high = table.astype(jnp.bfloat16)
    low = (table - high.astype(np.float32)).astype(jnp.bfloat16)
    return np.concatenate([high, low, high], axis)


def mm(a, b, dims):
    return lax.dot_general(a, b, (dims, ((), ())), preferred_element_type=jnp.float32)


class Plan:
    def __init__(self, cx, cy, cz, shape):
        comps, lx, ly, lz = shape
        self.comps, self.lx, self.ly, self.lz = comps, lx, ly, lz
        self.cx, self.cy, self.cz = cx, cy, cz
        self.nx, self.ny, self.nz = lx * cx, ly * cy, lz * cz
        self.planes = cx * cy
        self.groups = cx * cz
        self.devices = cx * cy * cz

    def fits(self):
        if self.devices % 1 or self.lz % self.planes:
            return False
        self.zc = self.lz // self.planes
        self.xl = LANES // self.ly if LANES % self.ly == 0 else 0
        return (
            self.comps == 3
            and self.xl == 4
            and self.cy == 2
            and self.nx == 16 * self.xl
            and self.lx % self.xl == 0
            and self.ly == 2 * self.groups
            and self.zc * SLOTS == LANES
            and self.lz == LANES
            and self.nz % self.zc == 0
        )


def slot_kx(kx2, slot):
    if slot:
        return slot + 16 * kx2
    return (0, 16, 8, 24)[kx2]


def xy_tables(plan):
    lane = np.arange(LANES)
    xl, yl = lane // plan.ly, lane % plan.ly
    half = plan.ny // 2
    fwd = np.zeros((2, 256, 512))
    back = np.zeros((2, 256, 512))
    for r in range(2):
        for k2h in range(2):
            for g in range(plan.groups):
                for ri in range(2):
                    for k2l in range(2):
                        for ql in range(2):
                            block = ri if r == 0 else 1 - ri
                            f = (k2h * plan.groups + g) * 8 + block * 4 + k2l * 2 + ql
                            kx2 = 2 * k2h + k2l
                            ky = 2 * (2 * g + ql) + r
                            ph = 2 * math.pi * (xl * kx2 / 4 + yl * ky / plan.ny)
                            c, s = np.cos(ph), np.sin(ph)
                            if ri == 0:
                                fwd[r, f, 0:128], fwd[r, f, 128:256] = c, s
                                back[r, f, 0:128], back[r, f, 128:256] = c, s
                            else:
                                fwd[r, f, 0:128], fwd[r, f, 128:256] = -s, c
                                back[r, f, 0:128], back[r, f, 128:256] = -s, c
                            kx = slot_kx(kx2, 0)
                            if kx2 == 0:
                                edge = ky in (0, half)
                                if edge:
                                    kx = 0 if ri == 0 else 32
                                else:
                                    kx = 0 if ky < half else 32
                            ph = 2 * math.pi * (xl * kx / plan.nx + yl * ky / plan.ny)
                            c, s = np.cos(ph), np.sin(ph)
                            at = 256 if kx % 16 == 0 else 384
                            if kx2 == 0 and edge:
                                fwd[r, f, at : at + 128] = c
                                back[r, f, at : at + 128] = c
                            else:
                                fwd[r, f, at : at + 128] = c if ri == 0 else -s
                                back[r, f, at : at + 128] = 2 * (c if ri == 0 else -s)
    return fwd.astype(np.float32), back.astype(np.float32)


def x_twiddles(plan):
    xl = np.arange(LANES) // plan.ly
    ph = 2 * math.pi * np.arange(SLOTS)[:, None] * xl[None, :] / plan.nx
    return np.stack([np.cos(ph), np.sin(ph)]).astype(np.float32)


def z_tables(plan):
    zc, nz = plan.zc, plan.nz
    lane = np.arange(LANES) % zc
    ph = 2 * math.pi * np.arange(plan.devices)[:, None] * lane[None, :] / nz
    twiddle = np.stack([np.cos(ph), np.sin(ph)]).astype(np.float32)
    small = 2 * math.pi * np.arange(zc)[:, None] * np.arange(zc)[None, :] / zc
    c = np.kron(np.eye(SLOTS), np.cos(small))
    s = np.kron(np.eye(SLOTS), np.sin(small))
    fwd = np.block([[c, -s], [s, c]]).astype(np.float32)
    back = np.block([[c, s], [-s, c]]).astype(np.float32)
    return twiddle, fwd, back


def fetch(source, target, sem):
    copy = pltpu.make_async_copy(source, target, sem)
    copy.start()
    return copy


def plane_index():
    return lax.axis_index("gx") * lax.axis_size("gy") + lax.axis_index("gy")


def pack_kernel(plan, m_ref, *rest):
    outs, (m_buf, buf, sem_in) = rest[: plan.planes], rest[plan.planes :]
    me = plane_index()
    per = plan.lx * plan.ly // LANES
    width = per * LANES
    loads = [
        fetch(m_ref.at[pl.ds(c * per, per)], m_buf.at[pl.ds(c * per, per)], sem_in.at[c])
        for c in range(plan.comps)
    ]
    for c in range(plan.comps):
        loads[c].wait()
        for t in range(c * per, (c + 1) * per):
            buf[:, LANES * t : LANES * (t + 1)] = m_buf[t].T
        for o in range(plan.planes):
            rows = pl.ds(plan.zc * (me ^ o), plan.zc)
            cols = slice(width * c, width * (c + 1))
            outs[o][:, cols] = buf[rows, cols]


def xy_forward_kernel(plan, *refs):
    chunks, refs = refs[: plan.planes], refs[plan.planes :]
    table_ref, edge_ref, tw_ref, out_ref, lines_ref, g_ref, e_ref = refs
    me = plane_index()
    for o in range(plan.planes):
        lines_ref[me ^ o] = chunks[o][...]
    zc = plan.zc
    per = plan.lx // plan.xl
    low = lax.broadcasted_iota(jnp.int32, (SUBS, LANES), 0) < 4
    first_slot = lax.broadcasted_iota(jnp.int32, (SUBS, LANES), 1) < zc
    blank = jnp.zeros((zc, LANES), jnp.bfloat16)
    for r in range(2):
        for k in range(plan.comps, SLOTS):
            for q in range(4):
                e_ref[r, zc * k : zc * (k + 1), LANES * q : LANES * (q + 1)] = blank

    def keep(ref, at, rows, parts):
        for q, part in enumerate(parts):
            hi, lo = split(part)
            ref[(*at, rows, slice(LANES * q, LANES * (q + 1)))] = hi
            ref[(*at, rows, slice(LANES * (q + 2), LANES * (q + 3)))] = lo

    for c in range(plan.comps):
        parts = [[], []]
        for gx in range(plan.cx):
            for xh in range(per):
                at = c * (plan.lx * plan.ly) + xh * LANES
                first = lines_ref[gx * 2, :, at : at + LANES]
                second = lines_ref[gx * 2 + 1, :, at : at + LANES]
                parts[0].append(first + second)
                parts[1].append(first - second)
        for r in range(2):
            spec = real_fft(parts[r])
            keep(e_ref, (r,), slice(zc * c, zc * (c + 1)), (spec[0], spec[8]))
            for k in range(1, SLOTS):
                re, im = spec[k]
                tc = tw_ref[0, k : k + 1, :]
                ts = tw_ref[1, k : k + 1, :]
                rows = slice(zc * k, zc * (k + 1))
                keep(g_ref, (r, c), rows, (re * tc + im * ts, im * tc - re * ts))
            g_ref[r, c, 0:zc, :] = jnp.zeros((zc, 512), jnp.bfloat16)

    def widen(value):
        return jnp.concatenate([value[:, 0:256], value[:, 0:256], value[:, 256:512]], 1)

    edges = [mm(edge_ref[r], widen(e_ref[r]), ((1,), (1,))) for r in range(2)]
    for c in range(plan.comps):
        outs = [mm(table_ref[r], widen(g_ref[r, c]), ((1,), (1,))) for r in range(2)]
        for k2h in range(2):
            for g in range(plan.groups):
                f = (k2h * plan.groups + g) * SUBS
                both = []
                for r in range(2):
                    edge = edges[r][f : f + SUBS]
                    if c:
                        edge = pltpu.roll(edge, LANES - zc * c, 1)
                    both.append(jnp.where(first_slot, edge, outs[r][f : f + SUBS]))
                one, two = both
                gx, gz = g // plan.cz, g % plan.cz
                dest = gz * plan.planes + gx * plan.cy + k2h
                out_ref[dest, 2 * c] = jnp.where(low, one, two)
                out_ref[dest, 2 * c + 1] = pltpu.roll(jnp.where(low, two, one), 4, 0)


def xy_inverse_kernel(plan, spec_ref, table_ref, edge_ref, tw_ref, *refs):
    outs, (h_ref, t_ref, u_ref, out_ref) = refs[: plan.planes], refs[plan.planes :]
    me = plane_index()
    zc = plan.zc
    per = plan.lx // plan.xl
    low = lax.broadcasted_iota(jnp.int32, (SUBS, LANES), 0) < 4
    for c in range(plan.comps):
        for k2h in range(2):
            for g in range(plan.groups):
                f = (k2h * plan.groups + g) * SUBS
                gx, gz = g // plan.cz, g % plan.cz
                src = gz * plan.planes + gx * plan.cy + k2h
                re = spec_ref[src, 2 * c]
                im = pltpu.roll(spec_ref[src, 2 * c + 1], 4, 0)
                h_ref[c, 0, f : f + SUBS, :] = jnp.where(low, re, im)
                h_ref[c, 1, f : f + SUBS, :] = jnp.where(low, im, re)
        for r in range(2):
            hi, lo = split(h_ref[c, r].T)
            t_ref[r, LANES * c : LANES * (c + 1), 0:256] = hi
            t_ref[r, LANES * c : LANES * (c + 1), 256:512] = lo

    def widen(value):
        return jnp.concatenate([value[:, 0:256], value[:, 0:256], value[:, 256:512]], 1)

    edges = []
    for r in range(2):
        u_ref[r] = mm(widen(t_ref[r]), table_ref[r], ((1,), (0,)))
        rows = jnp.concatenate(
            [t_ref[r, LANES * c : LANES * c + zc, :] for c in range(plan.comps)], 0
        )
        edges.append(mm(widen(rows), edge_ref[r], ((1,), (0,))))
    for c in range(plan.comps):
        fields = []
        for r in range(2):
            edge = edges[r][zc * c : zc * (c + 1)]
            values = [edge[:, 0:128]]
            for k in range(1, SLOTS):
                rows = slice(LANES * c + zc * k, LANES * c + zc * (k + 1))
                re = u_ref[r, rows, 0:128]
                im = u_ref[r, rows, 128:256]
                tc = tw_ref[0, k : k + 1, :]
                ts = tw_ref[1, k : k + 1, :]
                values.append((re * tc - im * ts, im * tc + re * ts))
            values.append(edge[:, 128:256])
            fields.append(real_ifft(values))
        for gx in range(plan.cx):
            for xh in range(per):
                at = c * (plan.lx * plan.ly) + xh * LANES
                one = fields[0][gx * per + xh]
                two = fields[1][gx * per + xh]
                out_ref[gx * 2, :, at : at + LANES] = one + two
                out_ref[gx * 2 + 1, :, at : at + LANES] = one - two
    for o in range(plan.planes):
        outs[o][...] = out_ref[me ^ o]


def z_kernel(
    plan, in_ref, k_ref, kx_ref, mask_ref, tw_ref, fwd_ref, back_ref, out_ref, s_ref, b_ref
):
    n = plan.devices
    half = n // 2 + 1
    mask = mask_ref[...]
    keep = 1.0 - mask

    def transform(at, count, table):
        hi, lo = split(s_ref[at, 0 : SUBS * count, :])
        wide = jnp.concatenate([hi, hi, lo], 1)
        s_ref[at, 0 : SUBS * count, :] = mm(wide, table[...], ((1,), (0,)))

    def to_spectrum(values, at):
        for k, (re, im) in enumerate(values):
            tc = tw_ref[0, k : k + 1, :]
            ts = tw_ref[1, k : k + 1, :]
            s_ref[at, SUBS * k : SUBS * (k + 1), 0:128] = re * tc + im * ts
            s_ref[at, SUBS * k : SUBS * (k + 1), 128:256] = im * tc - re * ts
        transform(at, len(values), fwd_ref)

    def from_spectrum(at, count):
        transform(at, count, back_ref)
        values = []
        for k in range(count):
            re = s_ref[at, SUBS * k : SUBS * (k + 1), 0:128]
            im = s_ref[at, SUBS * k : SUBS * (k + 1), 128:256]
            tc = tw_ref[0, k : k + 1, :]
            ts = tw_ref[1, k : k + 1, :]
            values.append((re * tc - im * ts, im * tc + re * ts))
        return values

    for c in range(plan.comps):
        values = [(in_ref[s, 2 * c], in_ref[s, 2 * c + 1] * keep) for s in range(n)]
        to_spectrum(complex_fft(values, -1), c)
    extra = []
    for s in range(n):
        e = in_ref[s, 1] * mask
        e = e + pltpu.roll(in_ref[s, 3] * mask, 1, 0)
        e = e + pltpu.roll(in_ref[s, 5] * mask, 2, 0)
        extra.append(e + pltpu.roll(e, 3, 0))
    extra = real_fft(extra)
    zero = jnp.zeros((SUBS, LANES), jnp.float32)
    extra[0] = (extra[0], zero)
    extra[-1] = (extra[-1], zero)
    to_spectrum(extra, 3)
    for k in range(n):
        rows = slice(SUBS * k, SUBS * (k + 1))
        t = [k_ref[i, k] for i in range(6)]
        for part in range(2):
            lanes = slice(LANES * part, LANES * (part + 1))
            a, b, g = (s_ref[c, rows, lanes] for c in range(3))
            s_ref[0, rows, lanes] = t[0] * a + t[3] * b + t[4] * g
            s_ref[1, rows, lanes] = t[3] * a + t[1] * b + t[5] * g
            s_ref[2, rows, lanes] = t[4] * a + t[5] * b + t[2] * g
            if k < half:
                d = [kx_ref[i, k] for i in range(3)]
                e = s_ref[3, rows, lanes]
                s_ref[3, rows, lanes] = (
                    d[0] * e + d[1] * pltpu.roll(e, 7, 0) + d[2] * pltpu.roll(e, 6, 0)
                )
    extra = from_spectrum(3, half)
    extra[0] = extra[0][0]
    extra[-1] = extra[-1][0]
    extra = real_ifft(extra)
    for s in range(n):
        b_ref[s] = extra[s]
    for c in range(plan.comps):
        values = complex_fft(from_spectrum(c, n), 1)
        for s in range(n):
            e = b_ref[s]
            if c:
                e = pltpu.roll(e, SUBS - c, 0)
            out_ref[s, 2 * c] = values[s][0]
            out_ref[s, 2 * c + 1] = values[s][1] * keep + e * mask


def finish_kernel(plan, *refs):
    chunks, refs = refs[: plan.planes], refs[plan.planes :]
    m_ref, applied_ref, pred_hbm, torque_hbm, *refs = refs
    field_ref, pred_ref, torque_ref, sem_out = refs
    me = plane_index()
    tiles = plan.lx * plan.ly // LANES
    for o in range(plan.planes):
        field_ref[pl.ds(plan.zc * (me ^ o), plan.zc), :] = chunks[o][...]
    stores = []
    scale = -1.0 / (1.0 + damping * damping)
    for t in range(tiles):
        h, m = [], []
        for c in range(3):
            at = (c * tiles + t) * LANES
            h.append(field_ref[:, at : at + LANES].T + applied_ref[c])
            m.append(m_ref[c, t])
        a = [m[1] * h[2] - m[2] * h[1], m[2] * h[0] - m[0] * h[2], m[0] * h[1] - m[1] * h[0]]
        b = [m[1] * a[2] - m[2] * a[1], m[2] * a[0] - m[0] * a[2], m[0] * a[1] - m[1] * a[0]]
        torque = [(a[c] + damping * b[c]) * scale for c in range(3)]
        step = [m[c] + time_step * torque[c] for c in range(3)]
        total = step[0] * step[0] + step[1] * step[1] + step[2] * step[2]
        inverse = lax.rsqrt(total)
        for c in range(3):
            torque_ref[c, t] = torque[c]
            pred_ref[c, t] = step[c] * inverse
        stores.append(fetch(torque_ref.at[:, t], torque_hbm.at[:, t], sem_out.at[0, t]))
        stores.append(fetch(pred_ref.at[:, t], pred_hbm.at[:, t], sem_out.at[1, t]))
    for store in stores:
        store.wait()


def lattice_eigen(wave_index, length):
    return 2.0 * jnp.cos(wave_index.astype(jnp.float32) * (2.0 * math.pi / length)) - 2.0


def tensor_pick_kernel(plan, k_hbm, own_ref, give_ref, k_ref, sem):
    parts = 6
    loads = [fetch(k_hbm.at[i], k_ref.at[i], sem.at[i]) for i in range(parts)]
    group = lax.axis_index("gx") * plan.cz + lax.axis_index("gz")
    low = lax.axis_index("gy") == 0
    sub = lax.broadcasted_iota(jnp.int32, (SUBS, k_ref.shape[3]), 0)
    top = sub == 0
    edge = jnp.zeros(sub.shape, jnp.float32)
    tile = lambda i, j, t: k_ref[i, j, SUBS * t : SUBS * (t + 1), :]
    for i in range(parts):
        loads[i].wait()
        edge = jnp.where(sub == i, pltpu.roll(tile(i, 0, 4), i, 0), edge)
        for j in range(4):
            far = 4 * group + j > plan.ny // 2
            values = [
                jnp.where(top & far, tile(i, j, 4), tile(i, j, 0)),
                tile(i, j, 2),
                jnp.where(top, tile(i, j, 1), tile(i, j, 4)),
                jnp.where(top, tile(i, j, 3), tile(i, j, 6)),
            ]
            for k2l in range(2):
                row = ((i * 4 + j) * 2 + k2l) * SUBS
                own_ref[row : row + SUBS, :] = jnp.where(low, values[k2l], values[2 + k2l])
                give_ref[row : row + SUBS, :] = jnp.where(low, values[2 + k2l], values[k2l])
    row = parts * 4 * 2 * SUBS
    own_ref[row : row + SUBS, :] = edge
    give_ref[row : row + SUBS, :] = edge


def tensor_pick(plan, kernel):
    rows = pltpu.VMEM((6 * 4 * 2 * SUBS + SUBS, kernel.shape[2]), jnp.float32)
    kt = jnp.swapaxes(kernel, 2, 3)
    return call(
        lambda *a: tensor_pick_kernel(plan, *a),
        "h",
        (rows, rows),
        [pltpu.VMEM(kt.shape, jnp.float32), pltpu.SemaphoreType.DMA((6,))],
    )(kt)


def field_tensor(plan, own, other):
    gx, gy, gz = (lax.axis_index(a) for a in ("gx", "gy", "gz"))
    group = gx * plan.cz + gz
    kzs = own.shape[1]
    other = lax.ppermute(other, "gy", [(0, 1), (1, 0)])
    own, other = own[None], other[None]
    got = jnp.where(gy == 0, jnp.concatenate([own, other]), jnp.concatenate([other, own]))
    main = got[:, : 6 * 4 * 2 * 8].reshape(2, 6, 2, 2, 2, 8, kzs // 32, 32)
    main = jnp.transpose(main, (1, 7, 3, 4, 2, 5, 0, 6)).reshape(6, 32, 8, 128)
    edge = got[:, 6 * 4 * 2 * 8 : 6 * 4 * 2 * 8 + 6].reshape(2, 6, kzs // 32, 32)
    edge = jnp.transpose(edge, (1, 3, 0, 2)).reshape(6, 32, plan.zc)
    kz = jnp.arange(plan.nz).reshape(plan.zc, 32).T
    table = np.array([[slot_kx(k2, s) for s in range(SLOTS)] for k2 in range(4)])
    kx = jnp.asarray(table.reshape(2, 2, SLOTS), jnp.int32)[gy]
    kyq = (4 * group + 2 * jnp.arange(2)[None, :] + jnp.arange(2)[:, None])
    kx_full = jnp.broadcast_to(kx[None, :, None, :], (2, 2, 2, SLOTS))
    swap = (gy == 0) & (kyq > plan.ny // 2)
    is_packed = (jnp.arange(2)[None, :, None, None] == 0) & (jnp.arange(SLOTS) == 0)
    kx_full = jnp.where(is_packed & swap[:, None, :, None], 32, kx_full)
    ex = lattice_eigen(kx_full, plan.nx)
    ey = lattice_eigen(kyq, plan.ny)
    ez = lattice_eigen(kz, plan.nz)
    plane = (ex + ey[:, None, :, None]).reshape(8, SLOTS)
    eig = plane[None, :, :, None] + ez[:, None, None, :]
    eig = eig.reshape(32, 8, 128)
    scale = 1.0 / (plan.nx * plan.ny * plan.nz)
    diag = jnp.asarray([1, 1, 1, 0, 0, 0], jnp.float32)[:, None, None, None]
    tensor = scale * (exchange_coeff * diag * eig[None] - main)
    edge_eig = lattice_eigen(jnp.asarray(32), plan.nx) + lattice_eigen(4 * group, plan.ny) + ez
    edge = scale * (exchange_coeff * diag[:, :, :, 0] * edge_eig[None] - edge)
    order = np.array([[0, 1, 2], [3, 5, 4], [4, 3, 5]])
    edge = edge[order]
    edge = jnp.transpose(edge, (0, 2, 1, 3))
    edge = jnp.pad(edge, ((0, 0), (0, 0), (0, 5), (0, LANES - plan.zc)))
    special = (gy == 0) & ((group == 0) | (group == plan.groups // 2))
    spot = (jnp.arange(8)[:, None] == 0) & (jnp.arange(LANES)[None, :] < plan.zc)
    mask = jnp.where(special & spot, 1.0, 0.0).astype(jnp.float32)
    return tensor, edge, mask


def call(body, places, outs, scratch):
    spaces = {"h": pltpu.HBM, "v": pltpu.VMEM, "s": pltpu.SMEM}

    def space_of(out):
        return pltpu.VMEM if isinstance(out, pl.MemoryRef) else pl.ANY

    step = pl.pallas_call(
        body,
        out_shape=outs,
        in_specs=[pl.BlockSpec(memory_space=spaces[p]) for p in places],
        out_specs=jax.tree.map(lambda o: pl.BlockSpec(memory_space=space_of(o)), outs),
        scratch_shapes=scratch,
        compiler_params=pltpu.CompilerParams(vmem_limit_bytes=8 * 2**20),
    )

    def run(*args):
        return step(
            *(
                x if p == "s" else pltpu.with_memory_space_constraint(x, spaces[p])
                for p, x in zip(places, args)
            )
        )

    return run


SEND_ORDER = (7, 4, 1, 5, 6, 3, 2)


def plane_swap(plan, chunks):
    members = range(plan.planes)
    out = list(chunks)
    for o in SEND_ORDER:
        out[o] = lax.ppermute(chunks[o], ("gx", "gy"), [(k, k ^ o) for k in members])
    return out


def on_chip(like, *tables):
    there = like > -jnp.inf
    return [jnp.where(there, t, jnp.zeros((), t.dtype)) for t in tables]


def fast_shards(plan, magnetization, kernel, applied):
    f32, bf16 = jnp.float32, jnp.bfloat16
    sds, vmem, dma = jax.ShapeDtypeStruct, pltpu.VMEM, pltpu.SemaphoreType.DMA
    n, zc, planes = plan.devices, plan.zc, plan.planes
    width = 3 * plan.lx * plan.ly
    tiles = width // LANES
    fwd, back = xy_tables(plan)
    fwd = [split_table(t, 2) for t in (fwd[:, :, 0:256], fwd[:, :, 256:512])]
    back = [split_table(t, 1) for t in (back[:, :, 0:256], back[:, :, 256:512])]
    tw = x_twiddles(plan)
    ztw, zf, zb = z_tables(plan)
    zf, zb = split_table(zf, 0), split_table(zb, 0)
    chunk = vmem((zc, width), f32)
    spectrum = (n, 6, SUBS, LANES)
    m_tiles = magnetization.reshape(tiles, LANES, LANES)
    packed = call(
        lambda *a: pack_kernel(plan, *a),
        "h",
        [chunk] * planes,
        [vmem((tiles, LANES, LANES), f32), vmem((plan.lz, width), f32), dma((3,))],
    )(m_tiles)
    first, kernel = lax.optimization_barrier((packed[0], kernel))
    packed = [first, *packed[1:]]
    own, other = tensor_pick(plan, kernel)
    *fwd, x_tw = on_chip(own[0, 0], *fwd, tw)
    tensor, edge, mask = field_tensor(plan, own, other)
    ztw, zf, zb = on_chip(tensor[0, 0, 0, 0], ztw, zf, zb)
    lines = plane_swap(plan, packed)
    spec = call(
        lambda *a: xy_forward_kernel(plan, *a),
        "v" * planes + "vvv",
        vmem(spectrum, f32),
        [
            vmem((planes, zc, width), f32),
            vmem((2, 3, LANES, 512), bf16),
            vmem((2, LANES, 512), bf16),
        ],
    )(*lines, *fwd, x_tw)
    spec = lax.all_to_all(spec, ("gz", "gx", "gy"), split_axis=0, concat_axis=0, tiled=True)
    spec = call(
        lambda *a: z_kernel(plan, *a),
        "vvvvvvv",
        vmem(spectrum, f32),
        [
            vmem((4, n * SUBS, 256), f32),
            vmem((n, SUBS, LANES), f32),
        ],
    )(spec, tensor, edge, mask, ztw, zf, zb)
    spec = lax.all_to_all(spec, ("gz", "gx", "gy"), split_axis=0, concat_axis=0, tiled=True)
    field = call(
        lambda *a: xy_inverse_kernel(plan, *a),
        "vvvv",
        [chunk] * planes,
        [
            vmem((3, 2, 256, LANES), f32),
            vmem((2, 3 * LANES, 512), bf16),
            vmem((2, 3 * LANES, 256), f32),
            vmem((planes, zc, width), f32),
        ],
    )(spec, *back, tw)
    field = plane_swap(plan, field)
    cells = (3, tiles // 3, LANES, LANES)
    pred, torque = call(
        lambda *a: finish_kernel(plan, *a),
        "v" * planes + "vs",
        (sds(cells, f32), sds(cells, f32)),
        [
            vmem((plan.lz, width), f32),
            vmem(cells, f32),
            vmem(cells, f32),
            dma((2, tiles // 3)),
        ],
    )(*field, magnetization.reshape(cells), applied)
    return pred.reshape(magnetization.shape), torque.reshape(magnetization.shape)


def solution(mesh):
    sizes = mesh.shape

    def shards(magnetization, kernel, applied):
        plan = Plan(sizes["gx"], sizes["gy"], sizes["gz"], magnetization.shape)
        if plan.fits():
            return fast_shards(plan, magnetization, kernel, applied)
        return general_shards(magnetization, kernel, applied)

    return jax.shard_map(
        shards,
        mesh=mesh,
        in_specs=(P(None, "gx", "gy", "gz"), P(None, ("gx", "gz"), "gy", None), P()),
        out_specs=(P(None, "gx", "gy", "gz"), P(None, "gx", "gy", "gz")),
        check_vma=False,
    )
```

```python
import math

import jax
import jax.numpy as jnp
import numpy as np
from jax import lax
from jax.experimental import pallas as pl
from jax.experimental.pallas import tpu as pltpu
from jax.sharding import PartitionSpec as P


exchange_coeff = 1.0
damping = 0.3
time_step = 0.2
highest = lax.Precision.HIGHEST
LANES = 128
SUBS = 8
SLOTS = 8


def phase_table(row_index, col_index, length):
    product = row_index[:, None] * col_index[None, :] % length
    angles = product.astype(jnp.float32) * (2.0 * math.pi / length)
    return (jnp.cos(angles), jnp.sin(angles))


def forward_mix(real_part, imag_part, cosine_table, sine_table, pattern):
    real_out = jnp.einsum(pattern, real_part, cosine_table, precision=highest) + jnp.einsum(
        pattern, imag_part, sine_table, precision=highest
    )
    imag_out = jnp.einsum(pattern, imag_part, cosine_table, precision=highest) - jnp.einsum(
        pattern, real_part, sine_table, precision=highest
    )
    return (real_out, imag_out)


def inverse_mix(real_part, imag_part, cosine_table, sine_table, pattern):
    real_out = jnp.einsum(pattern, real_part, cosine_table, precision=highest) - jnp.einsum(
        pattern, imag_part, sine_table, precision=highest
    )
    imag_out = jnp.einsum(pattern, imag_part, cosine_table, precision=highest) + jnp.einsum(
        pattern, real_part, sine_table, precision=highest
    )
    return (real_out, imag_out)


def apply_tensor(kernel, spectrum):
    return jnp.stack(
        [
            kernel[0] * spectrum[0] + kernel[3] * spectrum[1] + kernel[4] * spectrum[2],
            kernel[3] * spectrum[0] + kernel[1] * spectrum[1] + kernel[5] * spectrum[2],
            kernel[4] * spectrum[0] + kernel[5] * spectrum[1] + kernel[2] * spectrum[2],
        ]
    )


def cross_product(first_vec, second_vec):
    return jnp.stack(
        [
            first_vec[1] * second_vec[2] - first_vec[2] * second_vec[1],
            first_vec[2] * second_vec[0] - first_vec[0] * second_vec[2],
            first_vec[0] * second_vec[1] - first_vec[1] * second_vec[0],
        ]
    )


def general_shards(magnetization, kernel, applied):
    count_gx = lax.axis_size("gx")
    count_gy = lax.axis_size("gy")
    count_gz = lax.axis_size("gz")
    local_x = magnetization.shape[1]
    local_y = magnetization.shape[2]
    local_z = magnetization.shape[3]
    full_x = local_x * count_gx
    full_y = local_y * count_gy
    full_z = local_z * count_gz
    part_x = local_x // count_gz
    part_y = full_y // (count_gx * count_gz)
    part_z = full_z // count_gy
    outside = applied[:, None, None, None]
    z_index = jnp.arange(full_z, dtype=jnp.int32)
    weights = jnp.ones((full_z,), jnp.float32)
    planes = z_index.shape[0] // count_gy
    wave_count = z_index.shape[0]
    zlines = lax.all_to_all(magnetization, "gz", split_axis=1, concat_axis=3, tiled=True)
    cos_zf, sin_zf = phase_table(z_index, z_index, full_z)
    cos_zb, sin_zb = phase_table(z_index, z_index, full_z)
    cos_zb = cos_zb * weights[:, None]
    sin_zb = sin_zb * weights[:, None]
    lines_shape = (3, part_x, local_y, full_z)
    wave_shape = (3, part_x, local_y, wave_count)
    z_rows = zlines.reshape(-1, full_z)
    spec_real = jnp.dot(z_rows, cos_zf, precision=highest).reshape(wave_shape)
    spec_imag = -jnp.dot(z_rows, sin_zf, precision=highest).reshape(wave_shape)
    spec_real, spec_imag = (
        lax.all_to_all(spec_real, "gy", split_axis=3, concat_axis=2, tiled=True),
        lax.all_to_all(spec_imag, "gy", split_axis=3, concat_axis=2, tiled=True),
    )
    y_index = jnp.arange(full_y, dtype=jnp.int32)
    cos_y, sin_y = phase_table(y_index, y_index, full_y)
    spec_real, spec_imag = forward_mix(spec_real, spec_imag, cos_y, sin_y, "cxyz,yk->ckxz")
    x_index = jnp.arange(full_x, dtype=jnp.int32)
    cos_xn, sin_xn = phase_table(x_index, x_index, full_x)
    spec_real, spec_imag = (
        lax.all_to_all(spec_real, ("gx", "gz"), split_axis=1, concat_axis=2, tiled=True),
        lax.all_to_all(spec_imag, ("gx", "gz"), split_axis=1, concat_axis=2, tiled=True),
    )
    cos_x, sin_x = (cos_xn, sin_xn)
    spec_real, spec_imag = forward_mix(spec_real, spec_imag, cos_x, sin_x, "cyxz,xk->cyzk")
    inverse_count = 1.0 / (full_x * full_y * full_z)
    out_real = -inverse_count * apply_tensor(kernel, spec_real)
    out_imag = -inverse_count * apply_tensor(kernel, spec_imag)
    wave_y = (lax.axis_index("gx") * count_gz + lax.axis_index("gz")) * part_y + jnp.arange(
        part_y, dtype=jnp.int32
    )
    wave_z = lax.axis_index("gy") * part_z + jnp.arange(planes, dtype=jnp.int32)
    eigenvalue = (
        lattice_eigen(wave_y, full_y)[:, None, None]
        + lattice_eigen(wave_z, full_z)[None, :, None]
        + lattice_eigen(x_index, full_x)[None, None, :]
    )
    factor = inverse_count * exchange_coeff * eigenvalue
    out_real = out_real + factor * spec_real
    out_imag = out_imag + factor * spec_imag
    back_real, back_imag = inverse_mix(out_real, out_imag, cos_xn, sin_xn, "cyzk,kx->cyxz")
    back_real, back_imag = (
        lax.all_to_all(back_real, ("gx", "gz"), split_axis=2, concat_axis=1, tiled=True),
        lax.all_to_all(back_imag, ("gx", "gz"), split_axis=2, concat_axis=1, tiled=True),
    )
    cos_yb, sin_yb = (cos_y, sin_y)
    back_real, back_imag = inverse_mix(back_real, back_imag, cos_yb, sin_yb, "cyxz,yn->cxnz")
    back_real, back_imag = (
        lax.all_to_all(back_real, "gy", split_axis=2, concat_axis=3, tiled=True),
        lax.all_to_all(back_imag, "gy", split_axis=2, concat_axis=3, tiled=True),
    )
    real_rows = back_real.reshape(-1, wave_count)
    imag_rows = back_imag.reshape(-1, wave_count)
    field_lines = (
        jnp.dot(real_rows, cos_zb, precision=highest)
        - jnp.dot(imag_rows, sin_zb, precision=highest)
    ).reshape(lines_shape)
    field_block = lax.all_to_all(field_lines, "gz", split_axis=3, concat_axis=1, tiled=True)
    total_field = field_block + outside
    precess = cross_product(magnetization, total_field)
    double_twist = cross_product(magnetization, precess)
    torque = -(precess + damping * double_twist) / (1.0 + damping * damping)
    stepped = magnetization + time_step * torque
    length = jnp.sqrt(jnp.sum(stepped * stepped, axis=0))
    return (stepped / length, torque)


def cmul_const(value, angle):
    re, im = value
    quarter = angle / (math.pi / 2)
    if abs(quarter - round(quarter)) < 1e-9:
        turn = round(quarter) % 4
        if turn == 0:
            return (re, im)
        if turn == 1:
            return (-im, re)
        if turn == 2:
            return (-re, -im)
        return (im, -re)
    c, s = math.cos(angle), math.sin(angle)
    if abs(abs(c) - abs(s)) < 1e-9:
        h = abs(c)
        sc, ss = math.copysign(1, c), math.copysign(1, s)
        first = re if sc > 0 else -re
        out_re = (first - im) if ss > 0 else (first + im)
        second = im if sc > 0 else -im
        out_im = (second + re) if ss > 0 else (second - re)
        return (h * out_re, h * out_im)
    return (c * re - s * im, c * im + s * re)


def cadd(a, b):
    return (a[0] + b[0], a[1] + b[1])


def csub(a, b):
    return (a[0] - b[0], a[1] - b[1])


def conj(a):
    return (a[0], -a[1])


def complex_fft(values, sign):
    n = len(values)
    if n == 1:
        return values
    even = complex_fft(values[0::2], sign)
    odd = complex_fft(values[1::2], sign)
    odd = [cmul_const(v, sign * 2 * math.pi * k / n) for k, v in enumerate(odd)]
    return [cadd(e, o) for e, o in zip(even, odd)] + [csub(e, o) for e, o in zip(even, odd)]


def real_fft(values):
    n = len(values)
    if n == 2:
        return [values[0] + values[1], values[0] - values[1]]
    even = real_fft(values[0::2])
    odd = real_fft(values[1::2])
    quarter = n // 4
    out = [None] * (n // 2 + 1)
    out[0] = even[0] + odd[0]
    out[n // 2] = even[0] - odd[0]
    for k in range(1, quarter):
        turned = cmul_const(odd[k], -2 * math.pi * k / n)
        out[k] = cadd(even[k], turned)
        out[n // 2 - k] = conj(csub(even[k], turned))
    out[quarter] = (even[quarter], -odd[quarter])
    return out


def real_ifft(values):
    n = 2 * (len(values) - 1)
    if n == 2:
        return [values[0] + values[1], values[0] - values[1]]
    quarter = n // 4
    even = [None] * (quarter + 1)
    odd = [None] * (quarter + 1)
    even[0] = values[0] + values[n // 2]
    odd[0] = values[0] - values[n // 2]
    for k in range(1, quarter):
        mirror = conj(values[n // 2 - k])
        even[k] = cadd(values[k], mirror)
        odd[k] = cmul_const(csub(values[k], mirror), 2 * math.pi * k / n)
    mid = values[quarter]
    even[quarter] = 2.0 * mid[0]
    odd[quarter] = -2.0 * mid[1]
    even = real_ifft(even)
    odd = real_ifft(odd)
    out = [None] * n
    out[0::2] = even
    out[1::2] = odd
    return out


def split(value):
    high = value.astype(jnp.bfloat16)
    return high, (value - high.astype(jnp.float32)).astype(jnp.bfloat16)


def split_table(table, axis):
    high = table.astype(jnp.bfloat16)
    low = (table - high.astype(np.float32)).astype(jnp.bfloat16)
    return np.concatenate([high, low], axis)


def high_high_low(value):
    return jnp.concatenate([value[:, 0:256], value[:, 0:256], value[:, 256:512]], 1)


def high_low_high(table, axis):
    high, low = (lax.slice_in_dim(table, at, at + 256, axis=axis) for at in (0, 256))
    return jnp.concatenate([high, low, high], axis)


def mm(a, b, dims):
    return lax.dot_general(a, b, (dims, ((), ())), preferred_element_type=jnp.float32)


class Plan:
    def __init__(self, cx, cy, cz, shape):
        comps, lx, ly, lz = shape
        self.comps, self.lx, self.ly, self.lz = comps, lx, ly, lz
        self.cx, self.cy, self.cz = cx, cy, cz
        self.nx, self.ny, self.nz = lx * cx, ly * cy, lz * cz
        self.planes = cx * cy
        self.groups = cx * cz
        self.devices = cx * cy * cz

    def fits(self):
        if self.devices % 1 or self.lz % self.planes:
            return False
        self.zc = self.lz // self.planes
        self.xl = LANES // self.ly if LANES % self.ly == 0 else 0
        return (
            self.comps == 3
            and self.xl == 4
            and self.cy == 2
            and self.nx == 16 * self.xl
            and self.lx % self.xl == 0
            and self.ly == 2 * self.groups
            and self.zc * SLOTS == LANES
            and self.lz == LANES
            and self.nz % self.zc == 0
        )


def slot_kx(kx2, slot):
    if slot:
        return slot + 16 * kx2
    return (0, 16, 8, 24)[kx2]


def xy_tables(plan):
    lane = np.arange(LANES)
    xl, yl = lane // plan.ly, lane % plan.ly
    half = plan.ny // 2
    fwd = np.zeros((2, 256, 512))
    back = np.zeros((2, 256, 512))
    for r in range(2):
        for k2h in range(2):
            for g in range(plan.groups):
                for ri in range(2):
                    for k2l in range(2):
                        for ql in range(2):
                            block = ri if r == 0 else 1 - ri
                            f = (k2h * plan.groups + g) * 8 + block * 4 + k2l * 2 + ql
                            kx2 = 2 * k2h + k2l
                            ky = 2 * (2 * g + ql) + r
                            ph = 2 * math.pi * (xl * kx2 / 4 + yl * ky / plan.ny)
                            c, s = np.cos(ph), np.sin(ph)
                            if ri == 0:
                                fwd[r, f, 0:128], fwd[r, f, 128:256] = c, s
                                back[r, f, 0:128], back[r, f, 128:256] = c, s
                            else:
                                fwd[r, f, 0:128], fwd[r, f, 128:256] = -s, c
                                back[r, f, 0:128], back[r, f, 128:256] = -s, c
                            kx = slot_kx(kx2, 0)
                            if kx2 == 0:
                                edge = ky in (0, half)
                                if edge:
                                    kx = 0 if ri == 0 else 32
                                else:
                                    kx = 0 if ky < half else 32
                            ph = 2 * math.pi * (xl * kx / plan.nx + yl * ky / plan.ny)
                            c, s = np.cos(ph), np.sin(ph)
                            at = 256 if kx % 16 == 0 else 384
                            if kx2 == 0 and edge:
                                fwd[r, f, at : at + 128] = c
                                back[r, f, at : at + 128] = c
                            else:
                                fwd[r, f, at : at + 128] = c if ri == 0 else -s
                                back[r, f, at : at + 128] = 2 * (c if ri == 0 else -s)
    return fwd.astype(np.float32), back.astype(np.float32)


def fill_twiddles(ref, rows, lane_index, length):
    row = lax.broadcasted_iota(jnp.int32, (rows, LANES), 0)
    angle = (row * lane_index).astype(jnp.float32) * (2 * math.pi / length)
    ref[0] = jnp.cos(angle)
    ref[1] = jnp.sin(angle)


def fill_x_twiddles(plan, ref):
    lane = lax.broadcasted_iota(jnp.int32, (SUBS, LANES), 1)
    fill_twiddles(ref, SUBS, lane // plan.ly, plan.nx)


def z_tables(plan):
    zc = plan.zc
    small = 2 * math.pi * np.arange(zc)[:, None] * np.arange(zc)[None, :] / zc
    c = np.kron(np.eye(SLOTS), np.cos(small))
    s = np.kron(np.eye(SLOTS), np.sin(small))
    fwd = np.block([[c, -s], [s, c]]).astype(np.float32)
    back = np.block([[c, s], [-s, c]]).astype(np.float32)
    return fwd, back


def fetch(source, target, sem):
    copy = pltpu.make_async_copy(source, target, sem)
    copy.start()
    return copy


def plane_index():
    return lax.axis_index("gx") * lax.axis_size("gy") + lax.axis_index("gy")


def pack_kernel(plan, m_ref, *rest):
    outs, (m_buf, buf, sem_in) = rest[: plan.planes], rest[plan.planes :]
    me = plane_index()
    per = plan.lx * plan.ly // LANES
    width = per * LANES
    loads = [
        fetch(m_ref.at[pl.ds(c * per, per)], m_buf.at[pl.ds(c * per, per)], sem_in.at[c])
        for c in range(plan.comps)
    ]
    for c in range(plan.comps):
        loads[c].wait()
        for t in range(c * per, (c + 1) * per):
            buf[:, LANES * t : LANES * (t + 1)] = m_buf[t].T
        for o in range(plan.planes):
            rows = pl.ds(plan.zc * (me ^ o), plan.zc)
            cols = slice(width * c, width * (c + 1))
            outs[o][:, cols] = buf[rows, cols]


def xy_forward_kernel(plan, *refs):
    chunks, refs = refs[: plan.planes], refs[plan.planes :]
    table_ref, edge_ref, out_ref, lines_ref, g_ref, e_ref, tw_ref = refs
    me = plane_index()
    fill_x_twiddles(plan, tw_ref)
    for o in range(plan.planes):
        lines_ref[me ^ o] = chunks[o][...]
    zc = plan.zc
    per = plan.lx // plan.xl
    low = lax.broadcasted_iota(jnp.int32, (SUBS, LANES), 0) < 4
    first_slot = lax.broadcasted_iota(jnp.int32, (SUBS, LANES), 1) < zc
    blank = jnp.zeros((zc, LANES), jnp.bfloat16)
    for r in range(2):
        for k in range(plan.comps, SLOTS):
            for q in range(4):
                e_ref[r, zc * k : zc * (k + 1), LANES * q : LANES * (q + 1)] = blank

    def keep(ref, at, rows, parts):
        for q, part in enumerate(parts):
            hi, lo = split(part)
            ref[(*at, rows, slice(LANES * q, LANES * (q + 1)))] = hi
            ref[(*at, rows, slice(LANES * (q + 2), LANES * (q + 3)))] = lo

    for c in range(plan.comps):
        parts = [[], []]
        for gx in range(plan.cx):
            for xh in range(per):
                at = c * (plan.lx * plan.ly) + xh * LANES
                first = lines_ref[gx * 2, :, at : at + LANES]
                second = lines_ref[gx * 2 + 1, :, at : at + LANES]
                parts[0].append(first + second)
                parts[1].append(first - second)
        for r in range(2):
            spec = real_fft(parts[r])
            keep(e_ref, (r,), slice(zc * c, zc * (c + 1)), (spec[0], spec[8]))
            for k in range(1, SLOTS):
                re, im = spec[k]
                tc = tw_ref[0, k : k + 1, :]
                ts = tw_ref[1, k : k + 1, :]
                rows = slice(zc * k, zc * (k + 1))
                keep(g_ref, (r, c), rows, (re * tc + im * ts, im * tc - re * ts))
            g_ref[r, c, 0:zc, :] = jnp.zeros((zc, 512), jnp.bfloat16)

    edges = [mm(high_low_high(edge_ref[r], 1), high_high_low(e_ref[r]), ((1,), (1,))) for r in range(2)]
    for c in range(plan.comps):
        outs = [
            mm(high_low_high(table_ref[r], 1), high_high_low(g_ref[r, c]), ((1,), (1,)))
            for r in range(2)
        ]
        for k2h in range(2):
            for g in range(plan.groups):
                f = (k2h * plan.groups + g) * SUBS
                both = []
                for r in range(2):
                    edge = edges[r][f : f + SUBS]
                    if c:
                        edge = pltpu.roll(edge, LANES - zc * c, 1)
                    both.append(jnp.where(first_slot, edge, outs[r][f : f + SUBS]))
                one, two = both
                gx, gz = g // plan.cz, g % plan.cz
                dest = (gx * plan.cy + k2h) * plan.cz + gz
                out_ref[dest, 2 * c] = jnp.where(low, one, two)
                out_ref[dest, 2 * c + 1] = pltpu.roll(jnp.where(low, two, one), 4, 0)


def xy_inverse_kernel(plan, spec_ref, table_ref, edge_ref, *refs):
    outs, (h_ref, t_ref, u_ref, out_ref, tw_ref) = refs[: plan.planes], refs[plan.planes :]
    me = plane_index()
    fill_x_twiddles(plan, tw_ref)
    zc = plan.zc
    per = plan.lx // plan.xl
    low = lax.broadcasted_iota(jnp.int32, (SUBS, LANES), 0) < 4
    for c in range(plan.comps):
        for k2h in range(2):
            for g in range(plan.groups):
                f = (k2h * plan.groups + g) * SUBS
                gx, gz = g // plan.cz, g % plan.cz
                src = (gx * plan.cy + k2h) * plan.cz + gz
                re = spec_ref[src, 2 * c]
                im = pltpu.roll(spec_ref[src, 2 * c + 1], 4, 0)
                h_ref[c, 0, f : f + SUBS, :] = jnp.where(low, re, im)
                h_ref[c, 1, f : f + SUBS, :] = jnp.where(low, im, re)
        for r in range(2):
            hi, lo = split(h_ref[c, r].T)
            t_ref[r, LANES * c : LANES * (c + 1), 0:256] = hi
            t_ref[r, LANES * c : LANES * (c + 1), 256:512] = lo

    edges = []
    for r in range(2):
        u_ref[r] = mm(high_high_low(t_ref[r]), high_low_high(table_ref[r], 0), ((1,), (0,)))
        rows = jnp.concatenate(
            [t_ref[r, LANES * c : LANES * c + zc, :] for c in range(plan.comps)], 0
        )
        edges.append(mm(high_high_low(rows), high_low_high(edge_ref[r], 0), ((1,), (0,))))
    for c in range(plan.comps):
        fields = []
        for r in range(2):
            edge = edges[r][zc * c : zc * (c + 1)]
            values = [edge[:, 0:128]]
            for k in range(1, SLOTS):
                rows = slice(LANES * c + zc * k, LANES * c + zc * (k + 1))
                re = u_ref[r, rows, 0:128]
                im = u_ref[r, rows, 128:256]
                tc = tw_ref[0, k : k + 1, :]
                ts = tw_ref[1, k : k + 1, :]
                values.append((re * tc - im * ts, im * tc + re * ts))
            values.append(edge[:, 128:256])
            fields.append(real_ifft(values))
        for gx in range(plan.cx):
            for xh in range(per):
                at = c * (plan.lx * plan.ly) + xh * LANES
                one = fields[0][gx * per + xh]
                two = fields[1][gx * per + xh]
                out_ref[gx * 2, :, at : at + LANES] = one + two
                out_ref[gx * 2 + 1, :, at : at + LANES] = one - two
    for o in range(plan.planes):
        outs[o][...] = out_ref[me ^ o]


def z_kernel(
    plan, in_ref, k_ref, kx_ref, mask_ref, fwd_ref, back_ref, out_ref, s_ref, b_ref, tw_ref
):
    n = plan.devices
    lane = lax.broadcasted_iota(jnp.int32, (n, LANES), 1)
    fill_twiddles(tw_ref, n, lane % plan.zc, plan.nz)
    half = n // 2 + 1
    mask = mask_ref[...]
    place = [(s % plan.planes) * plan.cz + s // plan.planes for s in range(n)]
    keep = 1.0 - mask

    def transform(at, count, table):
        hi, lo = split(s_ref[at, 0 : SUBS * count, :])
        wide = jnp.concatenate([hi, hi, lo], 1)
        s_ref[at, 0 : SUBS * count, :] = mm(wide, high_low_high(table[...], 0), ((1,), (0,)))

    def to_spectrum(values, at):
        for k, (re, im) in enumerate(values):
            tc = tw_ref[0, k : k + 1, :]
            ts = tw_ref[1, k : k + 1, :]
            s_ref[at, SUBS * k : SUBS * (k + 1), 0:128] = re * tc + im * ts
            s_ref[at, SUBS * k : SUBS * (k + 1), 128:256] = im * tc - re * ts
        transform(at, len(values), fwd_ref)

    def from_spectrum(at, count):
        transform(at, count, back_ref)
        values = []
        for k in range(count):
            re = s_ref[at, SUBS * k : SUBS * (k + 1), 0:128]
            im = s_ref[at, SUBS * k : SUBS * (k + 1), 128:256]
            tc = tw_ref[0, k : k + 1, :]
            ts = tw_ref[1, k : k + 1, :]
            values.append((re * tc - im * ts, im * tc + re * ts))
        return values

    for c in range(plan.comps):
        values = [(in_ref[place[s], 2 * c], in_ref[place[s], 2 * c + 1] * keep) for s in range(n)]
        to_spectrum(complex_fft(values, -1), c)
    extra = []
    for s in range(n):
        e = in_ref[place[s], 1] * mask
        e = e + pltpu.roll(in_ref[place[s], 3] * mask, 1, 0)
        e = e + pltpu.roll(in_ref[place[s], 5] * mask, 2, 0)
        extra.append(e + pltpu.roll(e, 3, 0))
    extra = real_fft(extra)
    zero = jnp.zeros((SUBS, LANES), jnp.float32)
    extra[0] = (extra[0], zero)
    extra[-1] = (extra[-1], zero)
    to_spectrum(extra, 3)
    for k in range(n):
        rows = slice(SUBS * k, SUBS * (k + 1))
        t = [k_ref[i, k] for i in range(6)]
        for part in range(2):
            lanes = slice(LANES * part, LANES * (part + 1))
            a, b, g = (s_ref[c, rows, lanes] for c in range(3))
            s_ref[0, rows, lanes] = t[0] * a + t[3] * b + t[4] * g
            s_ref[1, rows, lanes] = t[3] * a + t[1] * b + t[5] * g
            s_ref[2, rows, lanes] = t[4] * a + t[5] * b + t[2] * g
            if k < half:
                d = [kx_ref[i, k] for i in range(3)]
                e = s_ref[3, rows, lanes]
                s_ref[3, rows, lanes] = (
                    d[0] * e + d[1] * pltpu.roll(e, 7, 0) + d[2] * pltpu.roll(e, 6, 0)
                )
    extra = from_spectrum(3, half)
    extra[0] = extra[0][0]
    extra[-1] = extra[-1][0]
    extra = real_ifft(extra)
    for s in range(n):
        b_ref[s] = extra[s]
    for c in range(plan.comps):
        values = complex_fft(from_spectrum(c, n), 1)
        for s in range(n):
            e = b_ref[s]
            if c:
                e = pltpu.roll(e, SUBS - c, 0)
            out_ref[place[s], 2 * c] = values[s][0]
            out_ref[place[s], 2 * c + 1] = values[s][1] * keep + e * mask


def finish_kernel(plan, *refs):
    chunks, refs = refs[: plan.planes], refs[plan.planes :]
    m_ref, applied_ref, pred_hbm, torque_hbm, *refs = refs
    field_ref, pred_ref, torque_ref, sem_out = refs
    me = plane_index()
    tiles = plan.lx * plan.ly // LANES
    for o in range(plan.planes):
        field_ref[pl.ds(plan.zc * (me ^ o), plan.zc), :] = chunks[o][...]
    stores = []
    scale = -1.0 / (1.0 + damping * damping)
    for t in range(tiles):
        h, m = [], []
        for c in range(3):
            at = (c * tiles + t) * LANES
            h.append(field_ref[:, at : at + LANES].T + applied_ref[c])
            m.append(m_ref[c, t])
        a = [m[1] * h[2] - m[2] * h[1], m[2] * h[0] - m[0] * h[2], m[0] * h[1] - m[1] * h[0]]
        b = [m[1] * a[2] - m[2] * a[1], m[2] * a[0] - m[0] * a[2], m[0] * a[1] - m[1] * a[0]]
        torque = [(a[c] + damping * b[c]) * scale for c in range(3)]
        step = [m[c] + time_step * torque[c] for c in range(3)]
        total = step[0] * step[0] + step[1] * step[1] + step[2] * step[2]
        inverse = lax.rsqrt(total)
        for c in range(3):
            torque_ref[c, t] = torque[c]
            pred_ref[c, t] = step[c] * inverse
        stores.append(fetch(torque_ref.at[:, t], torque_hbm.at[:, t], sem_out.at[0, t]))
        stores.append(fetch(pred_ref.at[:, t], pred_hbm.at[:, t], sem_out.at[1, t]))
    for store in stores:
        store.wait()


def lattice_eigen(wave_index, length):
    return 2.0 * jnp.cos(wave_index.astype(jnp.float32) * (2.0 * math.pi / length)) - 2.0


def tensor_pick_kernel(plan, k_hbm, own_ref, give_ref, k_ref, sem):
    parts = 6
    loads = [fetch(k_hbm.at[i], k_ref.at[i], sem.at[i]) for i in range(parts)]
    group = lax.axis_index("gx") * plan.cz + lax.axis_index("gz")
    low = lax.axis_index("gy") == 0
    sub = lax.broadcasted_iota(jnp.int32, (SUBS, k_ref.shape[3]), 0)
    top = sub == 0
    edge = jnp.zeros(sub.shape, jnp.float32)
    tile = lambda i, j, t: k_ref[i, j, SUBS * t : SUBS * (t + 1), :]
    for i in range(parts):
        loads[i].wait()
        edge = jnp.where(sub == i, pltpu.roll(tile(i, 0, 4), i, 0), edge)
        for j in range(4):
            far = 4 * group + j > plan.ny // 2
            values = [
                jnp.where(top & far, tile(i, j, 4), tile(i, j, 0)),
                tile(i, j, 2),
                jnp.where(top, tile(i, j, 1), tile(i, j, 4)),
                jnp.where(top, tile(i, j, 3), tile(i, j, 6)),
            ]
            for k2l in range(2):
                row = ((i * 4 + j) * 2 + k2l) * SUBS
                own_ref[row : row + SUBS, :] = jnp.where(low, values[k2l], values[2 + k2l])
                give_ref[row : row + SUBS, :] = jnp.where(low, values[2 + k2l], values[k2l])
    row = parts * 4 * 2 * SUBS
    own_ref[row : row + SUBS, :] = edge
    give_ref[row : row + SUBS, :] = edge


def tensor_pick(plan, kernel):
    rows = pltpu.VMEM((6 * 4 * 2 * SUBS + SUBS, kernel.shape[2]), jnp.float32)
    kt = jnp.swapaxes(kernel, 2, 3)
    return call(
        lambda *a: tensor_pick_kernel(plan, *a),
        "h",
        (rows, rows),
        [pltpu.VMEM(kt.shape, jnp.float32), pltpu.SemaphoreType.DMA((6,))],
    )(kt)


def field_tensor(plan, own, other):
    gx, gy, gz = (lax.axis_index(a) for a in ("gx", "gy", "gz"))
    group = gx * plan.cz + gz
    kzs = own.shape[1]
    other = lax.ppermute(other, "gy", [(0, 1), (1, 0)])
    own, other = own[None], other[None]
    got = jnp.where(gy == 0, jnp.concatenate([own, other]), jnp.concatenate([other, own]))
    main = got[:, : 6 * 4 * 2 * 8].reshape(2, 6, 2, 2, 2, 8, kzs // 32, 32)
    main = jnp.transpose(main, (1, 7, 3, 4, 2, 5, 0, 6)).reshape(6, 32, 8, 128)
    edge = got[:, 6 * 4 * 2 * 8 : 6 * 4 * 2 * 8 + 6].reshape(2, 6, kzs // 32, 32)
    edge = jnp.transpose(edge, (1, 3, 0, 2)).reshape(6, 32, plan.zc)
    kz = jnp.arange(plan.nz).reshape(plan.zc, 32).T
    table = np.array([[slot_kx(k2, s) for s in range(SLOTS)] for k2 in range(4)])
    table = table.reshape(2, 2, SLOTS).astype(np.int32)
    kx = jnp.where(gy == 0, table[0], table[1])
    kyq = (4 * group + 2 * jnp.arange(2)[None, :] + jnp.arange(2)[:, None])
    kx_full = jnp.broadcast_to(kx[None, :, None, :], (2, 2, 2, SLOTS))
    swap = (gy == 0) & (kyq > plan.ny // 2)
    is_packed = (jnp.arange(2)[None, :, None, None] == 0) & (jnp.arange(SLOTS) == 0)
    kx_full = jnp.where(is_packed & swap[:, None, :, None], 32, kx_full)
    ex = lattice_eigen(kx_full, plan.nx)
    ey = lattice_eigen(kyq, plan.ny)
    ez = lattice_eigen(kz, plan.nz)
    plane = (ex + ey[:, None, :, None]).reshape(8, SLOTS)
    eig = plane[None, :, :, None] + ez[:, None, None, :]
    eig = eig.reshape(32, 8, 128)
    scale = 1.0 / (plan.nx * plan.ny * plan.nz)
    diag = jnp.asarray([1, 1, 1, 0, 0, 0], jnp.float32)[:, None, None, None]
    tensor = scale * (exchange_coeff * diag * eig[None] - main)
    edge_eig = lattice_eigen(jnp.asarray(32), plan.nx) + lattice_eigen(4 * group, plan.ny) + ez
    edge = scale * (exchange_coeff * diag[:, :, :, 0] * edge_eig[None] - edge)
    order = ((0, 1, 2), (3, 5, 4), (4, 3, 5))
    edge = jnp.stack([jnp.stack([edge[i] for i in row]) for row in order])
    edge = jnp.transpose(edge, (0, 2, 1, 3))
    edge = jnp.pad(edge, ((0, 0), (0, 0), (0, 5), (0, LANES - plan.zc)))
    special = (gy == 0) & ((group == 0) | (group == plan.groups // 2))
    spot = (jnp.arange(8)[:, None] == 0) & (jnp.arange(LANES)[None, :] < plan.zc)
    mask = jnp.where(special & spot, 1.0, 0.0).astype(jnp.float32)
    return tensor, edge, mask


def call(body, places, outs, scratch):
    spaces = {"h": pltpu.HBM, "v": pltpu.VMEM, "s": pltpu.SMEM}

    def space_of(out):
        return pltpu.VMEM if isinstance(out, pl.MemoryRef) else pl.ANY

    step = pl.pallas_call(
        body,
        out_shape=outs,
        in_specs=[pl.BlockSpec(memory_space=spaces[p]) for p in places],
        out_specs=jax.tree.map(lambda o: pl.BlockSpec(memory_space=space_of(o)), outs),
        scratch_shapes=scratch,
        compiler_params=pltpu.CompilerParams(vmem_limit_bytes=8 * 2**20),
    )

    def run(*args):
        return step(
            *(
                x if p == "s" else pltpu.with_memory_space_constraint(x, spaces[p])
                for p, x in zip(places, args)
            )
        )

    return run


SEND_ORDER = (7, 4, 1, 5, 6, 3, 2)


def plane_swap(plan, chunks):
    members = range(plan.planes)
    out = list(chunks)
    for o in SEND_ORDER:
        out[o] = lax.ppermute(chunks[o], ("gx", "gy"), [(k, k ^ o) for k in members])
    return out


def on_chip(like, *tables):
    there = like > -1e30
    return [jnp.where(there, t, jnp.zeros((), t.dtype)) for t in tables]


def fast_shards(plan, magnetization, kernel, applied):
    f32, bf16 = jnp.float32, jnp.bfloat16
    sds, vmem, dma = jax.ShapeDtypeStruct, pltpu.VMEM, pltpu.SemaphoreType.DMA
    n, zc, planes = plan.devices, plan.zc, plan.planes
    width = 3 * plan.lx * plan.ly
    tiles = width // LANES
    fwd, back = xy_tables(plan)
    fwd = [split_table(t, 2) for t in (fwd[:, :, 0:256], fwd[:, :, 256:512])]
    back = [split_table(t, 1) for t in (back[:, :, 0:256], back[:, :, 256:512])]
    zf, zb = z_tables(plan)
    zf, zb = split_table(zf, 0), split_table(zb, 0)
    chunk = vmem((zc, width), f32)
    spectrum = (n, 6, SUBS, LANES)
    m_tiles = magnetization.reshape(tiles, LANES, LANES)
    packed = call(
        lambda *a: pack_kernel(plan, *a),
        "h",
        [chunk] * planes,
        [vmem((tiles, LANES, LANES), f32), vmem((plan.lz, width), f32), dma((3,))],
    )(m_tiles)
    late = lax.axis_index("gy").astype(f32)
    first, kernel, late = lax.optimization_barrier((packed[0], kernel, late))
    packed = [first, *packed[1:]]
    own, other = tensor_pick(plan, kernel)
    fwd = on_chip(late, *fwd)
    tensor, edge, mask = field_tensor(plan, own, other)
    zf, zb = on_chip(tensor[0, 0, 0, 0], zf, zb)
    lines = plane_swap(plan, packed)
    spec = call(
        lambda *a: xy_forward_kernel(plan, *a),
        "v" * planes + "vv",
        vmem(spectrum, f32),
        [
            vmem((planes, zc, width), f32),
            vmem((2, 3, LANES, 512), bf16),
            vmem((2, LANES, 512), bf16),
            vmem((2, SUBS, LANES), f32),
        ],
    )(*lines, *fwd)
    spec = lax.all_to_all(spec, ("gx", "gy", "gz"), split_axis=0, concat_axis=0, tiled=True)
    spec = call(
        lambda *a: z_kernel(plan, *a),
        "vvvvvv",
        vmem(spectrum, f32),
        [
            vmem((4, n * SUBS, 256), f32),
            vmem((n, SUBS, LANES), f32),
            vmem((2, n, LANES), f32),
        ],
    )(spec, tensor, edge, mask, zf, zb)
    spec = lax.all_to_all(spec, ("gx", "gy", "gz"), split_axis=0, concat_axis=0, tiled=True)
    field = call(
        lambda *a: xy_inverse_kernel(plan, *a),
        "vvv",
        [chunk] * planes,
        [
            vmem((3, 2, 256, LANES), f32),
            vmem((2, 3 * LANES, 512), bf16),
            vmem((2, 3 * LANES, 256), f32),
            vmem((planes, zc, width), f32),
            vmem((2, SUBS, LANES), f32),
        ],
    )(spec, *back)
    field = plane_swap(plan, field)
    cells = (3, tiles // 3, LANES, LANES)
    pred, torque = call(
        lambda *a: finish_kernel(plan, *a),
        "v" * planes + "vs",
        (sds(cells, f32), sds(cells, f32)),
        [
            vmem((plan.lz, width), f32),
            vmem(cells, f32),
            vmem(cells, f32),
            dma((2, tiles // 3)),
        ],
    )(*field, magnetization.reshape(cells), applied)
    return pred.reshape(magnetization.shape), torque.reshape(magnetization.shape)


def solution(mesh):
    sizes = mesh.shape

    def shards(magnetization, kernel, applied):
        plan = Plan(sizes["gx"], sizes["gy"], sizes["gz"], magnetization.shape)
        if plan.fits():
            return fast_shards(plan, magnetization, kernel, applied)
        return general_shards(magnetization, kernel, applied)

    return jax.shard_map(
        shards,
        mesh=mesh,
        in_specs=(P(None, "gx", "gy", "gz"), P(None, ("gx", "gz"), "gy", None), P()),
        out_specs=(P(None, "gx", "gy", "gz"), P(None, "gx", "gy", "gz")),
        check_vma=False,
    )
```

```python
import math

import jax
import jax.numpy as jnp
import numpy as np
from jax import lax
from jax.experimental import pallas as pl
from jax.experimental.pallas import tpu as pltpu
from jax.sharding import PartitionSpec as P


exchange_coeff = 1.0
damping = 0.3
time_step = 0.2
highest = lax.Precision.HIGHEST
LANES = 128
SUBS = 8
SLOTS = 8


def phase_table(row_index, col_index, length):
    product = row_index[:, None] * col_index[None, :] % length
    angles = product.astype(jnp.float32) * (2.0 * math.pi / length)
    return (jnp.cos(angles), jnp.sin(angles))


def forward_mix(real_part, imag_part, cosine_table, sine_table, pattern):
    real_out = jnp.einsum(pattern, real_part, cosine_table, precision=highest) + jnp.einsum(
        pattern, imag_part, sine_table, precision=highest
    )
    imag_out = jnp.einsum(pattern, imag_part, cosine_table, precision=highest) - jnp.einsum(
        pattern, real_part, sine_table, precision=highest
    )
    return (real_out, imag_out)


def inverse_mix(real_part, imag_part, cosine_table, sine_table, pattern):
    real_out = jnp.einsum(pattern, real_part, cosine_table, precision=highest) - jnp.einsum(
        pattern, imag_part, sine_table, precision=highest
    )
    imag_out = jnp.einsum(pattern, imag_part, cosine_table, precision=highest) + jnp.einsum(
        pattern, real_part, sine_table, precision=highest
    )
    return (real_out, imag_out)


def apply_tensor(kernel, spectrum):
    return jnp.stack(
        [
            kernel[0] * spectrum[0] + kernel[3] * spectrum[1] + kernel[4] * spectrum[2],
            kernel[3] * spectrum[0] + kernel[1] * spectrum[1] + kernel[5] * spectrum[2],
            kernel[4] * spectrum[0] + kernel[5] * spectrum[1] + kernel[2] * spectrum[2],
        ]
    )


def cross_product(first_vec, second_vec):
    return jnp.stack(
        [
            first_vec[1] * second_vec[2] - first_vec[2] * second_vec[1],
            first_vec[2] * second_vec[0] - first_vec[0] * second_vec[2],
            first_vec[0] * second_vec[1] - first_vec[1] * second_vec[0],
        ]
    )


def general_shards(magnetization, kernel, applied):
    count_gx = lax.axis_size("gx")
    count_gy = lax.axis_size("gy")
    count_gz = lax.axis_size("gz")
    local_x = magnetization.shape[1]
    local_y = magnetization.shape[2]
    local_z = magnetization.shape[3]
    full_x = local_x * count_gx
    full_y = local_y * count_gy
    full_z = local_z * count_gz
    part_x = local_x // count_gz
    part_y = full_y // (count_gx * count_gz)
    part_z = full_z // count_gy
    outside = applied[:, None, None, None]
    z_index = jnp.arange(full_z, dtype=jnp.int32)
    weights = jnp.ones((full_z,), jnp.float32)
    planes = z_index.shape[0] // count_gy
    wave_count = z_index.shape[0]
    zlines = lax.all_to_all(magnetization, "gz", split_axis=1, concat_axis=3, tiled=True)
    cos_zf, sin_zf = phase_table(z_index, z_index, full_z)
    cos_zb, sin_zb = phase_table(z_index, z_index, full_z)
    cos_zb = cos_zb * weights[:, None]
    sin_zb = sin_zb * weights[:, None]
    lines_shape = (3, part_x, local_y, full_z)
    wave_shape = (3, part_x, local_y, wave_count)
    z_rows = zlines.reshape(-1, full_z)
    spec_real = jnp.dot(z_rows, cos_zf, precision=highest).reshape(wave_shape)
    spec_imag = -jnp.dot(z_rows, sin_zf, precision=highest).reshape(wave_shape)
    spec_real, spec_imag = (
        lax.all_to_all(spec_real, "gy", split_axis=3, concat_axis=2, tiled=True),
        lax.all_to_all(spec_imag, "gy", split_axis=3, concat_axis=2, tiled=True),
    )
    y_index = jnp.arange(full_y, dtype=jnp.int32)
    cos_y, sin_y = phase_table(y_index, y_index, full_y)
    spec_real, spec_imag = forward_mix(spec_real, spec_imag, cos_y, sin_y, "cxyz,yk->ckxz")
    x_index = jnp.arange(full_x, dtype=jnp.int32)
    cos_xn, sin_xn = phase_table(x_index, x_index, full_x)
    spec_real, spec_imag = (
        lax.all_to_all(spec_real, ("gx", "gz"), split_axis=1, concat_axis=2, tiled=True),
        lax.all_to_all(spec_imag, ("gx", "gz"), split_axis=1, concat_axis=2, tiled=True),
    )
    cos_x, sin_x = (cos_xn, sin_xn)
    spec_real, spec_imag = forward_mix(spec_real, spec_imag, cos_x, sin_x, "cyxz,xk->cyzk")
    inverse_count = 1.0 / (full_x * full_y * full_z)
    out_real = -inverse_count * apply_tensor(kernel, spec_real)
    out_imag = -inverse_count * apply_tensor(kernel, spec_imag)
    wave_y = (lax.axis_index("gx") * count_gz + lax.axis_index("gz")) * part_y + jnp.arange(
        part_y, dtype=jnp.int32
    )
    wave_z = lax.axis_index("gy") * part_z + jnp.arange(planes, dtype=jnp.int32)
    eigenvalue = (
        lattice_eigen(wave_y, full_y)[:, None, None]
        + lattice_eigen(wave_z, full_z)[None, :, None]
        + lattice_eigen(x_index, full_x)[None, None, :]
    )
    factor = inverse_count * exchange_coeff * eigenvalue
    out_real = out_real + factor * spec_real
    out_imag = out_imag + factor * spec_imag
    back_real, back_imag = inverse_mix(out_real, out_imag, cos_xn, sin_xn, "cyzk,kx->cyxz")
    back_real, back_imag = (
        lax.all_to_all(back_real, ("gx", "gz"), split_axis=2, concat_axis=1, tiled=True),
        lax.all_to_all(back_imag, ("gx", "gz"), split_axis=2, concat_axis=1, tiled=True),
    )
    cos_yb, sin_yb = (cos_y, sin_y)
    back_real, back_imag = inverse_mix(back_real, back_imag, cos_yb, sin_yb, "cyxz,yn->cxnz")
    back_real, back_imag = (
        lax.all_to_all(back_real, "gy", split_axis=2, concat_axis=3, tiled=True),
        lax.all_to_all(back_imag, "gy", split_axis=2, concat_axis=3, tiled=True),
    )
    real_rows = back_real.reshape(-1, wave_count)
    imag_rows = back_imag.reshape(-1, wave_count)
    field_lines = (
        jnp.dot(real_rows, cos_zb, precision=highest)
        - jnp.dot(imag_rows, sin_zb, precision=highest)
    ).reshape(lines_shape)
    field_block = lax.all_to_all(field_lines, "gz", split_axis=3, concat_axis=1, tiled=True)
    total_field = field_block + outside
    precess = cross_product(magnetization, total_field)
    double_twist = cross_product(magnetization, precess)
    torque = -(precess + damping * double_twist) / (1.0 + damping * damping)
    stepped = magnetization + time_step * torque
    length = jnp.sqrt(jnp.sum(stepped * stepped, axis=0))
    return (stepped / length, torque)


def cmul_const(value, angle):
    re, im = value
    quarter = angle / (math.pi / 2)
    if abs(quarter - round(quarter)) < 1e-9:
        turn = round(quarter) % 4
        if turn == 0:
            return (re, im)
        if turn == 1:
            return (-im, re)
        if turn == 2:
            return (-re, -im)
        return (im, -re)
    c, s = math.cos(angle), math.sin(angle)
    if abs(abs(c) - abs(s)) < 1e-9:
        h = abs(c)
        sc, ss = math.copysign(1, c), math.copysign(1, s)
        first = re if sc > 0 else -re
        out_re = (first - im) if ss > 0 else (first + im)
        second = im if sc > 0 else -im
        out_im = (second + re) if ss > 0 else (second - re)
        return (h * out_re, h * out_im)
    return (c * re - s * im, c * im + s * re)


def cadd(a, b):
    return (a[0] + b[0], a[1] + b[1])


def csub(a, b):
    return (a[0] - b[0], a[1] - b[1])


def conj(a):
    return (a[0], -a[1])


def complex_fft(values, sign):
    n = len(values)
    if n == 1:
        return values
    even = complex_fft(values[0::2], sign)
    odd = complex_fft(values[1::2], sign)
    odd = [cmul_const(v, sign * 2 * math.pi * k / n) for k, v in enumerate(odd)]
    return [cadd(e, o) for e, o in zip(even, odd)] + [csub(e, o) for e, o in zip(even, odd)]


def real_fft(values):
    n = len(values)
    if n == 2:
        return [values[0] + values[1], values[0] - values[1]]
    even = real_fft(values[0::2])
    odd = real_fft(values[1::2])
    quarter = n // 4
    out = [None] * (n // 2 + 1)
    out[0] = even[0] + odd[0]
    out[n // 2] = even[0] - odd[0]
    for k in range(1, quarter):
        turned = cmul_const(odd[k], -2 * math.pi * k / n)
        out[k] = cadd(even[k], turned)
        out[n // 2 - k] = conj(csub(even[k], turned))
    out[quarter] = (even[quarter], -odd[quarter])
    return out


def real_ifft(values):
    n = 2 * (len(values) - 1)
    if n == 2:
        return [values[0] + values[1], values[0] - values[1]]
    quarter = n // 4
    even = [None] * (quarter + 1)
    odd = [None] * (quarter + 1)
    even[0] = values[0] + values[n // 2]
    odd[0] = values[0] - values[n // 2]
    for k in range(1, quarter):
        mirror = conj(values[n // 2 - k])
        even[k] = cadd(values[k], mirror)
        odd[k] = cmul_const(csub(values[k], mirror), 2 * math.pi * k / n)
    mid = values[quarter]
    even[quarter] = 2.0 * mid[0]
    odd[quarter] = -2.0 * mid[1]
    even = real_ifft(even)
    odd = real_ifft(odd)
    out = [None] * n
    out[0::2] = even
    out[1::2] = odd
    return out


def split(value):
    high = value.astype(jnp.bfloat16)
    return high, (value - high.astype(jnp.float32)).astype(jnp.bfloat16)


def split_table(table, axis):
    high = table.astype(jnp.bfloat16)
    low = (table - high.astype(np.float32)).astype(jnp.bfloat16)
    return np.concatenate([high, low], axis)


def high_high_low(value):
    return jnp.concatenate([value[:, 0:256], value[:, 0:256], value[:, 256:512]], 1)


def high_low_high(table, axis):
    high, low = (lax.slice_in_dim(table, at, at + 256, axis=axis) for at in (0, 256))
    return jnp.concatenate([high, low, high], axis)


def mm(a, b, dims):
    return lax.dot_general(a, b, (dims, ((), ())), preferred_element_type=jnp.float32)


class Plan:
    def __init__(self, cx, cy, cz, shape):
        comps, lx, ly, lz = shape
        self.comps, self.lx, self.ly, self.lz = comps, lx, ly, lz
        self.cx, self.cy, self.cz = cx, cy, cz
        self.nx, self.ny, self.nz = lx * cx, ly * cy, lz * cz
        self.planes = cx * cy
        self.groups = cx * cz
        self.devices = cx * cy * cz

    def fits(self):
        if self.devices % 1 or self.lz % self.planes:
            return False
        self.zc = self.lz // self.planes
        self.xl = LANES // self.ly if LANES % self.ly == 0 else 0
        return (
            self.comps == 3
            and self.xl == 4
            and self.cy == 2
            and self.nx == 16 * self.xl
            and self.lx % self.xl == 0
            and self.ly == 2 * self.groups
            and self.zc * SLOTS == LANES
            and self.lz == LANES
            and self.nz % self.zc == 0
        )


def slot_kx(kx2, slot):
    if slot:
        return slot + 16 * kx2
    return (0, 16, 8, 24)[kx2]


def xy_tables(plan):
    lane = np.arange(LANES)
    xl, yl = lane // plan.ly, lane % plan.ly
    half = plan.ny // 2
    fwd = np.zeros((2, 256, 512))
    back = np.zeros((2, 256, 512))
    for r in range(2):
        for k2h in range(2):
            for g in range(plan.groups):
                for ri in range(2):
                    for k2l in range(2):
                        for ql in range(2):
                            block = ri if r == 0 else 1 - ri
                            f = (k2h * plan.groups + g) * 8 + block * 4 + k2l * 2 + ql
                            kx2 = 2 * k2h + k2l
                            ky = 2 * (2 * g + ql) + r
                            ph = 2 * math.pi * (xl * kx2 / 4 + yl * ky / plan.ny)
                            c, s = np.cos(ph), np.sin(ph)
                            if ri == 0:
                                fwd[r, f, 0:128], fwd[r, f, 128:256] = c, s
                                back[r, f, 0:128], back[r, f, 128:256] = c, s
                            else:
                                fwd[r, f, 0:128], fwd[r, f, 128:256] = -s, c
                                back[r, f, 0:128], back[r, f, 128:256] = -s, c
                            kx = slot_kx(kx2, 0)
                            if kx2 == 0:
                                edge = ky in (0, half)
                                if edge:
                                    kx = 0 if ri == 0 else 32
                                else:
                                    kx = 0 if ky < half else 32
                            ph = 2 * math.pi * (xl * kx / plan.nx + yl * ky / plan.ny)
                            c, s = np.cos(ph), np.sin(ph)
                            at = 256 if kx % 16 == 0 else 384
                            if kx2 == 0 and edge:
                                fwd[r, f, at : at + 128] = c
                                back[r, f, at : at + 128] = c
                            else:
                                fwd[r, f, at : at + 128] = c if ri == 0 else -s
                                back[r, f, at : at + 128] = 2 * (c if ri == 0 else -s)
    return fwd.astype(np.float32), back.astype(np.float32)


def fill_twiddles(ref, rows, lane_index, length):
    row = lax.broadcasted_iota(jnp.int32, (rows, LANES), 0)
    angle = (row * lane_index).astype(jnp.float32) * (2 * math.pi / length)
    ref[0] = jnp.cos(angle)
    ref[1] = jnp.sin(angle)


def fill_x_twiddles(plan, ref):
    lane = lax.broadcasted_iota(jnp.int32, (SUBS, LANES), 1)
    fill_twiddles(ref, SUBS, lane // plan.ly, plan.nx)


def z_tables(plan):
    zc = plan.zc
    small = 2 * math.pi * np.arange(zc)[:, None] * np.arange(zc)[None, :] / zc
    c = np.kron(np.eye(SLOTS), np.cos(small))
    s = np.kron(np.eye(SLOTS), np.sin(small))
    fwd = np.block([[c, -s], [s, c]]).astype(np.float32)
    back = np.block([[c, s], [-s, c]]).astype(np.float32)
    return fwd, back


def fetch(source, target, sem):
    copy = pltpu.make_async_copy(source, target, sem)
    copy.start()
    return copy


def plane_index():
    return lax.axis_index("gx") * lax.axis_size("gy") + lax.axis_index("gy")


def pack_kernel(plan, m_ref, *rest):
    outs, (m_buf, buf, sem_in) = rest[: plan.planes], rest[plan.planes :]
    me = plane_index()
    per = plan.lx * plan.ly // LANES
    width = per * LANES
    loads = [
        fetch(m_ref.at[pl.ds(c * per, per)], m_buf.at[pl.ds(c * per, per)], sem_in.at[c])
        for c in range(plan.comps)
    ]
    for c in range(plan.comps):
        loads[c].wait()
        for t in range(c * per, (c + 1) * per):
            buf[:, LANES * t : LANES * (t + 1)] = m_buf[t].T
        for o in range(plan.planes):
            rows = pl.ds(plan.zc * (me ^ o), plan.zc)
            cols = slice(width * c, width * (c + 1))
            outs[o][:, cols] = buf[rows, cols]


def xy_forward_kernel(plan, *refs):
    chunks, refs = refs[: plan.planes], refs[plan.planes :]
    table_ref, edge_ref, out_hbm, lines_ref, g_ref, e_ref, tw_ref, out_ref, sem = refs
    stores = []
    me = plane_index()
    fill_x_twiddles(plan, tw_ref)
    for o in range(plan.planes):
        lines_ref[me ^ o] = chunks[o][...]
    zc = plan.zc
    per = plan.lx // plan.xl
    low = lax.broadcasted_iota(jnp.int32, (SUBS, LANES), 0) < 4
    first_slot = lax.broadcasted_iota(jnp.int32, (SUBS, LANES), 1) < zc
    blank = jnp.zeros((zc, LANES), jnp.bfloat16)
    for r in range(2):
        for k in range(plan.comps, SLOTS):
            for q in range(4):
                e_ref[r, zc * k : zc * (k + 1), LANES * q : LANES * (q + 1)] = blank

    def keep(ref, at, rows, parts):
        for q, part in enumerate(parts):
            hi, lo = split(part)
            ref[(*at, rows, slice(LANES * q, LANES * (q + 1)))] = hi
            ref[(*at, rows, slice(LANES * (q + 2), LANES * (q + 3)))] = lo

    for c in range(plan.comps):
        parts = [[], []]
        for gx in range(plan.cx):
            for xh in range(per):
                at = c * (plan.lx * plan.ly) + xh * LANES
                first = lines_ref[gx * 2, :, at : at + LANES]
                second = lines_ref[gx * 2 + 1, :, at : at + LANES]
                parts[0].append(first + second)
                parts[1].append(first - second)
        for r in range(2):
            spec = real_fft(parts[r])
            keep(e_ref, (r,), slice(zc * c, zc * (c + 1)), (spec[0], spec[8]))
            for k in range(1, SLOTS):
                re, im = spec[k]
                tc = tw_ref[0, k : k + 1, :]
                ts = tw_ref[1, k : k + 1, :]
                rows = slice(zc * k, zc * (k + 1))
                keep(g_ref, (r, c), rows, (re * tc + im * ts, im * tc - re * ts))
            g_ref[r, c, 0:zc, :] = jnp.zeros((zc, 512), jnp.bfloat16)

    edges = [mm(high_low_high(edge_ref[r], 1), high_high_low(e_ref[r]), ((1,), (1,))) for r in range(2)]
    for c in range(plan.comps):
        outs = [
            mm(high_low_high(table_ref[r], 1), high_high_low(g_ref[r, c]), ((1,), (1,)))
            for r in range(2)
        ]
        for k2h in range(2):
            for g in range(plan.groups):
                f = (k2h * plan.groups + g) * SUBS
                both = []
                for r in range(2):
                    edge = edges[r][f : f + SUBS]
                    if c:
                        edge = pltpu.roll(edge, LANES - zc * c, 1)
                    both.append(jnp.where(first_slot, edge, outs[r][f : f + SUBS]))
                one, two = both
                gx, gz = g // plan.cz, g % plan.cz
                dest = (gx * plan.cy + k2h) * plan.cz + gz
                out_ref[dest, 2 * c] = jnp.where(low, one, two)
                out_ref[dest, 2 * c + 1] = pltpu.roll(jnp.where(low, two, one), 4, 0)
        pair = pl.ds(2 * c, 2)
        stores.append(fetch(out_ref.at[:, pair], out_hbm.at[:, pair], sem.at[c]))
    for store in stores:
        store.wait()


def xy_inverse_kernel(plan, spec_ref, table_ref, edge_ref, *refs):
    outs, (h_ref, t_ref, u_ref, out_ref, tw_ref) = refs[: plan.planes], refs[plan.planes :]
    me = plane_index()
    fill_x_twiddles(plan, tw_ref)
    zc = plan.zc
    per = plan.lx // plan.xl
    low = lax.broadcasted_iota(jnp.int32, (SUBS, LANES), 0) < 4
    for c in range(plan.comps):
        for k2h in range(2):
            for g in range(plan.groups):
                f = (k2h * plan.groups + g) * SUBS
                gx, gz = g // plan.cz, g % plan.cz
                src = (gx * plan.cy + k2h) * plan.cz + gz
                re = spec_ref[src, 2 * c]
                im = pltpu.roll(spec_ref[src, 2 * c + 1], 4, 0)
                h_ref[c, 0, f : f + SUBS, :] = jnp.where(low, re, im)
                h_ref[c, 1, f : f + SUBS, :] = jnp.where(low, im, re)
        for r in range(2):
            hi, lo = split(h_ref[c, r].T)
            t_ref[r, LANES * c : LANES * (c + 1), 0:256] = hi
            t_ref[r, LANES * c : LANES * (c + 1), 256:512] = lo

    edges = []
    for r in range(2):
        u_ref[r] = mm(high_high_low(t_ref[r]), high_low_high(table_ref[r], 0), ((1,), (0,)))
        rows = jnp.concatenate(
            [t_ref[r, LANES * c : LANES * c + zc, :] for c in range(plan.comps)], 0
        )
        edges.append(mm(high_high_low(rows), high_low_high(edge_ref[r], 0), ((1,), (0,))))
    for c in range(plan.comps):
        fields = []
        for r in range(2):
            edge = edges[r][zc * c : zc * (c + 1)]
            values = [edge[:, 0:128]]
            for k in range(1, SLOTS):
                rows = slice(LANES * c + zc * k, LANES * c + zc * (k + 1))
                re = u_ref[r, rows, 0:128]
                im = u_ref[r, rows, 128:256]
                tc = tw_ref[0, k : k + 1, :]
                ts = tw_ref[1, k : k + 1, :]
                values.append((re * tc - im * ts, im * tc + re * ts))
            values.append(edge[:, 128:256])
            fields.append(real_ifft(values))
        for gx in range(plan.cx):
            for xh in range(per):
                at = c * (plan.lx * plan.ly) + xh * LANES
                one = fields[0][gx * per + xh]
                two = fields[1][gx * per + xh]
                out_ref[gx * 2, :, at : at + LANES] = one + two
                out_ref[gx * 2 + 1, :, at : at + LANES] = one - two
    for o in range(plan.planes):
        outs[o][...] = out_ref[me ^ o]


def z_kernel(
    plan, in_ref, k_ref, kx_ref, mask_ref, fwd_ref, back_ref, out_ref, s_ref, b_ref, tw_ref
):
    n = plan.devices
    lane = lax.broadcasted_iota(jnp.int32, (n, LANES), 1)
    fill_twiddles(tw_ref, n, lane % plan.zc, plan.nz)
    half = n // 2 + 1
    mask = mask_ref[...]
    place = [(s % plan.planes) * plan.cz + s // plan.planes for s in range(n)]
    keep = 1.0 - mask

    def transform(at, count, table):
        hi, lo = split(s_ref[at, 0 : SUBS * count, :])
        wide = jnp.concatenate([hi, hi, lo], 1)
        s_ref[at, 0 : SUBS * count, :] = mm(wide, high_low_high(table[...], 0), ((1,), (0,)))

    def to_spectrum(values, at):
        for k, (re, im) in enumerate(values):
            tc = tw_ref[0, k : k + 1, :]
            ts = tw_ref[1, k : k + 1, :]
            s_ref[at, SUBS * k : SUBS * (k + 1), 0:128] = re * tc + im * ts
            s_ref[at, SUBS * k : SUBS * (k + 1), 128:256] = im * tc - re * ts
        transform(at, len(values), fwd_ref)

    def from_spectrum(at, count):
        transform(at, count, back_ref)
        values = []
        for k in range(count):
            re = s_ref[at, SUBS * k : SUBS * (k + 1), 0:128]
            im = s_ref[at, SUBS * k : SUBS * (k + 1), 128:256]
            tc = tw_ref[0, k : k + 1, :]
            ts = tw_ref[1, k : k + 1, :]
            values.append((re * tc - im * ts, im * tc + re * ts))
        return values

    for c in range(plan.comps):
        values = [(in_ref[place[s], 2 * c], in_ref[place[s], 2 * c + 1] * keep) for s in range(n)]
        to_spectrum(complex_fft(values, -1), c)
    extra = []
    for s in range(n):
        e = in_ref[place[s], 1] * mask
        e = e + pltpu.roll(in_ref[place[s], 3] * mask, 1, 0)
        e = e + pltpu.roll(in_ref[place[s], 5] * mask, 2, 0)
        extra.append(e + pltpu.roll(e, 3, 0))
    extra = real_fft(extra)
    zero = jnp.zeros((SUBS, LANES), jnp.float32)
    extra[0] = (extra[0], zero)
    extra[-1] = (extra[-1], zero)
    to_spectrum(extra, 3)
    for k in range(n):
        rows = slice(SUBS * k, SUBS * (k + 1))
        t = [k_ref[i, k] for i in range(6)]
        for part in range(2):
            lanes = slice(LANES * part, LANES * (part + 1))
            a, b, g = (s_ref[c, rows, lanes] for c in range(3))
            s_ref[0, rows, lanes] = t[0] * a + t[3] * b + t[4] * g
            s_ref[1, rows, lanes] = t[3] * a + t[1] * b + t[5] * g
            s_ref[2, rows, lanes] = t[4] * a + t[5] * b + t[2] * g
            if k < half:
                d = [kx_ref[i, k] for i in range(3)]
                e = s_ref[3, rows, lanes]
                s_ref[3, rows, lanes] = (
                    d[0] * e + d[1] * pltpu.roll(e, 7, 0) + d[2] * pltpu.roll(e, 6, 0)
                )
    extra = from_spectrum(3, half)
    extra[0] = extra[0][0]
    extra[-1] = extra[-1][0]
    extra = real_ifft(extra)
    for s in range(n):
        b_ref[s] = extra[s]
    for c in range(plan.comps):
        values = complex_fft(from_spectrum(c, n), 1)
        for s in range(n):
            e = b_ref[s]
            if c:
                e = pltpu.roll(e, SUBS - c, 0)
            out_ref[place[s], 2 * c] = values[s][0]
            out_ref[place[s], 2 * c + 1] = values[s][1] * keep + e * mask


def finish_kernel(plan, *refs):
    chunks, refs = refs[: plan.planes], refs[plan.planes :]
    m_ref, applied_ref, pred_hbm, torque_hbm, *refs = refs
    field_ref, pred_ref, torque_ref, sem_out = refs
    me = plane_index()
    tiles = plan.lx * plan.ly // LANES
    for o in range(plan.planes):
        field_ref[pl.ds(plan.zc * (me ^ o), plan.zc), :] = chunks[o][...]
    stores = []
    scale = -1.0 / (1.0 + damping * damping)
    for t in range(tiles):
        h, m = [], []
        for c in range(3):
            at = (c * tiles + t) * LANES
            h.append(field_ref[:, at : at + LANES].T + applied_ref[c])
            m.append(m_ref[c, t])
        a = [m[1] * h[2] - m[2] * h[1], m[2] * h[0] - m[0] * h[2], m[0] * h[1] - m[1] * h[0]]
        b = [m[1] * a[2] - m[2] * a[1], m[2] * a[0] - m[0] * a[2], m[0] * a[1] - m[1] * a[0]]
        torque = [(a[c] + damping * b[c]) * scale for c in range(3)]
        step = [m[c] + time_step * torque[c] for c in range(3)]
        total = step[0] * step[0] + step[1] * step[1] + step[2] * step[2]
        inverse = lax.rsqrt(total)
        for c in range(3):
            torque_ref[c, t] = torque[c]
            pred_ref[c, t] = step[c] * inverse
        stores.append(fetch(torque_ref.at[:, t], torque_hbm.at[:, t], sem_out.at[0, t]))
        stores.append(fetch(pred_ref.at[:, t], pred_hbm.at[:, t], sem_out.at[1, t]))
    for store in stores:
        store.wait()


def lattice_eigen(wave_index, length):
    return 2.0 * jnp.cos(wave_index.astype(jnp.float32) * (2.0 * math.pi / length)) - 2.0


def tensor_pick_kernel(plan, k_hbm, own_ref, give_ref, k_ref, sem):
    parts = 6
    loads = [fetch(k_hbm.at[i], k_ref.at[i], sem.at[i]) for i in range(parts)]
    group = lax.axis_index("gx") * plan.cz + lax.axis_index("gz")
    low = lax.axis_index("gy") == 0
    sub = lax.broadcasted_iota(jnp.int32, (SUBS, k_ref.shape[3]), 0)
    top = sub == 0
    edge = jnp.zeros(sub.shape, jnp.float32)
    tile = lambda i, j, t: k_ref[i, j, SUBS * t : SUBS * (t + 1), :]
    for i in range(parts):
        loads[i].wait()
        edge = jnp.where(sub == i, pltpu.roll(tile(i, 0, 4), i, 0), edge)
        for j in range(4):
            far = 4 * group + j > plan.ny // 2
            values = [
                jnp.where(top & far, tile(i, j, 4), tile(i, j, 0)),
                tile(i, j, 2),
                jnp.where(top, tile(i, j, 1), tile(i, j, 4)),
                jnp.where(top, tile(i, j, 3), tile(i, j, 6)),
            ]
            for k2l in range(2):
                row = ((i * 4 + j) * 2 + k2l) * SUBS
                own_ref[row : row + SUBS, :] = jnp.where(low, values[k2l], values[2 + k2l])
                give_ref[row : row + SUBS, :] = jnp.where(low, values[2 + k2l], values[k2l])
    row = parts * 4 * 2 * SUBS
    own_ref[row : row + SUBS, :] = edge
    give_ref[row : row + SUBS, :] = edge


def tensor_pick(plan, kernel):
    rows = pltpu.VMEM((6 * 4 * 2 * SUBS + SUBS, kernel.shape[2]), jnp.float32)
    kt = jnp.swapaxes(kernel, 2, 3)
    return call(
        lambda *a: tensor_pick_kernel(plan, *a),
        "h",
        (rows, rows),
        [pltpu.VMEM(kt.shape, jnp.float32), pltpu.SemaphoreType.DMA((6,))],
    )(kt)


def field_tensor(plan, own, other):
    gx, gy, gz = (lax.axis_index(a) for a in ("gx", "gy", "gz"))
    group = gx * plan.cz + gz
    kzs = own.shape[1]
    other = lax.ppermute(other, "gy", [(0, 1), (1, 0)])
    own, other = own[None], other[None]
    got = jnp.where(gy == 0, jnp.concatenate([own, other]), jnp.concatenate([other, own]))
    main = got[:, : 6 * 4 * 2 * 8].reshape(2, 6, 2, 2, 2, 8, kzs // 32, 32)
    main = jnp.transpose(main, (1, 7, 3, 4, 2, 5, 0, 6)).reshape(6, 32, 8, 128)
    edge = got[:, 6 * 4 * 2 * 8 : 6 * 4 * 2 * 8 + 6].reshape(2, 6, kzs // 32, 32)
    edge = jnp.transpose(edge, (1, 3, 0, 2)).reshape(6, 32, plan.zc)
    kz = jnp.arange(plan.nz).reshape(plan.zc, 32).T
    table = np.array([[slot_kx(k2, s) for s in range(SLOTS)] for k2 in range(4)])
    table = table.reshape(2, 2, SLOTS).astype(np.int32)
    kx = jnp.where(gy == 0, table[0], table[1])
    kyq = (4 * group + 2 * jnp.arange(2)[None, :] + jnp.arange(2)[:, None])
    kx_full = jnp.broadcast_to(kx[None, :, None, :], (2, 2, 2, SLOTS))
    swap = (gy == 0) & (kyq > plan.ny // 2)
    is_packed = (jnp.arange(2)[None, :, None, None] == 0) & (jnp.arange(SLOTS) == 0)
    kx_full = jnp.where(is_packed & swap[:, None, :, None], 32, kx_full)
    ex = lattice_eigen(kx_full, plan.nx)
    ey = lattice_eigen(kyq, plan.ny)
    ez = lattice_eigen(kz, plan.nz)
    plane = (ex + ey[:, None, :, None]).reshape(8, SLOTS)
    eig = plane[None, :, :, None] + ez[:, None, None, :]
    eig = eig.reshape(32, 8, 128)
    scale = 1.0 / (plan.nx * plan.ny * plan.nz)
    diag = jnp.asarray([1, 1, 1, 0, 0, 0], jnp.float32)[:, None, None, None]
    tensor = scale * (exchange_coeff * diag * eig[None] - main)
    edge_eig = lattice_eigen(jnp.asarray(32), plan.nx) + lattice_eigen(4 * group, plan.ny) + ez
    edge = scale * (exchange_coeff * diag[:, :, :, 0] * edge_eig[None] - edge)
    order = ((0, 1, 2), (3, 5, 4), (4, 3, 5))
    edge = jnp.stack([jnp.stack([edge[i] for i in row]) for row in order])
    edge = jnp.transpose(edge, (0, 2, 1, 3))
    edge = jnp.pad(edge, ((0, 0), (0, 0), (0, 5), (0, LANES - plan.zc)))
    special = (gy == 0) & ((group == 0) | (group == plan.groups // 2))
    spot = (jnp.arange(8)[:, None] == 0) & (jnp.arange(LANES)[None, :] < plan.zc)
    mask = jnp.where(special & spot, 1.0, 0.0).astype(jnp.float32)
    return tensor, edge, mask


def call(body, places, outs, scratch):
    spaces = {"h": pltpu.HBM, "v": pltpu.VMEM, "s": pltpu.SMEM}

    def space_of(out):
        return pltpu.VMEM if isinstance(out, pl.MemoryRef) else pl.ANY

    step = pl.pallas_call(
        body,
        out_shape=outs,
        in_specs=[pl.BlockSpec(memory_space=spaces[p]) for p in places],
        out_specs=jax.tree.map(lambda o: pl.BlockSpec(memory_space=space_of(o)), outs),
        scratch_shapes=scratch,
        compiler_params=pltpu.CompilerParams(vmem_limit_bytes=8 * 2**20),
    )

    def run(*args):
        return step(
            *(
                x if p == "s" else pltpu.with_memory_space_constraint(x, spaces[p])
                for p, x in zip(places, args)
            )
        )

    return run


SEND_ORDER = (4, 1, 5, 7, 6, 3, 2)


def plane_swap(plan, chunks):
    members = range(plan.planes)
    out = list(chunks)
    for o in SEND_ORDER:
        out[o] = lax.ppermute(chunks[o], ("gx", "gy"), [(k, k ^ o) for k in members])
    return out


def on_chip(like, *tables):
    there = like > -1e30
    return [jnp.where(there, t, jnp.zeros((), t.dtype)) for t in tables]


def fast_shards(plan, magnetization, kernel, applied):
    f32, bf16 = jnp.float32, jnp.bfloat16
    sds, vmem, dma = jax.ShapeDtypeStruct, pltpu.VMEM, pltpu.SemaphoreType.DMA
    n, zc, planes = plan.devices, plan.zc, plan.planes
    width = 3 * plan.lx * plan.ly
    tiles = width // LANES
    fwd, back = xy_tables(plan)
    fwd = [split_table(t, 2) for t in (fwd[:, :, 0:256], fwd[:, :, 256:512])]
    back = [split_table(t, 1) for t in (back[:, :, 0:256], back[:, :, 256:512])]
    zf, zb = z_tables(plan)
    zf, zb = split_table(zf, 0), split_table(zb, 0)
    chunk = vmem((zc, width), f32)
    spectrum = (n, 6, SUBS, LANES)
    m_tiles = magnetization.reshape(tiles, LANES, LANES)
    packed = call(
        lambda *a: pack_kernel(plan, *a),
        "h",
        [chunk] * planes,
        [vmem((tiles, LANES, LANES), f32), vmem((plan.lz, width), f32), dma((3,))],
    )(m_tiles)
    late = lax.axis_index("gy").astype(f32)
    first, kernel, late = lax.optimization_barrier((packed[0], kernel, late))
    packed = [first, *packed[1:]]
    own, other = tensor_pick(plan, kernel)
    fwd = on_chip(late, *fwd)
    tensor, edge, mask = field_tensor(plan, own, other)
    zf, zb = on_chip(tensor[0, 0, 0, 0], zf, zb)
    lines = plane_swap(plan, packed)
    spec = call(
        lambda *a: xy_forward_kernel(plan, *a),
        "v" * planes + "vv",
        sds(spectrum, f32),
        [
            vmem((planes, zc, width), f32),
            vmem((2, 3, LANES, 512), bf16),
            vmem((2, LANES, 512), bf16),
            vmem((2, SUBS, LANES), f32),
            vmem(spectrum, f32),
            dma((3,)),
        ],
    )(*lines, *fwd)
    spec = lax.all_to_all(spec, ("gx", "gy", "gz"), split_axis=0, concat_axis=0, tiled=True)
    spec = call(
        lambda *a: z_kernel(plan, *a),
        "vvvvvv",
        vmem(spectrum, f32),
        [
            vmem((4, n * SUBS, 256), f32),
            vmem((n, SUBS, LANES), f32),
            vmem((2, n, LANES), f32),
        ],
    )(spec, tensor, edge, mask, zf, zb)
    spec = lax.all_to_all(spec, ("gx", "gy", "gz"), split_axis=0, concat_axis=0, tiled=True)
    field = call(
        lambda *a: xy_inverse_kernel(plan, *a),
        "vvv",
        [chunk] * planes,
        [
            vmem((3, 2, 256, LANES), f32),
            vmem((2, 3 * LANES, 512), bf16),
            vmem((2, 3 * LANES, 256), f32),
            vmem((planes, zc, width), f32),
            vmem((2, SUBS, LANES), f32),
        ],
    )(spec, *back)
    field = plane_swap(plan, field)
    cells = (3, tiles // 3, LANES, LANES)
    pred, torque = call(
        lambda *a: finish_kernel(plan, *a),
        "v" * planes + "vs",
        (sds(cells, f32), sds(cells, f32)),
        [
            vmem((plan.lz, width), f32),
            vmem(cells, f32),
            vmem(cells, f32),
            dma((2, tiles // 3)),
        ],
    )(*field, magnetization.reshape(cells), applied)
    return pred.reshape(magnetization.shape), torque.reshape(magnetization.shape)


def solution(mesh):
    sizes = mesh.shape

    def shards(magnetization, kernel, applied):
        plan = Plan(sizes["gx"], sizes["gy"], sizes["gz"], magnetization.shape)
        if plan.fits():
            return fast_shards(plan, magnetization, kernel, applied)
        return general_shards(magnetization, kernel, applied)

    return jax.shard_map(
        shards,
        mesh=mesh,
        in_specs=(P(None, "gx", "gy", "gz"), P(None, ("gx", "gz"), "gy", None), P()),
        out_specs=(P(None, "gx", "gy", "gz"), P(None, "gx", "gy", "gz")),
        check_vma=False,
    )
```

```python
import math

import jax
import jax.numpy as jnp
import numpy as np
from jax import lax
from jax.experimental import pallas as pl
from jax.experimental.pallas import tpu as pltpu
from jax.sharding import PartitionSpec as P


exchange_coeff = 1.0
damping = 0.3
time_step = 0.2
highest = lax.Precision.HIGHEST
LANES = 128
SUBS = 8
SLOTS = 8


def phase_table(row_index, col_index, length):
    product = row_index[:, None] * col_index[None, :] % length
    angles = product.astype(jnp.float32) * (2.0 * math.pi / length)
    return (jnp.cos(angles), jnp.sin(angles))


def forward_mix(real_part, imag_part, cosine_table, sine_table, pattern):
    real_out = jnp.einsum(pattern, real_part, cosine_table, precision=highest) + jnp.einsum(
        pattern, imag_part, sine_table, precision=highest
    )
    imag_out = jnp.einsum(pattern, imag_part, cosine_table, precision=highest) - jnp.einsum(
        pattern, real_part, sine_table, precision=highest
    )
    return (real_out, imag_out)


def inverse_mix(real_part, imag_part, cosine_table, sine_table, pattern):
    real_out = jnp.einsum(pattern, real_part, cosine_table, precision=highest) - jnp.einsum(
        pattern, imag_part, sine_table, precision=highest
    )
    imag_out = jnp.einsum(pattern, imag_part, cosine_table, precision=highest) + jnp.einsum(
        pattern, real_part, sine_table, precision=highest
    )
    return (real_out, imag_out)


def apply_tensor(kernel, spectrum):
    return jnp.stack(
        [
            kernel[0] * spectrum[0] + kernel[3] * spectrum[1] + kernel[4] * spectrum[2],
            kernel[3] * spectrum[0] + kernel[1] * spectrum[1] + kernel[5] * spectrum[2],
            kernel[4] * spectrum[0] + kernel[5] * spectrum[1] + kernel[2] * spectrum[2],
        ]
    )


def cross_product(first_vec, second_vec):
    return jnp.stack(
        [
            first_vec[1] * second_vec[2] - first_vec[2] * second_vec[1],
            first_vec[2] * second_vec[0] - first_vec[0] * second_vec[2],
            first_vec[0] * second_vec[1] - first_vec[1] * second_vec[0],
        ]
    )


def general_shards(magnetization, kernel, applied):
    count_gx = lax.axis_size("gx")
    count_gy = lax.axis_size("gy")
    count_gz = lax.axis_size("gz")
    local_x = magnetization.shape[1]
    local_y = magnetization.shape[2]
    local_z = magnetization.shape[3]
    full_x = local_x * count_gx
    full_y = local_y * count_gy
    full_z = local_z * count_gz
    part_x = local_x // count_gz
    part_y = full_y // (count_gx * count_gz)
    part_z = full_z // count_gy
    outside = applied[:, None, None, None]
    z_index = jnp.arange(full_z, dtype=jnp.int32)
    weights = jnp.ones((full_z,), jnp.float32)
    planes = z_index.shape[0] // count_gy
    wave_count = z_index.shape[0]
    zlines = lax.all_to_all(magnetization, "gz", split_axis=1, concat_axis=3, tiled=True)
    cos_zf, sin_zf = phase_table(z_index, z_index, full_z)
    cos_zb, sin_zb = phase_table(z_index, z_index, full_z)
    cos_zb = cos_zb * weights[:, None]
    sin_zb = sin_zb * weights[:, None]
    lines_shape = (3, part_x, local_y, full_z)
    wave_shape = (3, part_x, local_y, wave_count)
    z_rows = zlines.reshape(-1, full_z)
    spec_real = jnp.dot(z_rows, cos_zf, precision=highest).reshape(wave_shape)
    spec_imag = -jnp.dot(z_rows, sin_zf, precision=highest).reshape(wave_shape)
    spec_real, spec_imag = (
        lax.all_to_all(spec_real, "gy", split_axis=3, concat_axis=2, tiled=True),
        lax.all_to_all(spec_imag, "gy", split_axis=3, concat_axis=2, tiled=True),
    )
    y_index = jnp.arange(full_y, dtype=jnp.int32)
    cos_y, sin_y = phase_table(y_index, y_index, full_y)
    spec_real, spec_imag = forward_mix(spec_real, spec_imag, cos_y, sin_y, "cxyz,yk->ckxz")
    x_index = jnp.arange(full_x, dtype=jnp.int32)
    cos_xn, sin_xn = phase_table(x_index, x_index, full_x)
    spec_real, spec_imag = (
        lax.all_to_all(spec_real, ("gx", "gz"), split_axis=1, concat_axis=2, tiled=True),
        lax.all_to_all(spec_imag, ("gx", "gz"), split_axis=1, concat_axis=2, tiled=True),
    )
    cos_x, sin_x = (cos_xn, sin_xn)
    spec_real, spec_imag = forward_mix(spec_real, spec_imag, cos_x, sin_x, "cyxz,xk->cyzk")
    inverse_count = 1.0 / (full_x * full_y * full_z)
    out_real = -inverse_count * apply_tensor(kernel, spec_real)
    out_imag = -inverse_count * apply_tensor(kernel, spec_imag)
    wave_y = (lax.axis_index("gx") * count_gz + lax.axis_index("gz")) * part_y + jnp.arange(
        part_y, dtype=jnp.int32
    )
    wave_z = lax.axis_index("gy") * part_z + jnp.arange(planes, dtype=jnp.int32)
    eigenvalue = (
        lattice_eigen(wave_y, full_y)[:, None, None]
        + lattice_eigen(wave_z, full_z)[None, :, None]
        + lattice_eigen(x_index, full_x)[None, None, :]
    )
    factor = inverse_count * exchange_coeff * eigenvalue
    out_real = out_real + factor * spec_real
    out_imag = out_imag + factor * spec_imag
    back_real, back_imag = inverse_mix(out_real, out_imag, cos_xn, sin_xn, "cyzk,kx->cyxz")
    back_real, back_imag = (
        lax.all_to_all(back_real, ("gx", "gz"), split_axis=2, concat_axis=1, tiled=True),
        lax.all_to_all(back_imag, ("gx", "gz"), split_axis=2, concat_axis=1, tiled=True),
    )
    cos_yb, sin_yb = (cos_y, sin_y)
    back_real, back_imag = inverse_mix(back_real, back_imag, cos_yb, sin_yb, "cyxz,yn->cxnz")
    back_real, back_imag = (
        lax.all_to_all(back_real, "gy", split_axis=2, concat_axis=3, tiled=True),
        lax.all_to_all(back_imag, "gy", split_axis=2, concat_axis=3, tiled=True),
    )
    real_rows = back_real.reshape(-1, wave_count)
    imag_rows = back_imag.reshape(-1, wave_count)
    field_lines = (
        jnp.dot(real_rows, cos_zb, precision=highest)
        - jnp.dot(imag_rows, sin_zb, precision=highest)
    ).reshape(lines_shape)
    field_block = lax.all_to_all(field_lines, "gz", split_axis=3, concat_axis=1, tiled=True)
    total_field = field_block + outside
    precess = cross_product(magnetization, total_field)
    double_twist = cross_product(magnetization, precess)
    torque = -(precess + damping * double_twist) / (1.0 + damping * damping)
    stepped = magnetization + time_step * torque
    length = jnp.sqrt(jnp.sum(stepped * stepped, axis=0))
    return (stepped / length, torque)


def cmul_const(value, angle):
    re, im = value
    quarter = angle / (math.pi / 2)
    if abs(quarter - round(quarter)) < 1e-9:
        turn = round(quarter) % 4
        if turn == 0:
            return (re, im)
        if turn == 1:
            return (-im, re)
        if turn == 2:
            return (-re, -im)
        return (im, -re)
    c, s = math.cos(angle), math.sin(angle)
    if abs(abs(c) - abs(s)) < 1e-9:
        h = abs(c)
        sc, ss = math.copysign(1, c), math.copysign(1, s)
        first = re if sc > 0 else -re
        out_re = (first - im) if ss > 0 else (first + im)
        second = im if sc > 0 else -im
        out_im = (second + re) if ss > 0 else (second - re)
        return (h * out_re, h * out_im)
    return (c * re - s * im, c * im + s * re)


def cadd(a, b):
    return (a[0] + b[0], a[1] + b[1])


def csub(a, b):
    return (a[0] - b[0], a[1] - b[1])


def conj(a):
    return (a[0], -a[1])


def complex_fft(values, sign):
    n = len(values)
    if n == 1:
        return values
    even = complex_fft(values[0::2], sign)
    odd = complex_fft(values[1::2], sign)
    odd = [cmul_const(v, sign * 2 * math.pi * k / n) for k, v in enumerate(odd)]
    return [cadd(e, o) for e, o in zip(even, odd)] + [csub(e, o) for e, o in zip(even, odd)]


def real_fft(values):
    n = len(values)
    if n == 2:
        return [values[0] + values[1], values[0] - values[1]]
    even = real_fft(values[0::2])
    odd = real_fft(values[1::2])
    quarter = n // 4
    out = [None] * (n // 2 + 1)
    out[0] = even[0] + odd[0]
    out[n // 2] = even[0] - odd[0]
    for k in range(1, quarter):
        turned = cmul_const(odd[k], -2 * math.pi * k / n)
        out[k] = cadd(even[k], turned)
        out[n // 2 - k] = conj(csub(even[k], turned))
    out[quarter] = (even[quarter], -odd[quarter])
    return out


def real_ifft(values):
    n = 2 * (len(values) - 1)
    if n == 2:
        return [values[0] + values[1], values[0] - values[1]]
    quarter = n // 4
    even = [None] * (quarter + 1)
    odd = [None] * (quarter + 1)
    even[0] = values[0] + values[n // 2]
    odd[0] = values[0] - values[n // 2]
    for k in range(1, quarter):
        mirror = conj(values[n // 2 - k])
        even[k] = cadd(values[k], mirror)
        odd[k] = cmul_const(csub(values[k], mirror), 2 * math.pi * k / n)
    mid = values[quarter]
    even[quarter] = 2.0 * mid[0]
    odd[quarter] = -2.0 * mid[1]
    even = real_ifft(even)
    odd = real_ifft(odd)
    out = [None] * n
    out[0::2] = even
    out[1::2] = odd
    return out


def split(value):
    high = value.astype(jnp.bfloat16)
    return high, (value - high.astype(jnp.float32)).astype(jnp.bfloat16)


def split_table(table, axis):
    high = table.astype(jnp.bfloat16)
    low = (table - high.astype(np.float32)).astype(jnp.bfloat16)
    return np.concatenate([high, low], axis)


def high_high_low(value):
    return jnp.concatenate([value[:, 0:256], value[:, 0:256], value[:, 256:512]], 1)


def high_low_high(table, axis):
    high, low = (lax.slice_in_dim(table, at, at + 256, axis=axis) for at in (0, 256))
    return jnp.concatenate([high, low, high], axis)


def mm(a, b, dims):
    return lax.dot_general(a, b, (dims, ((), ())), preferred_element_type=jnp.float32)


class Plan:
    def __init__(self, cx, cy, cz, shape):
        comps, lx, ly, lz = shape
        self.comps, self.lx, self.ly, self.lz = comps, lx, ly, lz
        self.cx, self.cy, self.cz = cx, cy, cz
        self.nx, self.ny, self.nz = lx * cx, ly * cy, lz * cz
        self.planes = cx * cy
        self.groups = cx * cz
        self.devices = cx * cy * cz

    def fits(self):
        if self.devices % 1 or self.lz % self.planes:
            return False
        self.zc = self.lz // self.planes
        self.xl = LANES // self.ly if LANES % self.ly == 0 else 0
        return (
            self.comps == 3
            and self.xl == 4
            and self.cy == 2
            and self.nx == 16 * self.xl
            and self.lx % self.xl == 0
            and self.ly == 2 * self.groups
            and self.zc * SLOTS == LANES
            and self.lz == LANES
            and self.nz % self.zc == 0
        )


def slot_kx(kx2, slot):
    if slot:
        return slot + 16 * kx2
    return (0, 16, 8, 24)[kx2]


def xy_tables(plan):
    lane = np.arange(LANES)
    xl, yl = lane // plan.ly, lane % plan.ly
    half = plan.ny // 2
    fwd = np.zeros((2, 256, 512))
    back = np.zeros((2, 256, 512))
    for r in range(2):
        for k2h in range(2):
            for g in range(plan.groups):
                for ri in range(2):
                    for k2l in range(2):
                        for ql in range(2):
                            block = ri if r == 0 else 1 - ri
                            f = (k2h * plan.groups + g) * 8 + block * 4 + k2l * 2 + ql
                            kx2 = 2 * k2h + k2l
                            ky = 2 * (2 * g + ql) + r
                            ph = 2 * math.pi * (xl * kx2 / 4 + yl * ky / plan.ny)
                            c, s = np.cos(ph), np.sin(ph)
                            if ri == 0:
                                fwd[r, f, 0:128], fwd[r, f, 128:256] = c, s
                                back[r, f, 0:128], back[r, f, 128:256] = c, s
                            else:
                                fwd[r, f, 0:128], fwd[r, f, 128:256] = -s, c
                                back[r, f, 0:128], back[r, f, 128:256] = -s, c
                            kx = slot_kx(kx2, 0)
                            if kx2 == 0:
                                edge = ky in (0, half)
                                if edge:
                                    kx = 0 if ri == 0 else 32
                                else:
                                    kx = 0 if ky < half else 32
                            ph = 2 * math.pi * (xl * kx / plan.nx + yl * ky / plan.ny)
                            c, s = np.cos(ph), np.sin(ph)
                            at = 256 if kx % 16 == 0 else 384
                            if kx2 == 0 and edge:
                                fwd[r, f, at : at + 128] = c
                                back[r, f, at : at + 128] = c
                            else:
                                fwd[r, f, at : at + 128] = c if ri == 0 else -s
                                back[r, f, at : at + 128] = 2 * (c if ri == 0 else -s)
    return fwd.astype(np.float32), back.astype(np.float32)


def fill_twiddles(ref, rows, lane_index, length):
    row = lax.broadcasted_iota(jnp.int32, (rows, LANES), 0)
    angle = (row * lane_index).astype(jnp.float32) * (2 * math.pi / length)
    ref[0] = jnp.cos(angle)
    ref[1] = jnp.sin(angle)


def fill_x_twiddles(plan, ref):
    lane = lax.broadcasted_iota(jnp.int32, (SUBS, LANES), 1)
    fill_twiddles(ref, SUBS, lane // plan.ly, plan.nx)


def z_tables(plan):
    zc = plan.zc
    small = 2 * math.pi * np.arange(zc)[:, None] * np.arange(zc)[None, :] / zc
    c = np.kron(np.eye(SLOTS), np.cos(small))
    s = np.kron(np.eye(SLOTS), np.sin(small))
    fwd = np.block([[c, -s], [s, c]]).astype(np.float32)
    back = np.block([[c, s], [-s, c]]).astype(np.float32)
    return fwd, back


def fetch(source, target, sem):
    copy = pltpu.make_async_copy(source, target, sem)
    copy.start()
    return copy


def plane_index():
    return lax.axis_index("gx") * lax.axis_size("gy") + lax.axis_index("gy")


def pack_kernel(plan, m_ref, *rest):
    outs, (m_buf, buf, sem_in) = rest[: plan.planes], rest[plan.planes :]
    me = plane_index()
    per = plan.lx * plan.ly // LANES
    width = per * LANES
    loads = [
        fetch(m_ref.at[pl.ds(c * per, per)], m_buf.at[pl.ds(c * per, per)], sem_in.at[c])
        for c in range(plan.comps)
    ]
    for c in range(plan.comps):
        loads[c].wait()
        for t in range(c * per, (c + 1) * per):
            buf[:, LANES * t : LANES * (t + 1)] = m_buf[t].T
        for o in range(plan.planes):
            rows = pl.ds(plan.zc * (me ^ o), plan.zc)
            cols = slice(width * c, width * (c + 1))
            outs[o][:, cols] = buf[rows, cols]


def xy_forward_kernel(plan, *refs):
    chunks, refs = refs[: plan.planes], refs[plan.planes :]
    table_ref, edge_ref, out_hbm, lines_ref, g_ref, e_ref, tw_ref, out_ref, sem = refs
    stores = []
    me = plane_index()
    fill_x_twiddles(plan, tw_ref)
    for o in range(plan.planes):
        lines_ref[me ^ o] = chunks[o][...]
    zc = plan.zc
    per = plan.lx // plan.xl
    low = lax.broadcasted_iota(jnp.int32, (SUBS, LANES), 0) < 4
    first_slot = lax.broadcasted_iota(jnp.int32, (SUBS, LANES), 1) < zc
    blank = jnp.zeros((zc, LANES), jnp.bfloat16)
    for r in range(2):
        for k in range(plan.comps, SLOTS):
            for q in range(4):
                e_ref[r, zc * k : zc * (k + 1), LANES * q : LANES * (q + 1)] = blank

    def keep(ref, at, rows, parts):
        for q, part in enumerate(parts):
            hi, lo = split(part)
            ref[(*at, rows, slice(LANES * q, LANES * (q + 1)))] = hi
            ref[(*at, rows, slice(LANES * (q + 2), LANES * (q + 3)))] = lo

    for c in range(plan.comps):
        parts = [[], []]
        for gx in range(plan.cx):
            for xh in range(per):
                at = c * (plan.lx * plan.ly) + xh * LANES
                first = lines_ref[gx * 2, :, at : at + LANES]
                second = lines_ref[gx * 2 + 1, :, at : at + LANES]
                parts[0].append(first + second)
                parts[1].append(first - second)
        for r in range(2):
            spec = real_fft(parts[r])
            keep(e_ref, (r,), slice(zc * c, zc * (c + 1)), (spec[0], spec[8]))
            for k in range(1, SLOTS):
                re, im = spec[k]
                tc = tw_ref[0, k : k + 1, :]
                ts = tw_ref[1, k : k + 1, :]
                rows = slice(zc * k, zc * (k + 1))
                keep(g_ref, (r, c), rows, (re * tc + im * ts, im * tc - re * ts))
            g_ref[r, c, 0:zc, :] = jnp.zeros((zc, 512), jnp.bfloat16)

    edges = [mm(high_low_high(edge_ref[r], 1), high_high_low(e_ref[r]), ((1,), (1,))) for r in range(2)]
    for c in range(plan.comps):
        outs = [
            mm(high_low_high(table_ref[r], 1), high_high_low(g_ref[r, c]), ((1,), (1,)))
            for r in range(2)
        ]
        for k2h in range(2):
            for g in range(plan.groups):
                f = (k2h * plan.groups + g) * SUBS
                both = []
                for r in range(2):
                    edge = edges[r][f : f + SUBS]
                    if c:
                        edge = pltpu.roll(edge, LANES - zc * c, 1)
                    both.append(jnp.where(first_slot, edge, outs[r][f : f + SUBS]))
                one, two = both
                gx, gz = g // plan.cz, g % plan.cz
                dest = (gx * plan.cy + k2h) * plan.cz + gz
                out_ref[dest, 2 * c] = jnp.where(low, one, two)
                out_ref[dest, 2 * c + 1] = pltpu.roll(jnp.where(low, two, one), 4, 0)
        pair = pl.ds(2 * c, 2)
        stores.append(fetch(out_ref.at[:, pair], out_hbm.at[:, pair], sem.at[c]))
    for store in stores:
        store.wait()


def xy_inverse_kernel(plan, spec_ref, table_ref, edge_ref, *refs):
    outs, (h_ref, t_ref, u_ref, out_ref, tw_ref) = refs[: plan.planes], refs[plan.planes :]
    me = plane_index()
    fill_x_twiddles(plan, tw_ref)
    zc = plan.zc
    per = plan.lx // plan.xl
    low = lax.broadcasted_iota(jnp.int32, (SUBS, LANES), 0) < 4
    for c in range(plan.comps):
        for k2h in range(2):
            for g in range(plan.groups):
                f = (k2h * plan.groups + g) * SUBS
                gx, gz = g // plan.cz, g % plan.cz
                src = (gx * plan.cy + k2h) * plan.cz + gz
                re = spec_ref[src, 2 * c]
                im = pltpu.roll(spec_ref[src, 2 * c + 1], 4, 0)
                h_ref[c, 0, f : f + SUBS, :] = jnp.where(low, re, im)
                h_ref[c, 1, f : f + SUBS, :] = jnp.where(low, im, re)
        for r in range(2):
            hi, lo = split(h_ref[c, r].T)
            t_ref[r, LANES * c : LANES * (c + 1), 0:256] = hi
            t_ref[r, LANES * c : LANES * (c + 1), 256:512] = lo

    edges = []
    for r in range(2):
        u_ref[r] = mm(high_high_low(t_ref[r]), high_low_high(table_ref[r], 0), ((1,), (0,)))
        rows = jnp.concatenate(
            [t_ref[r, LANES * c : LANES * c + zc, :] for c in range(plan.comps)], 0
        )
        edges.append(mm(high_high_low(rows), high_low_high(edge_ref[r], 0), ((1,), (0,))))
    for c in range(plan.comps):
        fields = []
        for r in range(2):
            edge = edges[r][zc * c : zc * (c + 1)]
            values = [edge[:, 0:128]]
            for k in range(1, SLOTS):
                rows = slice(LANES * c + zc * k, LANES * c + zc * (k + 1))
                re = u_ref[r, rows, 0:128]
                im = u_ref[r, rows, 128:256]
                tc = tw_ref[0, k : k + 1, :]
                ts = tw_ref[1, k : k + 1, :]
                values.append((re * tc - im * ts, im * tc + re * ts))
            values.append(edge[:, 128:256])
            fields.append(real_ifft(values))
        for gx in range(plan.cx):
            for xh in range(per):
                at = c * (plan.lx * plan.ly) + xh * LANES
                one = fields[0][gx * per + xh]
                two = fields[1][gx * per + xh]
                out_ref[gx * 2, :, at : at + LANES] = one + two
                out_ref[gx * 2 + 1, :, at : at + LANES] = one - two
    for o in range(plan.planes):
        outs[o][...] = out_ref[me ^ o]


def z_kernel(
    plan, in_ref, k_ref, kx_ref, mask_ref, fwd_ref, back_ref, out_ref, s_ref, b_ref, tw_ref
):
    n = plan.devices
    lane = lax.broadcasted_iota(jnp.int32, (n, LANES), 1)
    fill_twiddles(tw_ref, n, lane % plan.zc, plan.nz)
    half = n // 2 + 1
    mask = mask_ref[...]
    place = [(s % plan.planes) * plan.cz + s // plan.planes for s in range(n)]
    keep = 1.0 - mask

    def transform(at, count, table):
        hi, lo = split(s_ref[at, 0 : SUBS * count, :])
        wide = jnp.concatenate([hi, hi, lo], 1)
        s_ref[at, 0 : SUBS * count, :] = mm(wide, high_low_high(table[...], 0), ((1,), (0,)))

    def to_spectrum(values, at):
        for k, (re, im) in enumerate(values):
            tc = tw_ref[0, k : k + 1, :]
            ts = tw_ref[1, k : k + 1, :]
            s_ref[at, SUBS * k : SUBS * (k + 1), 0:128] = re * tc + im * ts
            s_ref[at, SUBS * k : SUBS * (k + 1), 128:256] = im * tc - re * ts
        transform(at, len(values), fwd_ref)

    def from_spectrum(at, count):
        transform(at, count, back_ref)
        values = []
        for k in range(count):
            re = s_ref[at, SUBS * k : SUBS * (k + 1), 0:128]
            im = s_ref[at, SUBS * k : SUBS * (k + 1), 128:256]
            tc = tw_ref[0, k : k + 1, :]
            ts = tw_ref[1, k : k + 1, :]
            values.append((re * tc - im * ts, im * tc + re * ts))
        return values

    for c in range(plan.comps):
        values = [(in_ref[place[s], 2 * c], in_ref[place[s], 2 * c + 1] * keep) for s in range(n)]
        to_spectrum(complex_fft(values, -1), c)
    extra = []
    for s in range(n):
        e = in_ref[place[s], 1] * mask
        e = e + pltpu.roll(in_ref[place[s], 3] * mask, 1, 0)
        e = e + pltpu.roll(in_ref[place[s], 5] * mask, 2, 0)
        extra.append(e + pltpu.roll(e, 3, 0))
    extra = real_fft(extra)
    zero = jnp.zeros((SUBS, LANES), jnp.float32)
    extra[0] = (extra[0], zero)
    extra[-1] = (extra[-1], zero)
    to_spectrum(extra, 3)
    for k in range(n):
        rows = slice(SUBS * k, SUBS * (k + 1))
        t = [k_ref[i, k] for i in range(6)]
        for part in range(2):
            lanes = slice(LANES * part, LANES * (part + 1))
            a, b, g = (s_ref[c, rows, lanes] for c in range(3))
            s_ref[0, rows, lanes] = t[0] * a + t[3] * b + t[4] * g
            s_ref[1, rows, lanes] = t[3] * a + t[1] * b + t[5] * g
            s_ref[2, rows, lanes] = t[4] * a + t[5] * b + t[2] * g
            if k < half:
                d = [kx_ref[i, k] for i in range(3)]
                e = s_ref[3, rows, lanes]
                s_ref[3, rows, lanes] = (
                    d[0] * e + d[1] * pltpu.roll(e, 7, 0) + d[2] * pltpu.roll(e, 6, 0)
                )
    extra = from_spectrum(3, half)
    extra[0] = extra[0][0]
    extra[-1] = extra[-1][0]
    extra = real_ifft(extra)
    for s in range(n):
        b_ref[s] = extra[s]
    for c in range(plan.comps):
        values = complex_fft(from_spectrum(c, n), 1)
        for s in range(n):
            e = b_ref[s]
            if c:
                e = pltpu.roll(e, SUBS - c, 0)
            out_ref[place[s], 2 * c] = values[s][0]
            out_ref[place[s], 2 * c + 1] = values[s][1] * keep + e * mask


def finish_kernel(plan, *refs):
    chunks, refs = refs[: plan.planes], refs[plan.planes :]
    m_ref, applied_ref, pred_hbm, torque_hbm, *refs = refs
    field_ref, pred_ref, torque_ref, sem_out = refs
    me = plane_index()
    tiles = plan.lx * plan.ly // LANES
    for o in range(plan.planes):
        field_ref[pl.ds(plan.zc * (me ^ o), plan.zc), :] = chunks[o][...]
    stores = []
    scale = -1.0 / (1.0 + damping * damping)
    for t in range(tiles):
        h, m = [], []
        for c in range(3):
            at = (c * tiles + t) * LANES
            h.append(field_ref[:, at : at + LANES].T + applied_ref[c])
            m.append(m_ref[c, t])
        a = [m[1] * h[2] - m[2] * h[1], m[2] * h[0] - m[0] * h[2], m[0] * h[1] - m[1] * h[0]]
        b = [m[1] * a[2] - m[2] * a[1], m[2] * a[0] - m[0] * a[2], m[0] * a[1] - m[1] * a[0]]
        torque = [(a[c] + damping * b[c]) * scale for c in range(3)]
        step = [m[c] + time_step * torque[c] for c in range(3)]
        total = step[0] * step[0] + step[1] * step[1] + step[2] * step[2]
        inverse = lax.rsqrt(total)
        for c in range(3):
            torque_ref[c, t] = torque[c]
            pred_ref[c, t] = step[c] * inverse
        stores.append(fetch(torque_ref.at[:, t], torque_hbm.at[:, t], sem_out.at[0, t]))
        stores.append(fetch(pred_ref.at[:, t], pred_hbm.at[:, t], sem_out.at[1, t]))
    for store in stores:
        store.wait()


def lattice_eigen(wave_index, length):
    return 2.0 * jnp.cos(wave_index.astype(jnp.float32) * (2.0 * math.pi / length)) - 2.0


def tensor_pick_kernel(plan, k_hbm, own_ref, give_ref, k_ref, sem):
    parts = 6
    loads = [fetch(k_hbm.at[i], k_ref.at[i], sem.at[i]) for i in range(parts)]
    group = lax.axis_index("gx") * plan.cz + lax.axis_index("gz")
    low = lax.axis_index("gy") == 0
    sub = lax.broadcasted_iota(jnp.int32, (SUBS, k_ref.shape[3]), 0)
    top = sub == 0
    edge = jnp.zeros(sub.shape, jnp.float32)
    tile = lambda i, j, t: k_ref[i, j, SUBS * t : SUBS * (t + 1), :]
    for i in range(parts):
        loads[i].wait()
        edge = jnp.where(sub == i, pltpu.roll(tile(i, 0, 4), i, 0), edge)
        for j in range(4):
            far = 4 * group + j > plan.ny // 2
            values = [
                jnp.where(top & far, tile(i, j, 4), tile(i, j, 0)),
                tile(i, j, 2),
                jnp.where(top, tile(i, j, 1), tile(i, j, 4)),
                jnp.where(top, tile(i, j, 3), tile(i, j, 6)),
            ]
            for k2l in range(2):
                row = ((i * 4 + j) * 2 + k2l) * SUBS
                own_ref[row : row + SUBS, :] = jnp.where(low, values[k2l], values[2 + k2l])
                give_ref[row : row + SUBS, :] = jnp.where(low, values[2 + k2l], values[k2l])
    row = parts * 4 * 2 * SUBS
    own_ref[row : row + SUBS, :] = edge
    give_ref[row : row + SUBS, :] = edge


def tensor_pick(plan, kernel):
    rows = pltpu.VMEM((6 * 4 * 2 * SUBS + SUBS, kernel.shape[2]), jnp.float32)
    kt = jnp.swapaxes(kernel, 2, 3)
    return call(
        lambda *a: tensor_pick_kernel(plan, *a),
        "h",
        (rows, rows),
        [pltpu.VMEM(kt.shape, jnp.float32), pltpu.SemaphoreType.DMA((6,))],
    )(kt)


def field_tensor(plan, own, other):
    gx, gy, gz = (lax.axis_index(a) for a in ("gx", "gy", "gz"))
    group = gx * plan.cz + gz
    kzs = own.shape[1]
    other = lax.ppermute(other, "gy", [(0, 1), (1, 0)])
    own, other = own[None], other[None]
    got = jnp.where(gy == 0, jnp.concatenate([own, other]), jnp.concatenate([other, own]))
    main = got[:, : 6 * 4 * 2 * 8].reshape(2, 6, 2, 2, 2, 8, kzs // 32, 32)
    main = jnp.transpose(main, (1, 7, 3, 4, 2, 5, 0, 6)).reshape(6, 32, 8, 128)
    edge = got[:, 6 * 4 * 2 * 8 : 6 * 4 * 2 * 8 + 6].reshape(2, 6, kzs // 32, 32)
    edge = jnp.transpose(edge, (1, 3, 0, 2)).reshape(6, 32, plan.zc)
    kz = jnp.arange(plan.nz).reshape(plan.zc, 32).T
    table = np.array([[slot_kx(k2, s) for s in range(SLOTS)] for k2 in range(4)])
    table = table.reshape(2, 2, SLOTS).astype(np.int32)
    kx = jnp.where(gy == 0, table[0], table[1])
    kyq = (4 * group + 2 * jnp.arange(2)[None, :] + jnp.arange(2)[:, None])
    kx_full = jnp.broadcast_to(kx[None, :, None, :], (2, 2, 2, SLOTS))
    swap = (gy == 0) & (kyq > plan.ny // 2)
    is_packed = (jnp.arange(2)[None, :, None, None] == 0) & (jnp.arange(SLOTS) == 0)
    kx_full = jnp.where(is_packed & swap[:, None, :, None], 32, kx_full)
    ex = lattice_eigen(kx_full, plan.nx)
    ey = lattice_eigen(kyq, plan.ny)
    ez = lattice_eigen(kz, plan.nz)
    plane = (ex + ey[:, None, :, None]).reshape(8, SLOTS)
    eig = plane[None, :, :, None] + ez[:, None, None, :]
    eig = eig.reshape(32, 8, 128)
    scale = 1.0 / (plan.nx * plan.ny * plan.nz)
    diag = jnp.asarray([1, 1, 1, 0, 0, 0], jnp.float32)[:, None, None, None]
    tensor = scale * (exchange_coeff * diag * eig[None] - main)
    edge_eig = lattice_eigen(jnp.asarray(32), plan.nx) + lattice_eigen(4 * group, plan.ny) + ez
    edge = scale * (exchange_coeff * diag[:, :, :, 0] * edge_eig[None] - edge)
    order = ((0, 1, 2), (3, 5, 4), (4, 3, 5))
    edge = jnp.stack([jnp.stack([edge[i] for i in row]) for row in order])
    edge = jnp.transpose(edge, (0, 2, 1, 3))
    edge = jnp.pad(edge, ((0, 0), (0, 0), (0, 5), (0, LANES - plan.zc)))
    special = (gy == 0) & ((group == 0) | (group == plan.groups // 2))
    spot = (jnp.arange(8)[:, None] == 0) & (jnp.arange(LANES)[None, :] < plan.zc)
    mask = jnp.where(special & spot, 1.0, 0.0).astype(jnp.float32)
    return tensor, edge, mask


def call(body, places, outs, scratch):
    spaces = {"h": pltpu.HBM, "v": pltpu.VMEM, "s": pltpu.SMEM}

    def space_of(out):
        return pltpu.VMEM if isinstance(out, pl.MemoryRef) else pl.ANY

    step = pl.pallas_call(
        body,
        out_shape=outs,
        in_specs=[pl.BlockSpec(memory_space=spaces[p]) for p in places],
        out_specs=jax.tree.map(lambda o: pl.BlockSpec(memory_space=space_of(o)), outs),
        scratch_shapes=scratch,
        compiler_params=pltpu.CompilerParams(vmem_limit_bytes=8 * 2**20),
    )

    def run(*args):
        return step(
            *(
                x if p == "s" else pltpu.with_memory_space_constraint(x, spaces[p])
                for p, x in zip(places, args)
            )
        )

    return run


SEND_ORDER = {"gather": (4, 1, 5, 7, 6, 3, 2), "scatter": (4, 1, 5, 6, 3, 2, 7)}


def plane_swap(plan, chunks, name):
    members = range(plan.planes)
    out = list(chunks)
    for o in SEND_ORDER[name]:
        out[o] = lax.ppermute(chunks[o], ("gx", "gy"), [(k, k ^ o) for k in members])
    return out


def on_chip(like, *tables):
    there = like > -1e30
    return [jnp.where(there, t, jnp.zeros((), t.dtype)) for t in tables]


def fast_shards(plan, magnetization, kernel, applied):
    f32, bf16 = jnp.float32, jnp.bfloat16
    sds, vmem, dma = jax.ShapeDtypeStruct, pltpu.VMEM, pltpu.SemaphoreType.DMA
    n, zc, planes = plan.devices, plan.zc, plan.planes
    width = 3 * plan.lx * plan.ly
    tiles = width // LANES
    fwd, back = xy_tables(plan)
    fwd = [split_table(t, 2) for t in (fwd[:, :, 0:256], fwd[:, :, 256:512])]
    back = [split_table(t, 1) for t in (back[:, :, 0:256], back[:, :, 256:512])]
    zf, zb = z_tables(plan)
    zf, zb = split_table(zf, 0), split_table(zb, 0)
    chunk = vmem((zc, width), f32)
    spectrum = (n, 6, SUBS, LANES)
    m_tiles = magnetization.reshape(tiles, LANES, LANES)
    packed = call(
        lambda *a: pack_kernel(plan, *a),
        "h",
        [chunk] * planes,
        [vmem((tiles, LANES, LANES), f32), vmem((plan.lz, width), f32), dma((3,))],
    )(m_tiles)
    late = lax.axis_index("gy").astype(f32)
    first, kernel, late = lax.optimization_barrier((packed[0], kernel, late))
    packed = [first, *packed[1:]]
    own, other = tensor_pick(plan, kernel)
    fwd = on_chip(late, *fwd)
    tensor, edge, mask = field_tensor(plan, own, other)
    zf, zb = on_chip(tensor[0, 0, 0, 0], zf, zb)
    lines = plane_swap(plan, packed, "gather")
    spec = call(
        lambda *a: xy_forward_kernel(plan, *a),
        "v" * planes + "vv",
        sds(spectrum, f32),
        [
            vmem((planes, zc, width), f32),
            vmem((2, 3, LANES, 512), bf16),
            vmem((2, LANES, 512), bf16),
            vmem((2, SUBS, LANES), f32),
            vmem(spectrum, f32),
            dma((3,)),
        ],
    )(*lines, *fwd)
    spec = lax.all_to_all(spec, ("gx", "gy", "gz"), split_axis=0, concat_axis=0, tiled=True)
    spec = call(
        lambda *a: z_kernel(plan, *a),
        "vvvvvv",
        vmem(spectrum, f32),
        [
            vmem((4, n * SUBS, 256), f32),
            vmem((n, SUBS, LANES), f32),
            vmem((2, n, LANES), f32),
        ],
    )(spec, tensor, edge, mask, zf, zb)
    spec = lax.all_to_all(spec, ("gx", "gy", "gz"), split_axis=0, concat_axis=0, tiled=True)
    field = call(
        lambda *a: xy_inverse_kernel(plan, *a),
        "vvv",
        [chunk] * planes,
        [
            vmem((3, 2, 256, LANES), f32),
            vmem((2, 3 * LANES, 512), bf16),
            vmem((2, 3 * LANES, 256), f32),
            vmem((planes, zc, width), f32),
            vmem((2, SUBS, LANES), f32),
        ],
    )(spec, *back)
    field = plane_swap(plan, field, "scatter")
    cells = (3, tiles // 3, LANES, LANES)
    pred, torque = call(
        lambda *a: finish_kernel(plan, *a),
        "v" * planes + "vs",
        (sds(cells, f32), sds(cells, f32)),
        [
            vmem((plan.lz, width), f32),
            vmem(cells, f32),
            vmem(cells, f32),
            dma((2, tiles // 3)),
        ],
    )(*field, magnetization.reshape(cells), applied)
    return pred.reshape(magnetization.shape), torque.reshape(magnetization.shape)


def solution(mesh):
    sizes = mesh.shape

    def shards(magnetization, kernel, applied):
        plan = Plan(sizes["gx"], sizes["gy"], sizes["gz"], magnetization.shape)
        if plan.fits():
            return fast_shards(plan, magnetization, kernel, applied)
        return general_shards(magnetization, kernel, applied)

    return jax.shard_map(
        shards,
        mesh=mesh,
        in_specs=(P(None, "gx", "gy", "gz"), P(None, ("gx", "gz"), "gy", None), P()),
        out_specs=(P(None, "gx", "gy", "gz"), P(None, "gx", "gy", "gz")),
        check_vma=False,
    )
```
